128 devices in a mesh: seq: 16 (over x, z), feat: 8 (over y, core).
Axes of the slice: x: 4, y: 4, z: 4, core: 2. Of those that a mesh axis runs over, the one named last changes fastest.
Arguments:
- injection: bfloat16 [2048, 5120], P('seq', 'feat'), may hold values from -8 to 8
- warm_start: bfloat16 [2048, 5120], P('seq', 'feat'), may hold values from -12 to 12
- gain_in: float32 [5120], replicated, may hold values from 0.5 to 1.5
- gain_out: float32 [5120], replicated, may hold values from 0.5 to 1.5
- w_query: bfloat16 [5120, 5120], P(None, 'feat'), may hold values from -0.0848993624 to 0.0848993624
- w_key: bfloat16 [5120, 1024], P(None, 'feat'), may hold values from -0.0848993624 to 0.0848993624
- w_value: bfloat16 [5120, 1024], P(None, 'feat'), may hold values from -0.078125 to 0.078125
- w_out: bfloat16 [5120, 5120], P('feat'), may hold values from -0.078125 to 0.078125
Outputs:
- equilibrium: float32 [2048, 5120], P('seq', 'feat')
The draws below stay inside these ranges and needn't reach their ends.
All inputs are finite; a program needn't handle non-finite values.
Results may differ from the reference program's by a relative error of at most 0.009.
Values may be sent and summed in bfloat16 or wider, within the bound.
No kernel may reach another device: no remote copies, remote signals or barrier semaphores. Data moves between devices by JAX's collectives and lax.ppermute only.
A program may use at most 128 MiB of HBM per device.

```python
import math
import jax
import jax.numpy as jnp
from jax import lax

D = 5120
HEADS = 40
KV_HEADS = 8
HEAD_DIM = 128
ITERS = 4
TOKENS = 2048


ALIGN_TARGET = 325.0


def align_scale():
    return math.sqrt(ALIGN_TARGET / (D * math.sqrt(HEAD_DIM)))


def spike_layout(key):
    sign_query = jax.random.randint(jax.random.fold_in(key, 7001), (D,), 0, 2).astype(jnp.float32) * 2.0 - 1.0
    sign_key = jax.random.randint(jax.random.fold_in(key, 7002), (D,), 0, 2).astype(jnp.float32) * 2.0 - 1.0
    half_tokens = TOKENS // 2
    key_places = jax.random.permutation(jax.random.fold_in(key, 7003), half_tokens)[:8].astype(jnp.int32)
    query_places = (jax.random.permutation(jax.random.fold_in(key, 7004), half_tokens)[:8] + half_tokens).astype(jnp.int32)
    return (sign_query, sign_key, key_places, query_places)


def matrix_noise(key, columns):
    noise_part = jnp.clip(jax.random.normal(key, (D, columns), jnp.float32), -6.0, 6.0)
    return noise_part / math.sqrt(D)


def draw_injection(key, part):
    sign_query, sign_key, key_places, query_places = spike_layout(key)
    base_noise = jnp.clip(jax.random.normal(jax.random.fold_in(key, 11), (TOKENS, D), jnp.float32), -4.0, 4.0)
    position = jnp.arange(TOKENS, dtype=jnp.int32)
    query_strength = jnp.array([0.5, 0.5, 1.0, 1.0, 2.0, 2.0, 4.0, 4.0], jnp.float32)
    query_weight = jnp.sum(jnp.where(position[None, :] == query_places[:, None], query_strength[:, None], 0.0), axis=0)
    key_weight = jnp.sum(jnp.where(position[None, :] == key_places[:, None], 3.0, 0.0), axis=0)
    result = base_noise + query_weight[:, None] * sign_query[None, :] + key_weight[:, None] * sign_key[None, :]
    return result.astype(jnp.bfloat16)


def draw_w_query(key, part):
    sign_query, sign_key, key_places, query_places = spike_layout(key)
    noise_part = matrix_noise(jax.random.fold_in(key, 21), HEADS * HEAD_DIM)
    result = noise_part + align_scale() * sign_query[:, None] / math.sqrt(D)
    return result.astype(jnp.bfloat16)


def draw_w_key(key, part):
    sign_query, sign_key, key_places, query_places = spike_layout(key)
    noise_part = matrix_noise(jax.random.fold_in(key, 22), KV_HEADS * HEAD_DIM)
    result = noise_part + align_scale() * sign_key[:, None] / math.sqrt(D)
    return result.astype(jnp.bfloat16)


def draw_warm_start(key, part):
    row_frac = jnp.arange(TOKENS, dtype=jnp.float32) / (TOKENS - 1)
    col_frac = jnp.arange(D, dtype=jnp.float32) / (D - 1)
    row_rough = jnp.exp(jax.random.uniform(jax.random.fold_in(key, 31), (TOKENS,), jnp.float32, math.log(0.7), math.log(1.4)))
    col_rough = jnp.exp(jax.random.uniform(jax.random.fold_in(key, 32), (D,), jnp.float32, math.log(0.7), math.log(1.4)))
    col_scale = (0.6 + 0.9 * col_frac) * col_rough
    base_noise = jnp.clip(jax.random.normal(jax.random.fold_in(key, 33), (TOKENS, D), jnp.float32), -4.0, 4.0)
    row_scale = jnp.exp(math.log(0.25) + row_frac * math.log(10.0)) * row_rough
    result = base_noise * row_scale[:, None] * col_scale[None, :]
    return jnp.clip(result, -12.0, 12.0).astype(jnp.bfloat16)


def shard_levels(stream_key, shape, cuts, smallest, largest):
    loudness, own = 1.0, jax.random.fold_in(stream_key, 6)
    for dim, parts in cuts:
        heights = jnp.exp(jax.random.uniform(jax.random.fold_in(own, dim), (parts,), jnp.float32, smallest / len(cuts), largest / len(cuts)))
        loudness = loudness * jnp.repeat(heights, shape[dim] // parts).reshape([-1 if axis == dim else 1 for axis in range(len(shape))])
    return loudness


def centred(own_key, dims, width, limit, pieces=(), kind=jnp.bfloat16):
    values = jax.random.normal(own_key, dims, jnp.float32) * width
    if len(pieces) > 0:
        values = shard_levels(own_key, dims, pieces, -0.22, 0.18) * values
    return jnp.clip(values, min=-limit, max=limit).astype(kind)


def setup_inputs(seed: int = 0) -> dict:
    splits = jax.random.split(jax.random.key(seed), 9)
    return {
        "injection": draw_injection(jax.random.fold_in(splits[8], 71), 0),
        "warm_start": draw_warm_start(jax.random.fold_in(splits[8], 71), 0),
        "gain_in": jnp.clip(1.0 + 0.1 * jax.random.normal(splits[2], (D,), jnp.float32), 0.5, 1.5),
        "gain_out": jnp.clip(1.0 + 0.1 * jax.random.normal(splits[3], (D,), jnp.float32), 0.5, 1.5),
        "w_query": draw_w_query(jax.random.fold_in(splits[8], 71), 0),
        "w_key": draw_w_key(jax.random.fold_in(splits[8], 71), 0),
        "w_value": centred(splits[6], (D, KV_HEADS * HEAD_DIM), D ** -0.5, 0.078125, ((1, 8),)),
        "w_out": centred(splits[7], (HEADS * HEAD_DIM, D), (HEADS * HEAD_DIM) ** -0.5, 0.078125, ((0, 8),)),
    }


EPS = 1e-06
LAMBDA = 0.03

def rms_scale(matrix, gain_vec):
    return matrix * lax.rsqrt(lax.optimization_barrier(jnp.mean(matrix * matrix, axis=-1, keepdims=True)) + EPS) * gain_vec

def solve_small(matrix, target):
    size_now = target.shape[0]
    row_list = [matrix[idx_row] for idx_row in range(size_now)]
    value_list = [target[idx_row] for idx_row in range(size_now)]
    for pivot_at in range(size_now):
        for below_at in range(pivot_at + 1, size_now):
            ratio_now = row_list[below_at][pivot_at] / row_list[pivot_at][pivot_at]
            row_list[below_at] = row_list[below_at] - ratio_now * row_list[pivot_at]
            value_list[below_at] = value_list[below_at] - ratio_now * value_list[pivot_at]
    result_list = [None] * size_now
    for pivot_at in reversed(range(size_now)):
        running = value_list[pivot_at]
        for later_at in range(pivot_at + 1, size_now):
            running = running - row_list[pivot_at][later_at] * result_list[later_at]
        result_list[pivot_at] = running / row_list[pivot_at][pivot_at]
    return jnp.stack(result_list)

def coefficients(gram_matrix):
    history_len = gram_matrix.shape[0]
    system = gram_matrix / (TOKENS * D) + LAMBDA * jnp.eye(history_len, dtype=jnp.float32)
    unscaled = solve_small(system, jnp.ones((history_len,), jnp.float32))
    return unscaled / jnp.sum(unscaled)

def layer(current, injection, gain_in, gain_out, w_query, w_key, w_value, w_out):
    group = HEADS // KV_HEADS
    mixed = current + injection.astype(jnp.float32)
    normed = rms_scale(mixed, gain_in).astype(jnp.bfloat16)
    queries = jnp.dot(normed, w_query, preferred_element_type=jnp.float32).astype(jnp.bfloat16)
    key_rows = jnp.dot(normed, w_key, preferred_element_type=jnp.float32).astype(jnp.bfloat16)
    value_rows = jnp.dot(normed, w_value, preferred_element_type=jnp.float32).astype(jnp.bfloat16)
    queries = queries.reshape(TOKENS, KV_HEADS, group, HEAD_DIM).transpose(1, 2, 0, 3)
    key_rows = key_rows.reshape(TOKENS, KV_HEADS, HEAD_DIM).transpose(1, 0, 2)
    value_rows = value_rows.reshape(TOKENS, KV_HEADS, HEAD_DIM).transpose(1, 0, 2)
    position = jnp.arange(TOKENS, dtype=jnp.int32)
    allowed = position[:, None] >= position[None, :]
    score_scale = 1.0 / math.sqrt(HEAD_DIM)

    def one_head(operands):
        query_head, key_head, value_head = operands
        scores = jnp.einsum('gtd,sd->gts', query_head.astype(jnp.float32), key_head.astype(jnp.float32)) * score_scale
        scores = jnp.where(allowed[None], scores, -1e+30)
        row_max = lax.optimization_barrier(jnp.max(scores, axis=-1, keepdims=True))
        weights = jnp.where(allowed[None], jnp.exp(scores - row_max), 0.0)
        row_sum = lax.optimization_barrier(jnp.sum(weights, axis=-1, keepdims=True))
        summed = jnp.einsum('gts,sd->gtd', weights.astype(jnp.bfloat16).astype(jnp.float32), value_head.astype(jnp.float32))
        return (summed / row_sum).astype(jnp.bfloat16)
    attended = lax.map(one_head, (queries, key_rows, value_rows))
    attended = attended.transpose(2, 0, 1, 3).reshape(TOKENS, HEADS * HEAD_DIM)
    update = jnp.dot(attended, w_out, preferred_element_type=jnp.float32)
    return rms_scale(mixed + update, gain_out)

def reference(injection, warm_start, gain_in, gain_out, w_query, w_key, w_value, w_out):
    params = (injection, gain_in, gain_out, w_query, w_key, w_value, w_out)
    current = warm_start.astype(jnp.float32)
    evaluated = []
    residuals = []
    for iteration in range(ITERS):
        image = layer(current, *params)
        evaluated.append(image)
        residuals.append(image - current)
        if iteration == 0:
            current = image
        else:
            history_len = iteration + 1
            gram_matrix = jnp.stack([jnp.stack([jnp.sum(residuals[row_at] * residuals[col_at]) for col_at in range(history_len)]) for row_at in range(history_len)])
            weights_now = coefficients(gram_matrix)
            current = weights_now[0] * evaluated[0]
            for other in range(1, history_len):
                current = current + weights_now[other] * evaluated[other]
    return current
```

```python
import functools
import math

import jax
import jax.numpy as jnp
from jax import lax
from jax.experimental import pallas as pl
from jax.experimental.pallas import tpu as pltpu
from jax.sharding import Mesh
from jax.sharding import PartitionSpec as P

D = 5120
HEADS = 40
KV_HEADS = 8
HEAD_DIM = 128
GROUP = HEADS // KV_HEADS
ITERS = 4
TOKENS = 2048
SEQ = ("x", "z")
FEAT = ("y", "c")
EVERY = ("x", "z", "y", "c")
EPS = 1e-06
LAMBDA = 0.03
SCORE_SCALE = 1.0 / math.sqrt(HEAD_DIM)
F32 = jnp.float32
BF16 = jnp.bfloat16

VMEM = pl.BlockSpec(memory_space=pltpu.VMEM)
ANY = pl.BlockSpec(memory_space=pl.ANY)


def shift(n, by):
    return [(at, (at + by) % n) for at in range(n)]


def call(kernel, out_shape, *args, specs=None, scratch=(), flops=0, touched=0):
    return pl.pallas_call(
        kernel,
        out_shape=out_shape,
        in_specs=[VMEM] * len(args) if specs is None else specs,
        out_specs=jax.tree.map(lambda _: VMEM, out_shape),
        scratch_shapes=list(scratch),
        compiler_params=pltpu.CompilerParams(vmem_limit_bytes=48 * 1024 * 1024),
        cost_estimate=pl.CostEstimate(flops=flops, bytes_accessed=touched, transcendentals=0),
    )(*args)


def total(x):
    return jnp.sum(jnp.sum(x, axis=1, keepdims=True), axis=0, keepdims=True)


def norm_kernel(x_ref, inj_ref, gain_ref, mixed_ref, normed_ref):
    mixed = x_ref[...].astype(F32) + inj_ref[...].astype(F32)
    scale = lax.rsqrt(jnp.sum(mixed * mixed, axis=1, keepdims=True) / D + EPS)
    mixed_ref[...] = mixed
    normed_ref[...] = (mixed * scale * gain_ref[...]).astype(BF16)


def attend_kernel(q_ref, kv_ref, w_ref, own_ref, send_ref, w_held, sem):
    load = pltpu.make_async_copy(w_ref, w_held, sem)
    load.start()
    s = lax.axis_index("x") * 4 + lax.axis_index("z")
    y = lax.axis_index("y")
    c = lax.axis_index("c")

    def offset(row):
        half, block, inner = row // 64, (row // 16) % 4, row % 16
        return (((y - block + 4) % 4) * 2 + (c + half) % 2) * 16 + inner

    q_off = offset(lax.broadcasted_iota(jnp.int32, (128, 1), 0))
    column = lax.broadcasted_iota(jnp.int32, (1, TOKENS), 1)
    key_pos = (column // 128) * 128 + offset(column % 128)
    allowed = (s * 128 + q_off) >= key_pos
    kv = kv_ref[...].reshape(TOKENS, 2 * HEAD_DIM)
    keys, values = kv[:, :HEAD_DIM], kv[:, HEAD_DIM:]
    heads = []
    for g in range(GROUP):
        q = q_ref[:, g * HEAD_DIM : (g + 1) * HEAD_DIM]
        scores = lax.dot_general(q, keys, (((1,), (1,)), ((), ())), preferred_element_type=F32)
        scores = jnp.where(allowed, scores * SCORE_SCALE, -1e30)
        weights = jnp.exp(scores - jnp.max(scores, axis=1, keepdims=True))
        weights = jnp.where(allowed, weights, 0.0)
        row_sum = jnp.sum(weights, axis=1, keepdims=True)
        summed = jnp.dot(weights.astype(BF16), values, preferred_element_type=F32)
        heads.append((summed / row_sum).astype(BF16))
    attended = jnp.concatenate(heads, axis=1)
    load.wait()
    for at in range(0, D, 1280):
        part = jnp.dot(attended, w_held[:, at : at + 1280], preferred_element_type=F32)
        own_ref[:, at : at + 1280] = part[:64]
        send_ref[:, at : at + 1280] = part[64:].astype(BF16)


def finish_kernel(k, own_ref, a_ref, b_ref, d_ref, mixed_ref, x_ref, gain_ref, *rest):
    older, (image_ref, residual_ref, dots_ref) = rest[:-3], rest[-3:]
    summed = mixed_ref[...] + (
        own_ref[...] + a_ref[...].astype(F32) + b_ref[...].astype(F32) + d_ref[...].astype(F32)
    )
    scale = lax.rsqrt(jnp.sum(summed * summed, axis=1, keepdims=True) / D + EPS)
    image = summed * scale * gain_ref[...]
    residual = image - x_ref[...].astype(F32)
    image_ref[...] = image
    residual_ref[...] = residual
    lane = lax.broadcasted_iota(jnp.int32, (1, 128), 1)
    dots = jnp.where(lane == k, total(residual * residual), 0.0)
    for at, other in enumerate(older):
        dots = dots + jnp.where(lane == at, total(residual * other[...]), 0.0)
    if k == 1:
        dots = dots + jnp.where(lane == 7, total(older[0][...] * older[0][...]), 0.0)
    dots_ref[...] = dots


def solve_small(matrix, size_now):
    rows = [list(row) for row in matrix]
    values = [jnp.ones((1, 1), F32) for _ in range(size_now)]
    for pivot in range(size_now):
        for below in range(pivot + 1, size_now):
            ratio = rows[below][pivot] / rows[pivot][pivot]
            rows[below] = [b - ratio * p for b, p in zip(rows[below], rows[pivot])]
            values[below] = values[below] - ratio * values[pivot]
    result = [None] * size_now
    for pivot in reversed(range(size_now)):
        running = values[pivot]
        for later in range(pivot + 1, size_now):
            running = running - rows[pivot][later] * result[later]
        result[pivot] = running / rows[pivot][pivot]
    return result


def mix_kernel(k, last, *refs):
    tables, images = refs[:k], refs[k : 2 * k + 1]
    lane = lax.broadcasted_iota(jnp.int32, (1, 128), 1)
    gram = {}
    for at, table in enumerate(tables):
        sums = jnp.sum(table[...], axis=0, keepdims=True)
        for other in range(at + 2):
            gram[at + 1, other] = jnp.sum(jnp.where(lane == other, sums, 0.0), axis=1, keepdims=True)
        if at == 0:
            gram[0, 0] = jnp.sum(jnp.where(lane == 7, sums, 0.0), axis=1, keepdims=True)
    system = [
        [
            gram[max(i, j), min(i, j)] / float(TOKENS * D) + (LAMBDA if i == j else 0.0)
            for j in range(k + 1)
        ]
        for i in range(k + 1)
    ]
    unscaled = solve_small(system, k + 1)
    whole = functools.reduce(lambda a, b: a + b, unscaled)
    current = functools.reduce(
        lambda a, b: a + b, [u / whole * image[...] for u, image in zip(unscaled, images)]
    )
    if last:
        refs[-1][...] = current
        return
    inj_ref, gain_ref, current_ref, mixed_ref, normed_ref = refs[2 * k + 1 :]
    mixed = current + inj_ref[...].astype(F32)
    scale = lax.rsqrt(jnp.sum(mixed * mixed, axis=1, keepdims=True) / D + EPS)
    current_ref[...] = current
    mixed_ref[...] = mixed
    normed_ref[...] = (mixed * scale * gain_ref[...]).astype(BF16)


def on_device(injection, warm_start, gain_in, gain_out, w_query, w_key, w_value, w_out):
    gain_in, gain_out = gain_in.reshape(1, D), gain_out.reshape(1, D)
    w_kv = jnp.concatenate([w_key, w_value], axis=1)
    tokens = jax.ShapeDtypeStruct((16, D), F32)
    narrow = jax.ShapeDtypeStruct((16, D), BF16)
    both = jnp.stack([injection, warm_start]).reshape(2, 8, 16, 640)
    both = lax.all_to_all(both, FEAT, split_axis=1, concat_axis=1, tiled=True)
    both = both.transpose(0, 2, 1, 3).reshape(2, 16, D)
    inj, current = both[0], both[1]
    mixed, normed = call(norm_kernel, (tokens, narrow), current, inj, gain_in)
    images, residuals, tables = [], [], []
    for k in range(ITERS):
        pieces = [normed] + [lax.ppermute(normed, "y", shift(4, by)) for by in (1, 2, 3)]
        mine = jnp.concatenate(pieces, axis=0)
        rows = jnp.concatenate([mine, lax.ppermute(mine, "c", shift(2, 1))], axis=0)
        kv = jnp.dot(rows, w_kv, preferred_element_type=F32).astype(BF16)
        kv_all = lax.all_to_all(
            jnp.broadcast_to(kv, (16, 128, 2 * HEAD_DIM)), SEQ, split_axis=0, concat_axis=0, tiled=True
        )
        q = jnp.dot(rows, w_query, preferred_element_type=F32).astype(BF16)
        own, send = call(
            attend_kernel,
            (jax.ShapeDtypeStruct((64, D), F32), jax.ShapeDtypeStruct((64, D), BF16)),
            q,
            kv_all,
            w_out,
            specs=[VMEM, VMEM, ANY],
            scratch=[pltpu.VMEM((640, D), BF16), pltpu.SemaphoreType.DMA],
            flops=2 * 128 * 640 * (2 * TOKENS + D),
            touched=9_000_000,
        )
        pair = own + lax.ppermute(send, "c", shift(2, 1)).astype(F32)
        arrived = [
            lax.ppermute(pair[16 * by : 16 * by + 16].astype(BF16), "y", shift(4, -by))
            for by in (1, 2, 3)
        ]
        image, residual, dots = call(
            functools.partial(finish_kernel, k),
            (tokens, tokens, jax.ShapeDtypeStruct((1, 128), F32)),
            pair[:16],
            *arrived,
            mixed,
            current,
            gain_out,
            *residuals,
        )
        images.append(image)
        residuals.append(residual)
        if k == 0:
            current = image
            mixed, normed = call(norm_kernel, (tokens, narrow), current, inj, gain_in)
            continue
        tables.append(
            lax.all_to_all(
                jnp.broadcast_to(dots, (128, 128)), EVERY, split_axis=0, concat_axis=0, tiled=True
            )
        )
        if k < ITERS - 1:
            current, mixed, normed = call(
                functools.partial(mix_kernel, k, False),
                (tokens, tokens, narrow),
                *tables,
                *images,
                inj,
                gain_in,
            )
        else:
            current = call(functools.partial(mix_kernel, k, True), tokens, *tables, *images)
    return lax.all_to_all(current, FEAT, split_axis=1, concat_axis=0, tiled=True)


def solution(mesh):
    split = Mesh(mesh.devices.reshape(4, 4, 4, 2), EVERY)
    placed = (
        P(SEQ, FEAT),
        P(SEQ, FEAT),
        P(),
        P(),
        P(None, FEAT),
        P(None, FEAT),
        P(None, FEAT),
        P(FEAT, None),
    )
    return jax.shard_map(
        on_device, mesh=split, in_specs=placed, out_specs=P(SEQ, FEAT), check_vma=False
    )
```

```python
import functools
import math

import jax
import jax.numpy as jnp
from jax import lax
from jax.experimental import pallas as pl
from jax.experimental.pallas import tpu as pltpu
from jax.sharding import Mesh
from jax.sharding import PartitionSpec as P


D = 5120
HEADS = 40
KV_HEADS = 8
HEAD_DIM = 128
GROUP = HEADS // KV_HEADS
ITERS = 4
TOKENS = 2048
SEQ = ("x", "z")
FEAT = ("y", "c")
EVERY = ("x", "z", "y", "c")
EPS = 1e-06
LAMBDA = 0.03
SCORE_SCALE = 1.0 / math.sqrt(HEAD_DIM)
F32 = jnp.float32
BF16 = jnp.bfloat16

VMEM = pl.BlockSpec(memory_space=pltpu.VMEM)
HBM = pl.BlockSpec(memory_space=pltpu.HBM)


def shift(n, by):
    return [(at, (at + by) % n) for at in range(n)]


def call(kernel, out_shape, *args, specs=None, outs=None, scratch=(), vmem=8, flops=0, touched=0):
    return pl.pallas_call(
        kernel,
        out_shape=out_shape,
        in_specs=[VMEM] * len(args) if specs is None else specs,
        out_specs=jax.tree.map(lambda _: VMEM, out_shape) if outs is None else outs,
        scratch_shapes=list(scratch),
        compiler_params=pltpu.CompilerParams(vmem_limit_bytes=vmem * 1024 * 1024),
        cost_estimate=pl.CostEstimate(flops=flops, bytes_accessed=touched, transcendentals=0),
    )(*args)


def total(x):
    return jnp.sum(jnp.sum(x, axis=1, keepdims=True), axis=0, keepdims=True)


def row_offset(row):
    y, c = lax.axis_index("y"), lax.axis_index("c")
    half, block, inner = row // 64, (row // 16) % 4, row % 16
    return (((y - block + 4) % 4) * 2 + (c + half) % 2) * 16 + inner


def project_keys(rows_ref, squares, wk_ref, wv_ref, held, kv_held, sem, scale_ref, kv_ref):
    scale = lax.rsqrt(squares / D + EPS)
    scale_ref[...] = jnp.broadcast_to(scale, (128, 128))
    pltpu.make_async_copy(wk_ref, held.at[:, :HEAD_DIM], sem.at[0]).wait()
    pltpu.make_async_copy(wv_ref, held.at[:, HEAD_DIM:], sem.at[1]).wait()
    kv = jnp.dot(rows_ref[...], held[...], preferred_element_type=F32)
    kv = (kv * scale).astype(BF16)
    kv_held[...] = jnp.broadcast_to(kv.reshape(1, 128, 2 * HEAD_DIM), (16, 128, 2 * HEAD_DIM))
    store = pltpu.make_async_copy(kv_held, kv_ref, sem.at[0])
    store.start()
    store.wait()


def load_keys(wk_ref, wv_ref, held, sem):
    pltpu.make_async_copy(wk_ref, held.at[:, :HEAD_DIM], sem.at[0]).start()
    pltpu.make_async_copy(wv_ref, held.at[:, HEAD_DIM:], sem.at[1]).start()


def first_kernel(mine_ref, other_ref, gain_ref, wk_ref, wv_ref, rows_ref, scale_ref, kv_ref, held, kv_held, sem):
    load_keys(wk_ref, wv_ref, held, sem)
    y, c = lax.axis_index("y"), lax.axis_index("c")
    for half, pieces in enumerate((mine_ref, other_ref)):
        for block in range(4):
            column = (((y - block + 4) % 4) * 2 + (c + half) % 2) * 640
            columns = pl.ds(pl.multiple_of(column, 640), 640)
            for at in range(8):
                source = pl.multiple_of(row_offset(16 * at), 16)
                rows_ref[16 * at : 16 * at + 16, columns] = pieces[block, pl.ds(source, 16), :]
    squares = jnp.zeros((128, 1), F32)
    for at in range(0, D, 640):
        part = rows_ref[:, at : at + 640].astype(F32) / gain_ref[:, at : at + 640]
        squares = squares + jnp.sum(part * part, axis=1, keepdims=True)
    project_keys(rows_ref, squares, wk_ref, wv_ref, held, kv_held, sem, scale_ref, kv_ref)


def project_kernel(k, *refs):
    (wk_ref, wv_ref), refs = refs[:2], refs[2:]
    held, kv_held, sem = refs[-3:]
    load_keys(wk_ref, wv_ref, held, sem)
    rows_ref, scale_ref, kv_ref = refs[-6:-3]
    shares = mix_shares(k, refs[:k])
    parts, gain_ref = refs[k : 3 * k + 2], refs[3 * k + 2]
    squares = []
    for half in range(2):
        square = jnp.zeros((64, 1), F32)
        for at in range(0, D, 640):
            part = functools.reduce(
                lambda a, b: a + b,
                [
                    share * p[:, at : at + 640].astype(F32)
                    for share, p in zip(shares, parts[half::2])
                ],
            )
            rows_ref[64 * half : 64 * half + 64, at : at + 640] = part.astype(BF16)
            part = part / gain_ref[:, at : at + 640]
            square = square + jnp.sum(part * part, axis=1, keepdims=True)
        squares.append(square)
    squares = jnp.concatenate(squares, axis=0)
    project_keys(rows_ref, squares, wk_ref, wv_ref, held, kv_held, sem, scale_ref, kv_ref)


def attend_kernel(q_ref, scale_ref, kv_ref, w_ref, own_ref, send_ref, w_held, out_held, sem):
    load = pltpu.make_async_copy(w_ref, w_held, sem)
    load.start()
    s = lax.axis_index("x") * 4 + lax.axis_index("z")
    q_off = row_offset(lax.broadcasted_iota(jnp.int32, (128, 1), 0))
    column = lax.broadcasted_iota(jnp.int32, (1, TOKENS), 1)
    key_pos = (column // 128) * 128 + row_offset(column % 128)
    allowed = (s * 128 + q_off) >= key_pos
    scale = scale_ref[:, :1] * SCORE_SCALE

    def one_head(g, carry):
        at = pl.ds(pl.multiple_of(g * HEAD_DIM, HEAD_DIM), HEAD_DIM)
        keys = kv_ref[:, :, :HEAD_DIM].reshape(TOKENS, HEAD_DIM)
        values = kv_ref[:, :, HEAD_DIM:].reshape(TOKENS, HEAD_DIM)
        scores = lax.dot_general(
            q_ref[:, at], keys, (((1,), (1,)), ((), ())), preferred_element_type=F32
        )
        scores = jnp.where(allowed, scores * scale, -1e30)
        weights = jnp.exp(scores - jnp.max(scores, axis=1, keepdims=True))
        weights = jnp.where(allowed, weights, 0.0)
        row_sum = jnp.sum(weights, axis=1, keepdims=True)
        summed = jnp.dot(weights.astype(BF16), values, preferred_element_type=F32)
        out_held[:, at] = (summed / row_sum).astype(BF16)
        return carry

    lax.fori_loop(0, GROUP, one_head, 0)
    load.wait()

    def one_part(n, carry):
        at = pl.ds(pl.multiple_of(n * 1280, 1280), 1280)
        part = jnp.dot(out_held[...], w_held[:, at], preferred_element_type=F32)
        own_ref[:, at] = part[:64]
        send_ref[:, at] = part[64:].astype(BF16)
        return carry

    lax.fori_loop(0, 4, one_part, 0)


def finish_kernel(k, own_ref, a_ref, b_ref, d_ref, inj_ref, x_ref, gain_ref, gain_in_ref, *rest):
    older = rest[:k]
    image_ref, residual_ref = rest[k : k + 2]
    home_refs = rest[k + 2 : k + 6]
    inj, x = inj_ref[...].astype(F32), x_ref[...].astype(F32)
    summed = (x + inj) + (
        own_ref[...] + a_ref[...].astype(F32) + b_ref[...].astype(F32) + d_ref[...].astype(F32)
    )
    scale = lax.rsqrt(jnp.sum(summed * summed, axis=1, keepdims=True) / D + EPS)
    image = summed * scale * gain_ref[...]
    residual = image - x
    image_ref[...] = image
    residual_ref[...] = residual
    y, c = lax.axis_index("y"), lax.axis_index("c")
    for by in range(4):
        for half in range(2):
            column = (((y + by) % 4) * 2 + (c + half) % 2) * 640
            columns = pl.ds(pl.multiple_of(column, 640), 640)
            home_refs[by][half] = image_ref[:, columns]
    if k < ITERS - 1:
        rest[k + 6][...] = ((image + inj) * gain_in_ref[...]).astype(BF16)
    if k > 0:
        lane = lax.broadcasted_iota(jnp.int32, (1, 128), 1)
        dots = jnp.where(lane == k, total(residual * residual), 0.0)
        for at, other in enumerate(older):
            dots = dots + jnp.where(lane == at, total(residual * other[...]), 0.0)
        if k == 1:
            dots = dots + jnp.where(lane == 7, total(older[0][...] * older[0][...]), 0.0)
        rest[-1][...] = jnp.broadcast_to(dots.reshape(1, 1, 128), (128, 1, 128))


def solve_small(matrix, size_now):
    rows = [list(row) for row in matrix]
    values = [jnp.ones((1, 1), F32) for _ in range(size_now)]
    for pivot in range(size_now):
        for below in range(pivot + 1, size_now):
            ratio = rows[below][pivot] / rows[pivot][pivot]
            rows[below] = [b - ratio * p for b, p in zip(rows[below], rows[pivot])]
            values[below] = values[below] - ratio * values[pivot]
    result = [None] * size_now
    for pivot in reversed(range(size_now)):
        running = values[pivot]
        for later in range(pivot + 1, size_now):
            running = running - rows[pivot][later] * result[later]
        result[pivot] = running / rows[pivot][pivot]
    return result


def mix_shares(k, tables):
    if k == 0:
        return [1.0]
    lane = lax.broadcasted_iota(jnp.int32, (1, 128), 1)
    gram = {}
    for at, table in enumerate(tables):
        sums = jnp.sum(table[:, 0, :], axis=0, keepdims=True)
        for other in range(at + 2):
            gram[at + 1, other] = jnp.sum(jnp.where(lane == other, sums, 0.0), axis=1, keepdims=True)
        if at == 0:
            gram[0, 0] = jnp.sum(jnp.where(lane == 7, sums, 0.0), axis=1, keepdims=True)
    system = [
        [
            gram[max(i, j), min(i, j)] / float(TOKENS * D) + (LAMBDA if i == j else 0.0)
            for j in range(k + 1)
        ]
        for i in range(k + 1)
    ]
    unscaled = solve_small(system, k + 1)
    whole = functools.reduce(lambda a, b: a + b, unscaled)
    return [u / whole for u in unscaled]


def mix_kernel(k, *refs):
    shares = mix_shares(k, refs[:k])
    refs[-1][...] = functools.reduce(
        lambda a, b: a + b, [share * image[...] for share, image in zip(shares, refs[k:-1])]
    )


def last_kernel(k, *refs):
    shares = mix_shares(k, refs[:k])
    out_ref, refs = refs[-1], refs[k:-1]
    y, c = lax.axis_index("y"), lax.axis_index("c")
    for by in range(4):
        for half in range(2):
            row = (((y - by + 4) % 4) * 2 + (c + half) % 2) * 16
            rows = pl.ds(pl.multiple_of(row, 16), 16)
            pieces = [refs[5 * at + by][0] if half == 0 else refs[5 * at + 4][by] for at in range(k + 1)]
            out_ref[rows, :] = functools.reduce(
                lambda a, b: a + b, [share * piece for share, piece in zip(shares, pieces)]
            )


def start_kernel(inj_ref, warm_ref, gain_ref, payload_ref, *home_refs):
    inj, warm = inj_ref[...].astype(F32), warm_ref[...].astype(F32)
    payload_ref[...] = ((inj + warm) * gain_ref[...]).astype(BF16)
    y, c = lax.axis_index("y"), lax.axis_index("c")
    for by in range(4):
        for half in range(2):
            row = (((y + by) % 4) * 2 + (c + half) % 2) * 16
            rows = pl.ds(pl.multiple_of(row, 16), 16)
            home_refs[by][half, 0] = inj_ref[rows, :]
            home_refs[by][half, 1] = warm_ref[rows, :]


def settle_kernel(*refs):
    inj_ref, warm_ref = refs[5:]
    y, c = lax.axis_index("y"), lax.axis_index("c")
    for by in range(4):
        for half in range(2):
            column = (((y - by + 4) % 4) * 2 + (c + half) % 2) * 640
            columns = pl.ds(pl.multiple_of(column, 640), 640)
            piece = refs[by][0] if half == 0 else refs[4][by]
            inj_ref[:, columns] = piece[0]
            warm_ref[:, columns] = piece[1]


def move_home(pieces):
    near = [pieces[0]] + [lax.ppermute(pieces[by], "y", shift(4, by)) for by in (1, 2, 3)]
    joined = jnp.stack([piece[1] for piece in near])
    return [*near, lax.ppermute(joined, "c", shift(2, 1))]


def on_device(injection, warm_start, gain_in, gain_out, w_query, w_key, w_value, w_out):
    gain_here = lax.dynamic_slice_in_dim(gain_in, lax.axis_index(FEAT) * 640, 640)
    gain_in, gain_out = gain_in.reshape(1, D), gain_out.reshape(1, D)
    tokens = jax.ShapeDtypeStruct((16, D), F32)
    narrow = jax.ShapeDtypeStruct((16, D), BF16)
    home_narrow = jax.ShapeDtypeStruct((2, 2, 16, 640), BF16)
    home_wide = jax.ShapeDtypeStruct((2, 16, 640), F32)
    payload, *home = call(
        start_kernel,
        (jax.ShapeDtypeStruct((128, 640), BF16), *[home_narrow] * 4),
        injection,
        warm_start,
        gain_here.reshape(1, 640),
    )
    settled = []
    images, residuals, parts, tables, dots = [], [], [], [], None
    projected = (
        jax.ShapeDtypeStruct((128, D), BF16),
        jax.ShapeDtypeStruct((128, 128), F32),
        jax.ShapeDtypeStruct((16, 128, 2 * HEAD_DIM), BF16),
    )
    project_scratch = [
        pltpu.VMEM((D, 2 * HEAD_DIM), BF16),
        pltpu.VMEM((16, 128, 2 * HEAD_DIM), BF16),
        pltpu.SemaphoreType.DMA((2,)),
    ]
    for k in range(ITERS):
        pieces = [payload] + [lax.ppermute(payload, "y", shift(4, by)) for by in (1, 2, 3)]
        if dots is not None:
            tables.append(lax.all_to_all(dots, EVERY, split_axis=0, concat_axis=0, tiled=True))
        mine = jnp.stack(pieces) if k == 0 else jnp.concatenate(pieces, axis=0)
        other = lax.ppermute(mine, "c", shift(2, 1))
        if k == 0:
            rows, scale, kv = call(
                first_kernel,
                projected,
                mine,
                other,
                gain_in,
                w_key,
                w_value,
                specs=[VMEM] * 3 + [HBM] * 2,
                outs=(VMEM, VMEM, HBM),
                vmem=14,
                scratch=project_scratch,
                flops=2 * 128 * D * 256,
                touched=4_000_000,
            )
        else:
            parts += [mine, other]
            rows, scale, kv = call(
                functools.partial(project_kernel, k - 1),
                projected,
                w_key,
                w_value,
                *tables,
                *parts,
                gain_in,
                specs=[HBM] * 2 + [VMEM] * (len(tables) + len(parts) + 1),
                outs=(VMEM, VMEM, HBM),
                vmem=18,
                scratch=project_scratch,
                flops=2 * 128 * D * 256,
                touched=4_000_000,
            )
        kv_all = lax.all_to_all(kv, SEQ, split_axis=0, concat_axis=0, tiled=True)
        q = jnp.dot(rows, w_query, preferred_element_type=F32).astype(BF16)
        home = move_home(home)
        kv_all, home = lax.optimization_barrier((kv_all, home))
        if k == 0:
            inj, current = call(settle_kernel, (narrow, narrow), *home)
        else:
            settled += home
        if k > 1:
            current = call(functools.partial(mix_kernel, k - 1), tokens, *tables, *images)
        own, send = call(
            attend_kernel,
            (jax.ShapeDtypeStruct((64, D), F32), jax.ShapeDtypeStruct((64, D), BF16)),
            q,
            scale,
            kv_all,
            w_out,
            specs=[VMEM, VMEM, VMEM, HBM],
            vmem=24,
            scratch=[
                pltpu.VMEM((640, D), BF16),
                pltpu.VMEM((128, 640), BF16),
                pltpu.SemaphoreType.DMA,
            ],
            flops=2 * 128 * 640 * (2 * TOKENS + D),
            touched=9_000_000,
        )
        pair = own + lax.ppermute(send, "c", shift(2, 1)).astype(F32)
        arrived = [
            lax.ppermute(pair[16 * by : 16 * by + 16].astype(BF16), "y", shift(4, -by))
            for by in (1, 2, 3)
        ]
        shapes = [tokens, tokens, *[home_wide] * 4]
        if k < ITERS - 1:
            shapes.append(narrow)
        if k > 0:
            shapes.append(jax.ShapeDtypeStruct((128, 1, 128), F32))
        outs = call(
            functools.partial(finish_kernel, k),
            tuple(shapes),
            pair[:16],
            *arrived,
            inj,
            current,
            gain_out,
            gain_in,
            *residuals,
        )
        images.append(outs[0])
        residuals.append(outs[1])
        home = outs[2:6]
        payload = outs[6]
        if k == 0:
            current = outs[0]
        else:
            dots = outs[-1]
    settled += move_home(home)
    tables.append(lax.all_to_all(dots, EVERY, split_axis=0, concat_axis=0, tiled=True))
    return call(
        functools.partial(last_kernel, ITERS - 1),
        jax.ShapeDtypeStruct((128, 640), F32),
        *tables,
        *settled,
    )


def solution(mesh):
    split = Mesh(mesh.devices.reshape(4, 4, 4, 2), EVERY)
    placed = (
        P(SEQ, FEAT),
        P(SEQ, FEAT),
        P(),
        P(),
        P(None, FEAT),
        P(None, FEAT),
        P(None, FEAT),
        P(FEAT, None),
    )
    return jax.shard_map(
        on_device, mesh=split, in_specs=placed, out_specs=P(SEQ, FEAT), check_vma=False
    )
```

```python
import functools
import math

import jax
import jax.numpy as jnp
from jax import lax
from jax.experimental import pallas as pl
from jax.experimental.pallas import tpu as pltpu
from jax.sharding import Mesh
from jax.sharding import PartitionSpec as P


D = 5120
HEADS = 40
KV_HEADS = 8
HEAD_DIM = 128
GROUP = HEADS // KV_HEADS
ITERS = 4
TOKENS = 2048
SEQ = ("x", "z")
FEAT = ("y", "c")
EVERY = ("x", "z", "y", "c")
EPS = 1e-06
LAMBDA = 0.03
SCORE_SCALE = 1.0 / math.sqrt(HEAD_DIM)
F32 = jnp.float32
BF16 = jnp.bfloat16

VMEM = pl.BlockSpec(memory_space=pltpu.VMEM)
HBM = pl.BlockSpec(memory_space=pltpu.HBM)


def shift(n, by):
    return [(at, (at + by) % n) for at in range(n)]


def call(kernel, outs, *args, specs=None, scratch=(), vmem=8, flops=0, touched=0):
    return pl.pallas_call(
        kernel,
        out_shape=outs,
        in_specs=[VMEM] * len(args) if specs is None else specs,
        out_specs=jax.tree.map(lambda out: HBM if out.memory_space == pltpu.HBM else VMEM, outs),
        scratch_shapes=list(scratch),
        compiler_params=pltpu.CompilerParams(vmem_limit_bytes=vmem * 1024 * 1024),
        cost_estimate=pl.CostEstimate(flops=flops, bytes_accessed=touched, transcendentals=0),
    )(*args)


def total(x):
    return jnp.sum(jnp.sum(x, axis=1, keepdims=True), axis=0, keepdims=True)


def row_offset(row):
    y, c = lax.axis_index("y"), lax.axis_index("c")
    half, block, inner = row // 64, (row // 16) % 4, row % 16
    return (((y - block + 4) % 4) * 2 + (c + half) % 2) * 16 + inner


def project_keys(squares, wk_ref, wv_ref, rows_out, scale_ref, kv_ref, rows_ref, held, kv_held, sem):
    keep = pltpu.make_async_copy(rows_ref, rows_out, sem.at[2])
    keep.start()
    scale = lax.rsqrt(squares / D + EPS)
    scale_ref[...] = jnp.broadcast_to(scale, (128, 128))
    pltpu.make_async_copy(wk_ref, held.at[:, :HEAD_DIM], sem.at[0]).wait()
    pltpu.make_async_copy(wv_ref, held.at[:, HEAD_DIM:], sem.at[1]).wait()
    kv = jnp.dot(rows_ref[...], held[...], preferred_element_type=F32)
    kv = (kv * scale).astype(BF16)
    kv_held[...] = jnp.broadcast_to(kv.reshape(1, 128, 2 * HEAD_DIM), (16, 128, 2 * HEAD_DIM))
    store = pltpu.make_async_copy(kv_held, kv_ref, sem.at[0])
    store.start()
    store.wait()
    keep.wait()


def load_keys(wk_ref, wv_ref, held, sem):
    pltpu.make_async_copy(wk_ref, held.at[:, :HEAD_DIM], sem.at[0]).start()
    pltpu.make_async_copy(wv_ref, held.at[:, HEAD_DIM:], sem.at[1]).start()


def first_kernel(wk_ref, wv_ref, gain_ref, *refs):
    pieces, (rows_out, scale_ref, kv_ref, rows_ref, held, kv_held, sem) = refs[:8], refs[8:]
    load_keys(wk_ref, wv_ref, held, sem)
    y, c = lax.axis_index("y"), lax.axis_index("c")
    for half in range(2):
        for block in range(4):
            column = (((y - block + 4) % 4) * 2 + (c + half) % 2) * 640
            columns = pl.ds(pl.multiple_of(column, 640), 640)
            for at in range(8):
                source = pl.multiple_of(row_offset(16 * at), 16)
                rows_ref[16 * at : 16 * at + 16, columns] = pieces[4 * half + block][pl.ds(source, 16), :]
    squares = jnp.zeros((128, 1), F32)
    for at in range(0, D, 640):
        part = rows_ref[:, at : at + 640].astype(F32) * (1.0 / gain_ref[:, at : at + 640])
        squares = squares + jnp.sum(part * part, axis=1, keepdims=True)
    project_keys(
        squares, wk_ref, wv_ref, rows_out, scale_ref, kv_ref, rows_ref, held, kv_held, sem
    )


def project_kernel(k, keep, *refs):
    (wk_ref, wv_ref, gain_ref), refs = refs[:3], refs[3:]
    tables, older_hbm, pieces = refs[:k], refs[k : 2 * k], refs[2 * k : 2 * k + 8]
    rows_out, scale_ref, kv_ref, *kept = refs[2 * k + 8 : 2 * k + 11 + keep]
    rows_ref, held, kv_held, sem, newest_ref, older_ref, older_sem = refs[2 * k + 11 + keep :]
    for n in range(8):
        for at in range(k):
            columns = slice(640 * n, 640 * n + 640)
            pltpu.make_async_copy(
                older_hbm[at].at[:, columns], older_ref.at[at, :, columns], older_sem.at[at, n]
            ).start()
    load_keys(wk_ref, wv_ref, held, sem)
    shares = mix_shares(k, tables)

    def one_part(n, squares):
        at = pl.ds(pl.multiple_of(n * 640, 640), 640)
        newest = jnp.concatenate([piece[:, at] for piece in pieces], axis=0)
        if keep:
            newest_ref[:, at] = newest
        part = newest.astype(F32)
        if k > 0:
            part = shares[k] * part
            for old in range(k):
                pltpu.make_async_copy(
                    older_hbm[old].at[:, at], older_ref.at[old, :, at], older_sem.at[old, n]
                ).wait()
                part = part + shares[old] * older_ref[old, :, at].astype(F32)
            rows_ref[:, at] = part.astype(BF16)
        else:
            rows_ref[:, at] = newest
        part = part * (1.0 / gain_ref[:, at])
        return squares + jnp.sum(part * part, axis=1, keepdims=True)

    squares = lax.fori_loop(0, 8, one_part, jnp.zeros((128, 1), F32))
    if keep:
        save = pltpu.make_async_copy(newest_ref, kept[0], sem.at[3])
        save.start()
    project_keys(
        squares, wk_ref, wv_ref, rows_out, scale_ref, kv_ref, rows_ref, held, kv_held, sem
    )
    if keep:
        save.wait()


def query_kernel(rows_ref, w_ref, q_ref, acc):
    @pl.when(pl.program_id(0) == 0)
    def _():
        acc[...] = jnp.zeros_like(acc)

    acc[...] += jnp.dot(rows_ref[...], w_ref[...], preferred_element_type=F32)

    @pl.when(pl.program_id(0) == 4)
    def _():
        q_ref[...] = acc[...].astype(BF16)


def query_dot(rows, w_query):
    return pl.pallas_call(
        query_kernel,
        grid=(5,),
        out_shape=pltpu.VMEM((128, 640), BF16),
        in_specs=[
            pl.BlockSpec((128, 1024), lambda n: (0, n)),
            pl.BlockSpec((1024, 640), lambda n: (n, 0)),
        ],
        out_specs=pl.BlockSpec((128, 640), lambda n: (0, 0)),
        scratch_shapes=[pltpu.VMEM((128, 640), F32)],
        compiler_params=pltpu.CompilerParams(vmem_limit_bytes=8 * 1024 * 1024),
        cost_estimate=pl.CostEstimate(
            flops=2 * 128 * D * 640, bytes_accessed=8_000_000, transcendentals=0
        ),
    )(rows, w_query)


def attend_kernel(q_ref, scale_ref, kv_ref, w_ref, own_ref, send_ref, w_held, out_held, sem):
    load = pltpu.make_async_copy(w_ref, w_held, sem)
    load.start()
    s = lax.axis_index("x") * 4 + lax.axis_index("z")
    q_off = row_offset(lax.broadcasted_iota(jnp.int32, (128, 1), 0))
    column = lax.broadcasted_iota(jnp.int32, (1, TOKENS), 1)
    key_pos = (column // 128) * 128 + row_offset(column % 128)
    allowed = (s * 128 + q_off) >= key_pos
    scale = scale_ref[:, :1] * SCORE_SCALE

    def one_head(g, carry):
        at = pl.ds(pl.multiple_of(g * HEAD_DIM, HEAD_DIM), HEAD_DIM)
        keys = kv_ref[:, :, :HEAD_DIM].reshape(TOKENS, HEAD_DIM)
        values = kv_ref[:, :, HEAD_DIM:].reshape(TOKENS, HEAD_DIM)
        scores = lax.dot_general(
            q_ref[:, at], keys, (((1,), (1,)), ((), ())), preferred_element_type=F32
        )
        scores = jnp.where(allowed, scores * scale, -1e30)
        weights = jnp.exp(scores - jnp.max(scores, axis=1, keepdims=True))
        weights = jnp.where(allowed, weights, 0.0)
        row_sum = jnp.sum(weights, axis=1, keepdims=True)
        summed = jnp.dot(weights.astype(BF16), values, preferred_element_type=F32)
        out_held[:, at] = (summed / row_sum).astype(BF16)
        return carry

    lax.fori_loop(0, GROUP, one_head, 0)
    load.wait()

    def one_part(n, carry):
        at = pl.ds(pl.multiple_of(n * 1280, 1280), 1280)
        part = jnp.dot(out_held[...], w_held[:, at], preferred_element_type=F32)
        own_ref[:, at] = part[:64]
        send_ref[:, at] = part[64:].astype(BF16)
        return carry

    lax.fori_loop(0, 4, one_part, 0)


def finish_kernel(k, own_ref, a_ref, b_ref, d_ref, inj_ref, x_ref, gain_ref, gain_in_ref, *rest):
    older, rest = rest[:k], rest[k:]
    image_held, residual_held, dots_held, sem = rest[-4:]
    image_out, residual_out, *home_out = rest[:6]
    inj, x = inj_ref[...].astype(F32), x_ref[...].astype(F32)
    summed = (x + inj) + (
        own_ref[...] + a_ref[...].astype(F32) + b_ref[...].astype(F32) + d_ref[...].astype(F32)
    )
    scale = lax.rsqrt(jnp.sum(summed * summed, axis=1, keepdims=True) / D + EPS)
    image = summed * scale * gain_ref[...]
    residual = image - x
    image_held[...] = image
    residual_held[...] = residual
    copies = [
        pltpu.make_async_copy(image_held, image_out, sem.at[0]),
        pltpu.make_async_copy(residual_held, residual_out, sem.at[1]),
    ]
    y, c = lax.axis_index("y"), lax.axis_index("c")
    for by in range(4):
        for half in range(2):
            column = (((y + by) % 4) * 2 + (c + half) % 2) * 640
            columns = pl.ds(pl.multiple_of(column, 640), 640)
            copies.append(
                pltpu.make_async_copy(
                    image_held.at[:, columns], home_out[by].at[half], sem.at[2 + 2 * by + half]
                )
            )
    for copy in copies:
        copy.start()
    if k < ITERS - 1:
        rest[6][...] = ((image + inj) * gain_in_ref[...]).astype(BF16)
    if k > 0:
        lane = lax.broadcasted_iota(jnp.int32, (1, 128), 1)
        dots = jnp.where(lane == k, total(residual * residual), 0.0)
        for at, other in enumerate(older):
            dots = dots + jnp.where(lane == at, total(residual * other[...]), 0.0)
        if k == 1:
            dots = dots + jnp.where(lane == 7, total(older[0][...] * older[0][...]), 0.0)
        dots_held[...] = jnp.broadcast_to(dots.reshape(1, 1, 128), (128, 1, 128))
        table_out = rest[7] if k < ITERS - 1 else rest[6]
        copies.append(pltpu.make_async_copy(dots_held, table_out, sem.at[10]))
        copies[-1].start()
    for copy in copies:
        copy.wait()


def solve_small(matrix, size_now):
    rows = [list(row) for row in matrix]
    values = [jnp.ones((1, 1), F32) for _ in range(size_now)]
    for pivot in range(size_now):
        for below in range(pivot + 1, size_now):
            ratio = rows[below][pivot] / rows[pivot][pivot]
            rows[below] = [b - ratio * p for b, p in zip(rows[below], rows[pivot])]
            values[below] = values[below] - ratio * values[pivot]
    result = [None] * size_now
    for pivot in reversed(range(size_now)):
        running = values[pivot]
        for later in range(pivot + 1, size_now):
            running = running - rows[pivot][later] * result[later]
        result[pivot] = running / rows[pivot][pivot]
    return result


def mix_shares(k, tables):
    if k == 0:
        return [1.0]
    lane = lax.broadcasted_iota(jnp.int32, (1, 128), 1)
    gram = {}
    for at, table in enumerate(tables):
        sums = jnp.sum(table[:, 0, :], axis=0, keepdims=True)
        for other in range(at + 2):
            gram[at + 1, other] = jnp.sum(jnp.where(lane == other, sums, 0.0), axis=1, keepdims=True)
        if at == 0:
            gram[0, 0] = jnp.sum(jnp.where(lane == 7, sums, 0.0), axis=1, keepdims=True)
    system = [
        [
            gram[max(i, j), min(i, j)] / float(TOKENS * D) + (LAMBDA if i == j else 0.0)
            for j in range(k + 1)
        ]
        for i in range(k + 1)
    ]
    unscaled = solve_small(system, k + 1)
    whole = functools.reduce(lambda a, b: a + b, unscaled)
    return [u / whole for u in unscaled]


def mix_kernel(k, *refs):
    shares = mix_shares(k, refs[:k])
    refs[-1][...] = functools.reduce(
        lambda a, b: a + b, [share * image[...] for share, image in zip(shares, refs[k:-1])]
    )


def last_kernel(k, *refs):
    shares = mix_shares(k, refs[:k])
    out_ref, refs = refs[-1], refs[k:-1]
    y, c = lax.axis_index("y"), lax.axis_index("c")
    for by in range(4):
        for half in range(2):
            row = (((y - by + 4) % 4) * 2 + (c + half) % 2) * 16
            rows = pl.ds(pl.multiple_of(row, 16), 16)
            pieces = [refs[5 * at + by][0] if half == 0 else refs[5 * at + 4][by] for at in range(k + 1)]
            out_ref[rows, :] = functools.reduce(
                lambda a, b: a + b, [share * piece for share, piece in zip(shares, pieces)]
            )


def start_kernel(inj_ref, warm_ref, gain_ref, payload_ref, *home_refs):
    inj, warm = inj_ref[...].astype(F32), warm_ref[...].astype(F32)
    payload_ref[...] = ((inj + warm) * gain_ref[...]).astype(BF16)
    y, c = lax.axis_index("y"), lax.axis_index("c")
    for by in range(4):
        for half in range(2):
            row = (((y + by) % 4) * 2 + (c + half) % 2) * 16
            rows = pl.ds(pl.multiple_of(row, 16), 16)
            home_refs[by][half, 0] = inj_ref[rows, :]
            home_refs[by][half, 1] = warm_ref[rows, :]


def settle_kernel(*refs):
    inj_ref, warm_ref = refs[5:]
    y, c = lax.axis_index("y"), lax.axis_index("c")
    for by in range(4):
        for half in range(2):
            column = (((y - by + 4) % 4) * 2 + (c + half) % 2) * 640
            columns = pl.ds(pl.multiple_of(column, 640), 640)
            piece = refs[by][0] if half == 0 else refs[4][by]
            inj_ref[:, columns] = piece[0]
            warm_ref[:, columns] = piece[1]


def move_home(pieces):
    near = [pieces[0]] + [lax.ppermute(pieces[by], "y", shift(4, by)) for by in (1, 2, 3)]
    joined = jnp.stack([piece[1] for piece in near])
    return [*near, lax.ppermute(joined, "c", shift(2, 1))]


def on_device(injection, warm_start, gain_in, gain_out, w_query, w_key, w_value, w_out):
    gain_here = lax.dynamic_slice_in_dim(gain_in, lax.axis_index(FEAT) * 640, 640)
    gain_in, gain_out = gain_in.reshape(1, D), gain_out.reshape(1, D)
    w_key, w_value, w_query, w_out = (
        pltpu.with_memory_space_constraint(w, pltpu.HBM) for w in (w_key, w_value, w_query, w_out)
    )
    tokens = pltpu.HBM((16, D), F32)
    wide = pltpu.VMEM((16, D), F32)
    narrow = pltpu.VMEM((16, D), BF16)
    home_narrow = pltpu.VMEM((2, 2, 16, 640), BF16)
    home_wide = pltpu.HBM((2, 16, 640), F32)
    payload, *home = call(
        start_kernel,
        (pltpu.VMEM((128, 640), BF16), *[home_narrow] * 4),
        injection,
        warm_start,
        gain_here.reshape(1, 640),
    )
    settled = []
    images, residuals, parts, tables, dots = [], [], [], [], None
    projected = (
        pltpu.HBM((128, D), BF16),
        pltpu.VMEM((128, 128), F32),
        pltpu.HBM((16, 128, 2 * HEAD_DIM), BF16),
    )
    project_scratch = [
        pltpu.VMEM((128, D), BF16),
        pltpu.VMEM((D, 2 * HEAD_DIM), BF16),
        pltpu.VMEM((16, 128, 2 * HEAD_DIM), BF16),
        pltpu.SemaphoreType.DMA((4,)),
    ]
    for k in range(ITERS):
        pieces = [payload] + [lax.ppermute(payload, "y", shift(4, by)) for by in (1, 2, 3)]
        if dots is not None:
            tables.append(lax.all_to_all(dots, EVERY, split_axis=0, concat_axis=0, tiled=True))
        pieces += [lax.ppermute(piece, "c", shift(2, 1)) for piece in pieces]
        if k == 0:
            rows, scale, kv = call(
                first_kernel,
                projected,
                w_key,
                w_value,
                gain_in,
                *pieces,
                specs=[HBM] * 2 + [VMEM] * 9,
                vmem=10,
                scratch=project_scratch,
                flops=2 * 128 * D * 256,
                touched=4_000_000,
            )
        else:
            keep = k == 2
            rows, scale, kv, *kept = call(
                functools.partial(project_kernel, k - 1, keep),
                projected + ((pltpu.HBM((128, D), BF16),) if keep else ()),
                w_key,
                w_value,
                gain_in,
                *tables,
                *parts,
                *pieces,
                specs=[HBM] * 2 + [VMEM] * (1 + len(tables)) + [HBM] * len(parts) + [VMEM] * 8,
                vmem=12,
                scratch=project_scratch
                + [
                    pltpu.VMEM((128, D) if keep else (8, 128), BF16),
                    pltpu.VMEM((k - 1, 128, D) if k > 1 else (1, 8, 128), BF16),
                    pltpu.SemaphoreType.DMA((max(k - 1, 1), 8)),
                ],
                flops=2 * 128 * D * 256,
                touched=4_000_000,
            )
            parts += kept if keep else [rows]
        kv_all = lax.all_to_all(kv, SEQ, split_axis=0, concat_axis=0, tiled=True)
        q = query_dot(rows, w_query)
        home = move_home(home)
        kv_all, home = lax.optimization_barrier((kv_all, home))
        if k == 0:
            inj, current = call(settle_kernel, (narrow, narrow), *home)
        else:
            settled += home
        if k > 1:
            current = call(functools.partial(mix_kernel, k - 1), wide, *tables, *images)
        own, send = call(
            attend_kernel,
            (pltpu.VMEM((64, D), F32), pltpu.VMEM((64, D), BF16)),
            q,
            scale,
            kv_all,
            w_out,
            specs=[VMEM, VMEM, VMEM, HBM],
            vmem=16,
            scratch=[
                pltpu.VMEM((640, D), BF16),
                pltpu.VMEM((128, 640), BF16),
                pltpu.SemaphoreType.DMA,
            ],
            flops=2 * 128 * 640 * (2 * TOKENS + D),
            touched=9_000_000,
        )
        pair = own + lax.ppermute(send, "c", shift(2, 1)).astype(F32)
        arrived = [
            lax.ppermute(pair[16 * by : 16 * by + 16].astype(BF16), "y", shift(4, -by))
            for by in (1, 2, 3)
        ]
        shapes = [tokens, tokens, *[home_wide] * 4]
        if k < ITERS - 1:
            shapes.append(narrow)
        if k > 0:
            shapes.append(pltpu.HBM((128, 1, 128), F32))
        outs = call(
            functools.partial(finish_kernel, k),
            tuple(shapes),
            pair[:16],
            *arrived,
            inj,
            current,
            gain_out,
            gain_in,
            *residuals,
            scratch=[
                pltpu.VMEM((16, D), F32),
                pltpu.VMEM((16, D), F32),
                pltpu.VMEM((128, 1, 128), F32),
                pltpu.SemaphoreType.DMA((11,)),
            ],
        )
        images.append(outs[0])
        residuals.append(outs[1])
        home = outs[2:6]
        payload = outs[6]
        if k == 0:
            current = outs[0]
        else:
            dots = outs[-1]
    settled += move_home(home)
    tables.append(lax.all_to_all(dots, EVERY, split_axis=0, concat_axis=0, tiled=True))
    return call(
        functools.partial(last_kernel, ITERS - 1),
        pltpu.VMEM((128, 640), F32),
        *tables,
        *settled,
    )


def solution(mesh):
    split = Mesh(mesh.devices.reshape(4, 4, 4, 2), EVERY)
    placed = (
        P(SEQ, FEAT),
        P(SEQ, FEAT),
        P(),
        P(),
        P(None, FEAT),
        P(None, FEAT),
        P(None, FEAT),
        P(FEAT, None),
    )
    return jax.shard_map(
        on_device, mesh=split, in_specs=placed, out_specs=P(SEQ, FEAT), check_vma=False
    )
```

```python
import functools
import math

import jax
import jax.numpy as jnp
from jax import lax
from jax.experimental import pallas as pl
from jax.experimental.pallas import tpu as pltpu
from jax.sharding import Mesh
from jax.sharding import PartitionSpec as P


D = 5120
HEADS = 40
KV_HEADS = 8
HEAD_DIM = 128
GROUP = HEADS // KV_HEADS
ITERS = 4
TOKENS = 2048
SEQ = ("x", "z")
FEAT = ("y", "c")
EVERY = ("x", "z", "y", "c")
EPS = 1e-06
LAMBDA = 0.03
SCORE_SCALE = 1.0 / math.sqrt(HEAD_DIM)
F32 = jnp.float32
BF16 = jnp.bfloat16

VMEM = pl.BlockSpec(memory_space=pltpu.VMEM)
HBM = pl.BlockSpec(memory_space=pltpu.HBM)


def shift(n, by):
    return [(at, (at + by) % n) for at in range(n)]


def call(kernel, outs, *args, specs=None, scratch=(), vmem=8, flops=0, touched=0):
    return pl.pallas_call(
        kernel,
        out_shape=outs,
        in_specs=[VMEM] * len(args) if specs is None else specs,
        out_specs=jax.tree.map(lambda out: HBM if out.memory_space == pltpu.HBM else VMEM, outs),
        scratch_shapes=list(scratch),
        compiler_params=pltpu.CompilerParams(vmem_limit_bytes=vmem * 1024 * 1024),
        cost_estimate=pl.CostEstimate(flops=flops, bytes_accessed=touched, transcendentals=0),
    )(*args)


def total(x):
    return jnp.sum(jnp.sum(x, axis=1, keepdims=True), axis=0, keepdims=True)


def row_offset(row):
    y, c = lax.axis_index("y"), lax.axis_index("c")
    half, block, inner = row // 64, (row // 16) % 4, row % 16
    return (((y - block + 4) % 4) * 2 + (c + half) % 2) * 16 + inner


def load_keys(wk_ref, wv_ref, held, sem):
    copies = [
        pltpu.make_async_copy(wk_ref, held.at[:, :HEAD_DIM], sem.at[0]),
        pltpu.make_async_copy(wv_ref, held.at[:, HEAD_DIM:], sem.at[1]),
    ]
    for copy in copies:
        copy.start()
    return copies


def first_kernel(wk_ref, wv_ref, gain_ref, *refs):
    pieces, (rows_out, raw_ref, pairs_ref, rows_ref, held, sem) = refs[:8], refs[8:]
    loads = load_keys(wk_ref, wv_ref, held, sem)
    y, c = lax.axis_index("y"), lax.axis_index("c")
    for half in range(2):
        for block in range(4):
            column = (((y - block + 4) % 4) * 2 + (c + half) % 2) * 640
            columns = pl.ds(pl.multiple_of(column, 640), 640)
            for at in range(8):
                source = pl.multiple_of(row_offset(16 * at), 16)
                rows_ref[16 * at : 16 * at + 16, columns] = pieces[4 * half + block][
                    pl.ds(source, 16), :
                ]
    keep = pltpu.make_async_copy(rows_ref, rows_out, sem.at[2])
    keep.start()

    def one_part(n, squares):
        at = pl.ds(pl.multiple_of(n * 640, 640), 640)
        part = rows_ref[:, at].astype(F32) * (1.0 / gain_ref[:, at])
        return squares + jnp.sum(part * part, axis=1, keepdims=True)

    squares = lax.fori_loop(0, 8, one_part, jnp.zeros((128, 1), F32))
    pairs_ref[...] = jnp.broadcast_to(squares, (128, 128))
    for load in loads:
        load.wait()
    raw_ref[...] = jnp.dot(rows_ref[...], held[...], preferred_element_type=F32)
    keep.wait()


def project_kernel(k, *refs):
    (wk_ref, wv_ref, gain_ref), refs = refs[:3], refs[3:]
    older_hbm, pieces = refs[:k], refs[k : k + 8]
    rows_out, raw_ref, pairs_ref, rows_ref, held, sem, older_ref, older_sem = refs[k + 8 :]
    for n in range(8):
        for at in range(k):
            columns = slice(640 * n, 640 * n + 640)
            pltpu.make_async_copy(
                older_hbm[at].at[:, columns], older_ref.at[at, :, columns], older_sem.at[at, n]
            ).start()
    loads = load_keys(wk_ref, wv_ref, held, sem)

    def one_part(n, sums):
        at = pl.ds(pl.multiple_of(n * 640, 640), 640)
        newest = jnp.concatenate([piece[:, at] for piece in pieces], axis=0)
        rows_ref[:, at] = newest
        newest = newest.astype(F32)
        inverse = 1.0 / gain_ref[:, at]
        weighed = newest * (inverse * inverse)
        sums = list(sums)
        for old in range(k):
            pltpu.make_async_copy(
                older_hbm[old].at[:, at], older_ref.at[old, :, at], older_sem.at[old, n]
            ).wait()
            other = older_ref[old, :, at].astype(F32)
            sums[old] = sums[old] + jnp.sum(weighed * other, axis=1, keepdims=True)
        sums[k] = sums[k] + jnp.sum(weighed * newest, axis=1, keepdims=True)
        return tuple(sums)

    sums = lax.fori_loop(0, 8, one_part, tuple(jnp.zeros((128, 1), F32) for _ in range(k + 1)))
    keep = pltpu.make_async_copy(rows_ref, rows_out, sem.at[2])
    keep.start()
    lane = lax.broadcasted_iota(jnp.int32, (1, 128), 1)
    pairs_ref[...] = functools.reduce(
        lambda a, b: a + b, [jnp.where(lane == at, value, 0.0) for at, value in enumerate(sums)]
    )
    for load in loads:
        load.wait()
    raw_ref[...] = jnp.dot(rows_ref[...], held[...], preferred_element_type=F32)
    keep.wait()


def share_kernel(k, *refs):
    raws, pairs = refs[k : 2 * k + 1], refs[2 * k + 1 : 3 * k + 2]
    share_ref, scale_ref, kv_ref, kv_held, sem = refs[3 * k + 2 :]
    shares = mix_shares(k, refs[:k])
    lane = lax.broadcasted_iota(jnp.int32, (1, 128), 1)
    share_ref[...] = functools.reduce(
        lambda a, b: a + b, [jnp.where(lane == at, share, 0.0) for at, share in enumerate(shares)]
    )
    squares = jnp.zeros((128, 1), F32)
    for at in range(k + 1):
        for other in range(at + 1):
            twice = 1.0 if other == at else 2.0
            squares = squares + (twice * shares[at] * shares[other]) * pairs[at][:, other : other + 1]
    scale = lax.rsqrt(jnp.maximum(squares, 0.0) / D + EPS)
    scale_ref[...] = jnp.broadcast_to(scale, (128, 128))
    kv = functools.reduce(lambda a, b: a + b, [share * raw[...] for share, raw in zip(shares, raws)])
    kv_held[...] = (kv * scale).astype(BF16)
    stores = [pltpu.make_async_copy(kv_held, kv_ref.at[at], sem.at[at]) for at in range(16)]
    for store in stores:
        store.start()
    for store in stores:
        store.wait()


def take_share(share_ref, at):
    lane = lax.broadcasted_iota(jnp.int32, (1, 128), 1)
    return jnp.sum(jnp.where(lane == at, share_ref[...], 0.0), axis=1, keepdims=True)


def query_kernel(k, share_ref, *refs):
    parts, (w_ref, q_ref, acc) = refs[: k + 1], refs[k + 1 :]

    @pl.when(pl.program_id(0) == 0)
    def _():
        acc[...] = jnp.zeros_like(acc)

    if k == 0:
        rows = parts[0][...]
    else:
        rows = functools.reduce(
            lambda a, b: a + b,
            [take_share(share_ref, at) * part[...].astype(F32) for at, part in enumerate(parts)],
        ).astype(BF16)
    acc[...] += jnp.dot(rows, w_ref[...], preferred_element_type=F32)

    @pl.when(pl.program_id(0) == 4)
    def _():
        q_ref[...] = acc[...].astype(BF16)


def query_dot(share, parts, w_query):
    return pl.pallas_call(
        functools.partial(query_kernel, len(parts) - 1),
        grid=(5,),
        out_shape=pltpu.VMEM((128, 640), BF16),
        in_specs=[pl.BlockSpec((1, 128), lambda n: (0, 0))]
        + [pl.BlockSpec((128, 1024), lambda n: (0, n))] * len(parts)
        + [pl.BlockSpec((1024, 640), lambda n: (n, 0))],
        out_specs=pl.BlockSpec((128, 640), lambda n: (0, 0)),
        scratch_shapes=[pltpu.VMEM((128, 640), F32)],
        compiler_params=pltpu.CompilerParams(vmem_limit_bytes=10 * 1024 * 1024),
        cost_estimate=pl.CostEstimate(
            flops=2 * 128 * D * 640, bytes_accessed=8_000_000, transcendentals=0
        ),
    )(share, *[pltpu.with_memory_space_constraint(part, pltpu.HBM) for part in parts], w_query)


def attend_kernel(
    q_ref, scale_ref, kv_ref, w_ref, own_ref, send_ref, w_held, q_held, scores, weights, sums, attended, sem
):
    load = pltpu.make_async_copy(w_ref, w_held, sem)
    load.start()
    s = lax.axis_index("x") * 4 + lax.axis_index("z")
    for g in range(GROUP):
        q_held[128 * g : 128 * g + 128, :] = q_ref[:, HEAD_DIM * g : HEAD_DIM * g + HEAD_DIM]

    def one_block(n, carry):
        keys = kv_ref[pl.ds(2 * n, 2), :, :HEAD_DIM].reshape(256, HEAD_DIM)
        scores[:, pl.ds(pl.multiple_of(n * 256, 256), 256)] = lax.dot_general(
            q_held[...], keys, (((1,), (1,)), ((), ())), preferred_element_type=F32
        )
        return carry

    lax.fori_loop(0, 8, one_block, 0)
    own = pl.ds(pl.multiple_of(s * 128, 128), 128)
    row_at = row_offset(lax.broadcasted_iota(jnp.int32, (128, 1), 0))
    column_at = row_offset(lax.broadcasted_iota(jnp.int32, (1, 128), 1))
    later = lax.broadcasted_iota(jnp.int32, (1, TOKENS), 1) // 128 > s
    bias = jnp.where(later, -1e30, 0.0)
    factor = scale_ref[:, :1] * (SCORE_SCALE / math.log(2.0))

    def one_head(g, carry):
        rows = pl.ds(pl.multiple_of(g * 128, 128), 128)
        scores[rows, own] = jnp.where(row_at >= column_at, scores[rows, own], -1e30)
        raw = scores[rows, :] + bias
        raw = raw - jnp.max(raw, axis=1, keepdims=True)
        weight = jnp.exp2(raw * factor)
        sums[rows, :] = jnp.broadcast_to(jnp.sum(weight, axis=1, keepdims=True), (128, 128))
        weights[rows, :] = weight.astype(BF16)
        return carry

    lax.fori_loop(0, GROUP, one_head, 0)
    values = kv_ref[:, :, HEAD_DIM:].reshape(TOKENS, HEAD_DIM)
    summed = jnp.dot(weights[...], values, preferred_element_type=F32) / sums[...]
    for g in range(GROUP):
        attended[:, HEAD_DIM * g : HEAD_DIM * g + HEAD_DIM] = summed[128 * g : 128 * g + 128].astype(BF16)
    load.wait()

    def one_part(n, carry):
        at = pl.ds(pl.multiple_of(n * 1280, 1280), 1280)
        part = jnp.dot(attended[...], w_held[:, at], preferred_element_type=F32)
        own_ref[:, at] = part[:64]
        send_ref[:, at] = part[64:].astype(BF16)
        return carry

    lax.fori_loop(0, 4, one_part, 0)


def finish_kernel(k, own_ref, a_ref, b_ref, d_ref, inj_ref, x_ref, gain_ref, gain_in_ref, *rest):
    older, rest = rest[:k], rest[k:]
    image_held, residual_held, dots_held, sem = rest[-4:]
    image_out, residual_out, *home_out = rest[:6]
    inj, x = inj_ref[...].astype(F32), x_ref[...].astype(F32)
    summed = (x + inj) + (
        own_ref[...] + a_ref[...].astype(F32) + b_ref[...].astype(F32) + d_ref[...].astype(F32)
    )
    scale = lax.rsqrt(jnp.sum(summed * summed, axis=1, keepdims=True) / D + EPS)
    image = summed * scale * gain_ref[...]
    residual = image - x
    image_held[...] = image
    residual_held[...] = residual
    copies = [
        pltpu.make_async_copy(image_held, image_out, sem.at[0]),
        pltpu.make_async_copy(residual_held, residual_out, sem.at[1]),
    ]
    y, c = lax.axis_index("y"), lax.axis_index("c")
    for by in range(4):
        for half in range(2):
            column = (((y + by) % 4) * 2 + (c + half) % 2) * 640
            columns = pl.ds(pl.multiple_of(column, 640), 640)
            copies.append(
                pltpu.make_async_copy(
                    image_held.at[:, columns], home_out[by].at[half], sem.at[2 + 2 * by + half]
                )
            )
    for copy in copies:
        copy.start()
    if k < ITERS - 1:
        rest[6][...] = ((image + inj) * gain_in_ref[...]).astype(BF16)
    if k > 0:
        lane = lax.broadcasted_iota(jnp.int32, (1, 128), 1)
        dots = jnp.where(lane == k, total(residual * residual), 0.0)
        for at, other in enumerate(older):
            dots = dots + jnp.where(lane == at, total(residual * other[...]), 0.0)
        if k == 1:
            dots = dots + jnp.where(lane == 7, total(older[0][...] * older[0][...]), 0.0)
        dots_held[...] = jnp.broadcast_to(dots.reshape(1, 1, 128), (128, 1, 128))
        table_out = rest[7] if k < ITERS - 1 else rest[6]
        copies.append(pltpu.make_async_copy(dots_held, table_out, sem.at[10]))
        copies[-1].start()
    for copy in copies:
        copy.wait()


def solve_small(matrix, size_now):
    rows = [list(row) for row in matrix]
    values = [jnp.ones((1, 1), F32) for _ in range(size_now)]
    for pivot in range(size_now):
        for below in range(pivot + 1, size_now):
            ratio = rows[below][pivot] / rows[pivot][pivot]
            rows[below] = [b - ratio * p for b, p in zip(rows[below], rows[pivot])]
            values[below] = values[below] - ratio * values[pivot]
    result = [None] * size_now
    for pivot in reversed(range(size_now)):
        running = values[pivot]
        for later in range(pivot + 1, size_now):
            running = running - rows[pivot][later] * result[later]
        result[pivot] = running / rows[pivot][pivot]
    return result


def mix_shares(k, tables):
    if k == 0:
        return [1.0]
    lane = lax.broadcasted_iota(jnp.int32, (1, 128), 1)
    gram = {}
    for at, table in enumerate(tables):
        sums = jnp.sum(table[:, 0, :], axis=0, keepdims=True)
        for other in range(at + 2):
            gram[at + 1, other] = jnp.sum(jnp.where(lane == other, sums, 0.0), axis=1, keepdims=True)
        if at == 0:
            gram[0, 0] = jnp.sum(jnp.where(lane == 7, sums, 0.0), axis=1, keepdims=True)
    system = [
        [
            gram[max(i, j), min(i, j)] / float(TOKENS * D) + (LAMBDA if i == j else 0.0)
            for j in range(k + 1)
        ]
        for i in range(k + 1)
    ]
    unscaled = solve_small(system, k + 1)
    whole = functools.reduce(lambda a, b: a + b, unscaled)
    return [u / whole for u in unscaled]


def mix_kernel(share_ref, *refs):
    refs[-1][...] = functools.reduce(
        lambda a, b: a + b,
        [take_share(share_ref, at) * image[...] for at, image in enumerate(refs[:-1])],
    )


def last_kernel(k, *refs):
    shares = mix_shares(k, refs[:k])
    out_ref, refs = refs[-1], refs[k:-1]
    y, c = lax.axis_index("y"), lax.axis_index("c")
    for by in range(4):
        for half in range(2):
            row = (((y - by + 4) % 4) * 2 + (c + half) % 2) * 16
            rows = pl.ds(pl.multiple_of(row, 16), 16)
            pieces = [refs[5 * at + by][0] if half == 0 else refs[5 * at + 4][by] for at in range(k + 1)]
            out_ref[rows, :] = functools.reduce(
                lambda a, b: a + b, [share * piece for share, piece in zip(shares, pieces)]
            )


def start_kernel(inj_hbm, warm_hbm, gain_ref, payload_ref, *refs):
    home_refs, (inj_ref, warm_ref, sem) = refs[:4], refs[4:]
    loads = [
        pltpu.make_async_copy(inj_hbm, inj_ref, sem.at[0]),
        pltpu.make_async_copy(warm_hbm, warm_ref, sem.at[1]),
    ]
    for load in loads:
        load.start()
    y, c = lax.axis_index("y"), lax.axis_index("c")
    gain = gain_ref[:, pl.ds(pl.multiple_of((y * 2 + c) * 640, 640), 640)]
    for load in loads:
        load.wait()
    inj, warm = inj_ref[...].astype(F32), warm_ref[...].astype(F32)
    payload_ref[...] = ((inj + warm) * gain).astype(BF16)
    for by in range(4):
        for half in range(2):
            row = (((y + by) % 4) * 2 + (c + half) % 2) * 16
            rows = pl.ds(pl.multiple_of(row, 16), 16)
            home_refs[by][half, 0] = inj_ref[rows, :]
            home_refs[by][half, 1] = warm_ref[rows, :]


def settle_kernel(*refs):
    inj_ref, warm_ref = refs[5:]
    y, c = lax.axis_index("y"), lax.axis_index("c")
    for by in range(4):
        for half in range(2):
            column = (((y - by + 4) % 4) * 2 + (c + half) % 2) * 640
            columns = pl.ds(pl.multiple_of(column, 640), 640)
            piece = refs[by][0] if half == 0 else refs[4][by]
            inj_ref[:, columns] = piece[0]
            warm_ref[:, columns] = piece[1]


def move_home(pieces):
    near = [pieces[0]] + [lax.ppermute(pieces[by], "y", shift(4, by)) for by in (1, 2, 3)]
    joined = jnp.stack([piece[1] for piece in near])
    return [*near, lax.ppermute(joined, "c", shift(2, 1))]


def on_device(injection, warm_start, gain_in, gain_out, w_query, w_key, w_value, w_out):
    gain_in, gain_out = gain_in.reshape(1, D), gain_out.reshape(1, D)
    w_key, w_value, w_query, w_out = (
        pltpu.with_memory_space_constraint(w, pltpu.HBM) for w in (w_key, w_value, w_query, w_out)
    )
    tokens = pltpu.HBM((16, D), F32)
    wide = pltpu.VMEM((16, D), F32)
    narrow = pltpu.VMEM((16, D), BF16)
    home_narrow = pltpu.VMEM((2, 2, 16, 640), BF16)
    home_wide = pltpu.HBM((2, 16, 640), F32)
    payload, *home = call(
        start_kernel,
        (pltpu.VMEM((128, 640), BF16), *[home_narrow] * 4),
        pltpu.with_memory_space_constraint(injection, pltpu.HBM),
        pltpu.with_memory_space_constraint(warm_start, pltpu.HBM),
        gain_in,
        specs=[HBM, HBM, VMEM],
        scratch=[
            pltpu.VMEM((128, 640), BF16),
            pltpu.VMEM((128, 640), BF16),
            pltpu.SemaphoreType.DMA((2,)),
        ],
    )
    settled = []
    images, residuals, parts, tables, dots = [], [], [], [], None
    raws, pairs = [], []
    projected = (
        pltpu.HBM((128, D), BF16),
        pltpu.VMEM((128, 2 * HEAD_DIM), F32),
        pltpu.VMEM((128, 128), F32),
    )
    project_scratch = [
        pltpu.VMEM((128, D), BF16),
        pltpu.VMEM((D, 2 * HEAD_DIM), BF16),
        pltpu.SemaphoreType.DMA((3,)),
    ]
    for k in range(ITERS):
        pieces = [payload] + [lax.ppermute(payload, "y", shift(4, by)) for by in (1, 2, 3)]
        if dots is not None:
            tables.append(lax.all_to_all(dots, EVERY, split_axis=0, concat_axis=0, tiled=True))
        pieces += [lax.ppermute(piece, "c", shift(2, 1)) for piece in pieces]
        if k == 1:
            parts, raws, pairs = [], [], []
        if k == 0:
            rows, raw, pair = call(
                first_kernel,
                projected,
                w_key,
                w_value,
                gain_in,
                *pieces,
                specs=[HBM] * 2 + [VMEM] * 9,
                vmem=8,
                scratch=project_scratch,
                flops=2 * 128 * D * 256,
                touched=4_000_000,
            )
        else:
            rows, raw, pair = call(
                functools.partial(project_kernel, k - 1),
                projected,
                w_key,
                w_value,
                gain_in,
                *parts,
                *pieces,
                specs=[HBM] * 2 + [VMEM] + [HBM] * len(parts) + [VMEM] * 8,
                vmem=10,
                scratch=project_scratch
                + [
                    pltpu.VMEM((k - 1, 128, D) if k > 1 else (1, 8, 128), BF16),
                    pltpu.SemaphoreType.DMA((max(k - 1, 1), 8)),
                ],
                flops=2 * 128 * D * 256,
                touched=4_000_000,
            )
        parts.append(rows)
        raws.append(raw)
        pairs.append(pair)
        share, scale, kv = call(
            functools.partial(share_kernel, len(parts) - 1),
            (
                pltpu.VMEM((1, 128), F32),
                pltpu.VMEM((128, 128), F32),
                pltpu.HBM((16, 128, 2 * HEAD_DIM), BF16),
            ),
            *tables,
            *raws,
            *pairs,
            vmem=4,
            scratch=[
                pltpu.VMEM((128, 2 * HEAD_DIM), BF16),
                pltpu.SemaphoreType.DMA((16,)),
            ],
        )
        kv_all = lax.all_to_all(kv, SEQ, split_axis=0, concat_axis=0, tiled=True)
        q = query_dot(share, parts, w_query)
        home = move_home(home)
        kv_all, home = lax.optimization_barrier((kv_all, home))
        if k == 0:
            inj, current = call(settle_kernel, (narrow, narrow), *home)
        else:
            settled += home
        if k > 1:
            current = call(mix_kernel, wide, share, *images)
        own, send = call(
            attend_kernel,
            (pltpu.VMEM((64, D), F32), pltpu.VMEM((64, D), BF16)),
            q,
            scale,
            kv_all,
            w_out,
            specs=[VMEM, VMEM, VMEM, HBM],
            vmem=26,
            scratch=[
                pltpu.VMEM((640, D), BF16),
                pltpu.VMEM((640, HEAD_DIM), BF16),
                pltpu.VMEM((640, TOKENS), F32),
                pltpu.VMEM((640, TOKENS), BF16),
                pltpu.VMEM((640, 128), F32),
                pltpu.VMEM((128, 640), BF16),
                pltpu.SemaphoreType.DMA,
            ],
            flops=2 * 128 * 640 * (2 * TOKENS + D),
            touched=9_000_000,
        )
        pair = own + lax.ppermute(send, "c", shift(2, 1)).astype(F32)
        arrived = [
            lax.ppermute(pair[16 * by : 16 * by + 16].astype(BF16), "y", shift(4, -by))
            for by in (1, 2, 3)
        ]
        shapes = [tokens, tokens, *[home_wide] * 4]
        if k < ITERS - 1:
            shapes.append(narrow)
        if k > 0:
            shapes.append(pltpu.HBM((128, 1, 128), F32))
        outs = call(
            functools.partial(finish_kernel, k),
            tuple(shapes),
            pair[:16],
            *arrived,
            inj,
            current,
            gain_out,
            gain_in,
            *residuals,
            scratch=[
                pltpu.VMEM((16, D), F32),
                pltpu.VMEM((16, D), F32),
                pltpu.VMEM((128, 1, 128), F32),
                pltpu.SemaphoreType.DMA((11,)),
            ],
        )
        images.append(outs[0])
        residuals.append(outs[1])
        home = outs[2:6]
        payload = outs[6]
        if k == 0:
            current = outs[0]
        else:
            dots = outs[-1]
    settled += move_home(home)
    tables.append(lax.all_to_all(dots, EVERY, split_axis=0, concat_axis=0, tiled=True))
    return call(
        functools.partial(last_kernel, ITERS - 1),
        pltpu.VMEM((128, 640), F32),
        *tables,
        *settled,
    )


def solution(mesh):
    split = Mesh(mesh.devices.reshape(4, 4, 4, 2), EVERY)
    placed = (
        P(SEQ, FEAT),
        P(SEQ, FEAT),
        P(),
        P(),
        P(None, FEAT),
        P(None, FEAT),
        P(None, FEAT),
        P(FEAT, None),
    )
    return jax.shard_map(
        on_device, mesh=split, in_specs=placed, out_specs=P(SEQ, FEAT), check_vma=False
    )
```

```python
import functools
import math

import jax
import jax.numpy as jnp
from jax import lax
from jax.experimental import pallas as pl
from jax.experimental.pallas import tpu as pltpu
from jax.sharding import Mesh
from jax.sharding import PartitionSpec as P


D = 5120
HEADS = 40
KV_HEADS = 8
HEAD_DIM = 128
GROUP = HEADS // KV_HEADS
ITERS = 4
TOKENS = 2048
SEQ = ("x", "z")
FEAT = ("y", "c")
EVERY = ("x", "z", "y", "c")
EPS = 1e-06
LAMBDA = 0.03
SCORE_SCALE = 1.0 / math.sqrt(HEAD_DIM)
F32 = jnp.float32
BF16 = jnp.bfloat16

VMEM = pl.BlockSpec(memory_space=pltpu.VMEM)
HBM = pl.BlockSpec(memory_space=pltpu.HBM)


def shift(n, by):
    return [(at, (at + by) % n) for at in range(n)]


def call(kernel, outs, *args, specs=None, scratch=(), vmem=8, flops=0, touched=0):
    specs = [VMEM] * len(args) if specs is None else specs
    args = [
        pltpu.with_memory_space_constraint(arg, pltpu.HBM) if spec is HBM else arg
        for arg, spec in zip(args, specs)
    ]
    return pl.pallas_call(
        kernel,
        out_shape=outs,
        in_specs=specs,
        out_specs=jax.tree.map(lambda out: HBM if out.memory_space == pltpu.HBM else VMEM, outs),
        scratch_shapes=list(scratch),
        compiler_params=pltpu.CompilerParams(vmem_limit_bytes=vmem * 1024 * 1024),
        cost_estimate=pl.CostEstimate(flops=flops, bytes_accessed=touched, transcendentals=0),
    )(*args)


def total(x):
    return jnp.sum(jnp.sum(x, axis=1, keepdims=True), axis=0, keepdims=True)


def row_offset(row):
    y, c = lax.axis_index("y"), lax.axis_index("c")
    half, block, inner = row // 64, (row // 16) % 4, row % 16
    return (((y - block + 4) % 4) * 2 + (c + half) % 2) * 16 + inner


def load_keys(wk_ref, wv_ref, held, sem):
    copies = [
        pltpu.make_async_copy(wk_ref, held.at[:, :HEAD_DIM], sem.at[0]),
        pltpu.make_async_copy(wv_ref, held.at[:, HEAD_DIM:], sem.at[1]),
    ]
    for copy in copies:
        copy.start()
    return copies


def first_kernel(wk_ref, wv_ref, gain_ref, *refs):
    pieces, (rows_out, raw_out, rows_ref, held, raw_ref, sem) = refs[:2], refs[2:]
    loads = load_keys(wk_ref, wv_ref, held, sem)
    y, c = lax.axis_index("y"), lax.axis_index("c")
    for half in range(2):
        for block in range(4):
            column = (((y - block + 4) % 4) * 2 + (c + half) % 2) * 640
            columns = pl.ds(pl.multiple_of(column, 640), 640)
            for at in range(8):
                source = pl.multiple_of(row_offset(16 * at), 16)
                rows_ref[16 * at : 16 * at + 16, columns] = pieces[half][block, pl.ds(source, 16), :]
    keep = pltpu.make_async_copy(rows_ref, rows_out, sem.at[2])
    keep.start()

    def one_part(n, squares):
        at = pl.ds(pl.multiple_of(n * 640, 640), 640)
        part = rows_ref[:, at].astype(F32) * (1.0 / gain_ref[:, at])
        return squares + jnp.sum(part * part, axis=1, keepdims=True)

    squares = lax.fori_loop(0, 8, one_part, jnp.zeros((128, 1), F32))
    raw_ref[:, 256:] = jnp.broadcast_to(squares, (128, 128))
    for load in loads:
        load.wait()
    raw_ref[:, :256] = jnp.dot(rows_ref[...], held[...], preferred_element_type=F32)
    save = pltpu.make_async_copy(raw_ref, raw_out, sem.at[3])
    save.start()
    save.wait()
    keep.wait()


def project_kernel(k, *refs):
    (wk_ref, wv_ref, gain_ref), refs = refs[:3], refs[3:]
    older_hbm, pieces = refs[:k], refs[k : k + 2]
    rows_out, raw_out, rows_ref, held, raw_ref, sem, older_ref, older_sem = refs[k + 2 :]
    for n in range(8):
        for at in range(k):
            columns = slice(640 * n, 640 * n + 640)
            pltpu.make_async_copy(
                older_hbm[at].at[:, columns], older_ref.at[at, :, columns], older_sem.at[at, n]
            ).start()
    loads = load_keys(wk_ref, wv_ref, held, sem)

    def one_part(n, sums):
        at = pl.ds(pl.multiple_of(n * 640, 640), 640)
        newest = jnp.concatenate([piece[:, at] for piece in pieces], axis=0)
        rows_ref[:, at] = newest
        newest = newest.astype(F32)
        inverse = 1.0 / gain_ref[:, at]
        weighed = newest * (inverse * inverse)
        sums = list(sums)
        for old in range(k):
            pltpu.make_async_copy(
                older_hbm[old].at[:, at], older_ref.at[old, :, at], older_sem.at[old, n]
            ).wait()
            other = older_ref[old, :, at].astype(F32)
            sums[old] = sums[old] + jnp.sum(weighed * other, axis=1, keepdims=True)
        sums[k] = sums[k] + jnp.sum(weighed * newest, axis=1, keepdims=True)
        return tuple(sums)

    sums = lax.fori_loop(0, 8, one_part, tuple(jnp.zeros((128, 1), F32) for _ in range(k + 1)))
    keep = pltpu.make_async_copy(rows_ref, rows_out, sem.at[2])
    keep.start()
    lane = lax.broadcasted_iota(jnp.int32, (1, 128), 1)
    raw_ref[:, 256:] = functools.reduce(
        lambda a, b: a + b, [jnp.where(lane == at, value, 0.0) for at, value in enumerate(sums)]
    )
    for load in loads:
        load.wait()
    raw_ref[:, :256] = jnp.dot(rows_ref[...], held[...], preferred_element_type=F32)
    save = pltpu.make_async_copy(raw_ref, raw_out, sem.at[3])
    save.start()
    save.wait()
    keep.wait()


def share_kernel(k, *refs):
    raw_hbm, (share_ref, scale_out, kv_ref) = refs[k : 2 * k + 1], refs[2 * k + 1 : 2 * k + 4]
    raws, scale_ref, kv_held, sem = refs[2 * k + 4 :]
    loads = [
        pltpu.make_async_copy(raw, raws.at[at], sem.at[at]) for at, raw in enumerate(raw_hbm)
    ]
    for load in loads:
        load.start()
    shares = mix_shares(k, refs[:k])
    lane = lax.broadcasted_iota(jnp.int32, (1, 128), 1)
    share_ref[...] = functools.reduce(
        lambda a, b: a + b, [jnp.where(lane == at, share, 0.0) for at, share in enumerate(shares)]
    )
    for load in loads:
        load.wait()
    squares = jnp.zeros((128, 1), F32)
    for at in range(k + 1):
        for other in range(at + 1):
            twice = 1.0 if other == at else 2.0
            pair = raws[at, :, 256 + other : 257 + other]
            squares = squares + (twice * shares[at] * shares[other]) * pair
    scale = lax.rsqrt(jnp.maximum(squares, 0.0) / D + EPS)
    scale_ref[...] = jnp.broadcast_to(scale, (128, 128))
    kv = functools.reduce(
        lambda a, b: a + b, [share * raws[at, :, :256] for at, share in enumerate(shares)]
    )
    kv_held[...] = (kv * scale).astype(BF16)
    stores = [pltpu.make_async_copy(kv_held, kv_ref.at[at], sem.at[at]) for at in range(16)]
    stores.append(pltpu.make_async_copy(scale_ref, scale_out, sem.at[16]))
    for store in stores:
        store.start()
    for store in stores:
        store.wait()


def take_share(share_ref, at):
    lane = lax.broadcasted_iota(jnp.int32, (1, 128), 1)
    return jnp.sum(jnp.where(lane == at, share_ref[...], 0.0), axis=1, keepdims=True)


def query_kernel(k, share_ref, *refs):
    parts, (w_ref, q_ref, acc) = refs[: k + 1], refs[k + 1 :]

    @pl.when(pl.program_id(0) == 0)
    def _():
        acc[...] = jnp.zeros_like(acc)

    if k == 0:
        rows = parts[0][...]
    else:
        rows = functools.reduce(
            lambda a, b: a + b,
            [take_share(share_ref, at) * part[...].astype(F32) for at, part in enumerate(parts)],
        ).astype(BF16)
    acc[...] += jnp.dot(rows, w_ref[...], preferred_element_type=F32)

    @pl.when(pl.program_id(0) == 4)
    def _():
        q_ref[...] = acc[...].astype(BF16)


def query_dot(share, parts, w_query):
    return pl.pallas_call(
        functools.partial(query_kernel, len(parts) - 1),
        grid=(5,),
        out_shape=pltpu.VMEM((128, 640), BF16),
        in_specs=[pl.BlockSpec((1, 128), lambda n: (0, 0))]
        + [pl.BlockSpec((128, 1024), lambda n: (0, n))] * len(parts)
        + [pl.BlockSpec((1024, 640), lambda n: (n, 0))],
        out_specs=pl.BlockSpec((128, 640), lambda n: (0, 0)),
        scratch_shapes=[pltpu.VMEM((128, 640), F32)],
        compiler_params=pltpu.CompilerParams(vmem_limit_bytes=10 * 1024 * 1024),
        cost_estimate=pl.CostEstimate(
            flops=2 * 128 * D * 640, bytes_accessed=8_000_000, transcendentals=0
        ),
    )(share, *[pltpu.with_memory_space_constraint(part, pltpu.HBM) for part in (*parts, w_query)])


def attend_kernel(
    q_ref, scale_hbm, kv_ref, w_ref, own_ref, send_ref, w_held, scale_ref, attended, sem
):
    small = pltpu.make_async_copy(scale_hbm, scale_ref, sem.at[1])
    small.start()
    load = pltpu.make_async_copy(w_ref, w_held, sem.at[0])
    load.start()
    s = lax.axis_index("x") * 4 + lax.axis_index("z")
    row_at = s * 128 + row_offset(lax.broadcasted_iota(jnp.int32, (128, 1), 0))
    column = lax.broadcasted_iota(jnp.int32, (1, TOKENS), 1)
    allowed = row_at >= (column // 128) * 128 + row_offset(column % 128)
    small.wait()
    factor = scale_ref[:, :1] * (SCORE_SCALE / math.log(2.0))

    def one_head(g, carry):
        at = pl.ds(pl.multiple_of(g * HEAD_DIM, HEAD_DIM), HEAD_DIM)
        keys = kv_ref[:, :, :HEAD_DIM].reshape(TOKENS, HEAD_DIM)
        values = kv_ref[:, :, HEAD_DIM:].reshape(TOKENS, HEAD_DIM)
        raw = lax.dot_general(
            q_ref[:, at], keys, (((1,), (1,)), ((), ())), preferred_element_type=F32
        )
        raw = jnp.where(allowed, raw, -1e30)
        weight = jnp.exp2((raw - jnp.max(raw, axis=1, keepdims=True)) * factor)
        row_sum = jnp.sum(weight, axis=1, keepdims=True)
        summed = jnp.dot(weight.astype(BF16), values, preferred_element_type=F32)
        attended[:, at] = (summed / row_sum).astype(BF16)
        return carry

    lax.fori_loop(0, GROUP, one_head, 0)
    load.wait()

    def one_part(n, carry):
        at = pl.ds(pl.multiple_of(n * 1280, 1280), 1280)
        part = jnp.dot(attended[...], w_held[:, at], preferred_element_type=F32)
        own_ref[:, at] = part[:64]
        send_ref[:, at] = part[64:].astype(BF16)
        return carry

    lax.fori_loop(0, 4, one_part, 0)


def home_copies(held, target, sem, start):
    y, c = lax.axis_index("y"), lax.axis_index("c")
    copies = []
    for by in range(4):
        for half in range(2):
            column = (((y + by) % 4) * 2 + (c + half) % 2) * 640
            columns = pl.ds(pl.multiple_of(column, 640), 640)
            copies.append(
                pltpu.make_async_copy(
                    held.at[:, columns], target(by, half), sem.at[start + 2 * by + half]
                )
            )
    return copies


def pack_kernel(*refs):
    images, outs, (held, sem) = refs[:3], refs[3:7], refs[7:]
    loads = [
        pltpu.make_async_copy(image, held.at[at], sem.at[at]) for at, image in enumerate(images)
    ]
    for load in loads:
        load.start()
    copies = []
    for at in range(3):
        loads[at].wait()
        fresh = home_copies(
            held.at[at], lambda by, half: outs[by].at[half, at], sem, 3 + 8 * at
        )
        for copy in fresh:
            copy.start()
        copies += fresh
    for copy in copies:
        copy.wait()


def finish_kernel(k, own_ref, a_ref, b_ref, d_ref, inj_ref, x_ref, gain_ref, gain_in_ref, *rest):
    older, rest = rest[:k], rest[k:]
    image_held, residual_held, dots_held, sem = rest[-4:]
    image_out, residual_out = rest[:2]
    inj, x = inj_ref[...].astype(F32), x_ref[...].astype(F32)
    summed = (x + inj) + (
        own_ref[...] + a_ref[...].astype(F32) + b_ref[...].astype(F32) + d_ref[...].astype(F32)
    )
    scale = lax.rsqrt(jnp.sum(summed * summed, axis=1, keepdims=True) / D + EPS)
    image = summed * scale * gain_ref[...]
    residual = image - x
    image_held[...] = image
    residual_held[...] = residual
    copies = [
        pltpu.make_async_copy(image_held, image_out, sem.at[0]),
        pltpu.make_async_copy(residual_held, residual_out, sem.at[1]),
    ]
    if k == ITERS - 1:
        copies += home_copies(image_held, lambda by, half: rest[2 + by].at[half], sem, 2)
    for copy in copies:
        copy.start()
    if k < ITERS - 1:
        rest[2][...] = ((image + inj) * gain_in_ref[...]).astype(BF16)
    if k > 0:
        lane = lax.broadcasted_iota(jnp.int32, (1, 128), 1)
        dots = jnp.where(lane == k, total(residual * residual), 0.0)
        for at, other in enumerate(older):
            dots = dots + jnp.where(lane == at, total(residual * other[...]), 0.0)
        if k == 1:
            dots = dots + jnp.where(lane == 7, total(older[0][...] * older[0][...]), 0.0)
        dots_held[...] = jnp.broadcast_to(dots.reshape(1, 1, 128), (128, 1, 128))
        table_out = rest[3] if k < ITERS - 1 else rest[6]
        copies.append(pltpu.make_async_copy(dots_held, table_out, sem.at[10]))
        copies[-1].start()
    for copy in copies:
        copy.wait()


def solve_small(matrix, size_now):
    rows = [list(row) for row in matrix]
    values = [jnp.ones((1, 1), F32) for _ in range(size_now)]
    for pivot in range(size_now):
        for below in range(pivot + 1, size_now):
            ratio = rows[below][pivot] / rows[pivot][pivot]
            rows[below] = [b - ratio * p for b, p in zip(rows[below], rows[pivot])]
            values[below] = values[below] - ratio * values[pivot]
    result = [None] * size_now
    for pivot in reversed(range(size_now)):
        running = values[pivot]
        for later in range(pivot + 1, size_now):
            running = running - rows[pivot][later] * result[later]
        result[pivot] = running / rows[pivot][pivot]
    return result


def mix_shares(k, tables):
    if k == 0:
        return [1.0]
    lane = lax.broadcasted_iota(jnp.int32, (1, 128), 1)
    gram = {}
    for at, table in enumerate(tables):
        sums = jnp.sum(table[:, 0, :], axis=0, keepdims=True)
        for other in range(at + 2):
            gram[at + 1, other] = jnp.sum(jnp.where(lane == other, sums, 0.0), axis=1, keepdims=True)
        if at == 0:
            gram[0, 0] = jnp.sum(jnp.where(lane == 7, sums, 0.0), axis=1, keepdims=True)
    system = [
        [
            gram[max(i, j), min(i, j)] / float(TOKENS * D) + (LAMBDA if i == j else 0.0)
            for j in range(k + 1)
        ]
        for i in range(k + 1)
    ]
    unscaled = solve_small(system, k + 1)
    whole = functools.reduce(lambda a, b: a + b, unscaled)
    return [u / whole for u in unscaled]


def mix_kernel(share_ref, *refs):
    refs[-1][...] = functools.reduce(
        lambda a, b: a + b,
        [take_share(share_ref, at) * image[...] for at, image in enumerate(refs[:-1])],
    )


def last_kernel(k, *refs):
    shares = mix_shares(k, refs[:k])
    older, newest, (out_hbm, out_ref, sem) = refs[k : k + 5], refs[k + 5 : k + 10], refs[-3:]
    y, c = lax.axis_index("y"), lax.axis_index("c")
    for by in range(4):
        for half in range(2):
            row = (((y - by + 4) % 4) * 2 + (c + half) % 2) * 16
            rows = pl.ds(pl.multiple_of(row, 16), 16)
            old = older[by][0] if half == 0 else older[4][by]
            mixed = shares[k] * (newest[by][0] if half == 0 else newest[4][by])
            for at in range(k):
                mixed = mixed + shares[at] * old[at]
            out_ref[rows, :] = mixed
    store = pltpu.make_async_copy(out_ref, out_hbm, sem)
    store.start()
    store.wait()


def start_kernel(inj_hbm, warm_hbm, gain_hbm, payload_ref, *refs):
    home_refs, (inj_ref, warm_ref, gain_ref, sem) = refs[:4], refs[4:]
    loads = [
        pltpu.make_async_copy(gain_hbm, gain_ref, sem.at[2]),
        pltpu.make_async_copy(inj_hbm, inj_ref, sem.at[0]),
        pltpu.make_async_copy(warm_hbm, warm_ref, sem.at[1]),
    ]
    for load in loads:
        load.start()
    y, c = lax.axis_index("y"), lax.axis_index("c")
    for load in loads:
        load.wait()
    gain = gain_ref[:, pl.ds(pl.multiple_of((y * 2 + c) * 640, 640), 640)]
    inj, warm = inj_ref[...].astype(F32), warm_ref[...].astype(F32)
    payload_ref[...] = ((inj + warm) * gain).astype(BF16)
    for by in range(4):
        for half in range(2):
            row = (((y + by) % 4) * 2 + (c + half) % 2) * 16
            rows = pl.ds(pl.multiple_of(row, 16), 16)
            home_refs[by][half, 0] = inj_ref[rows, :]
            home_refs[by][half, 1] = warm_ref[rows, :]


def settle_kernel(*refs):
    inj_ref, warm_ref = refs[5:]
    y, c = lax.axis_index("y"), lax.axis_index("c")
    for by in range(4):
        for half in range(2):
            column = (((y - by + 4) % 4) * 2 + (c + half) % 2) * 640
            columns = pl.ds(pl.multiple_of(column, 640), 640)
            piece = refs[by][0] if half == 0 else refs[4][by]
            inj_ref[:, columns] = piece[0]
            warm_ref[:, columns] = piece[1]


def move_home(pieces):
    near = [pieces[0]] + [lax.ppermute(pieces[by], "y", shift(4, by)) for by in (1, 2, 3)]
    joined = jnp.stack([piece[1] for piece in near])
    return [*near, lax.ppermute(joined, "c", shift(2, 1))]


def on_device(injection, warm_start, gain_in, gain_out, w_query, w_key, w_value, w_out):
    gain_in, gain_out = gain_in.reshape(1, D), gain_out.reshape(1, D)
    tokens = pltpu.HBM((16, D), F32)
    wide = pltpu.VMEM((16, D), F32)
    narrow = pltpu.VMEM((16, D), BF16)
    home_narrow = pltpu.VMEM((2, 2, 16, 640), BF16)
    home_wide = pltpu.HBM((2, 16, 640), F32)
    payload, *home = call(
        start_kernel,
        (pltpu.VMEM((128, 640), BF16), *[home_narrow] * 4),
        injection,
        warm_start,
        gain_in,
        specs=[HBM, HBM, HBM],
        scratch=[
            pltpu.VMEM((128, 640), BF16),
            pltpu.VMEM((128, 640), BF16),
            pltpu.VMEM((1, D), F32),
            pltpu.SemaphoreType.DMA((3,)),
        ],
    )
    settled = []
    images, residuals, parts, tables, dots = [], [], [], [], None
    raws = []
    projected = (pltpu.HBM((128, D), BF16), pltpu.HBM((128, 384), F32))
    project_scratch = [
        pltpu.VMEM((128, D), BF16),
        pltpu.VMEM((D, 2 * HEAD_DIM), BF16),
        pltpu.VMEM((128, 384), F32),
        pltpu.SemaphoreType.DMA((4,)),
    ]
    for k in range(ITERS):
        pieces = [payload] + [lax.ppermute(payload, "y", shift(4, by)) for by in (1, 2, 3)]
        if dots is not None:
            tables.append(lax.all_to_all(dots, EVERY, split_axis=0, concat_axis=0, tiled=True))
        mine = jnp.stack(pieces) if k == 0 else jnp.concatenate(pieces, axis=0)
        pieces = [mine, lax.ppermute(mine, "c", shift(2, 1))]
        if k == 1:
            parts, raws = [], []
        if k == 0:
            rows, raw = call(
                first_kernel,
                projected,
                w_key,
                w_value,
                gain_in,
                *pieces,
                specs=[HBM] * 2 + [VMEM] * 3,
                vmem=8,
                scratch=project_scratch,
                flops=2 * 128 * D * 256,
                touched=4_000_000,
            )
        else:
            rows, raw = call(
                functools.partial(project_kernel, k - 1),
                projected,
                w_key,
                w_value,
                gain_in,
                *parts,
                *pieces,
                specs=[HBM] * 2 + [VMEM] + [HBM] * len(parts) + [VMEM] * 2,
                vmem=10,
                scratch=project_scratch
                + [
                    pltpu.VMEM((k - 1, 128, D) if k > 1 else (1, 8, 128), BF16),
                    pltpu.SemaphoreType.DMA((max(k - 1, 1), 8)),
                ],
                flops=2 * 128 * D * 256,
                touched=4_000_000,
            )
        parts.append(rows)
        raws.append(raw)
        share, scale, kv = call(
            functools.partial(share_kernel, len(parts) - 1),
            (
                pltpu.VMEM((1, 128), F32),
                pltpu.HBM((128, 128), F32),
                pltpu.HBM((16, 128, 2 * HEAD_DIM), BF16),
            ),
            *tables,
            *raws,
            specs=[VMEM] * len(tables) + [HBM] * len(raws),
            vmem=4,
            scratch=[
                pltpu.VMEM((len(raws), 128, 384), F32),
                pltpu.VMEM((128, 128), F32),
                pltpu.VMEM((128, 2 * HEAD_DIM), BF16),
                pltpu.SemaphoreType.DMA((17,)),
            ],
        )
        kv_all = lax.all_to_all(kv, SEQ, split_axis=0, concat_axis=0, tiled=True)
        q = query_dot(share, parts, w_query)
        if k == ITERS - 1:
            home = call(
                pack_kernel,
                [pltpu.HBM((2, 3, 16, 640), F32)] * 4,
                *images,
                specs=[HBM] * 3,
                scratch=[pltpu.VMEM((3, 16, D), F32), pltpu.SemaphoreType.DMA((27,))],
            )
        if k in (0, ITERS - 1):
            home = move_home(home)
            kv_all, home = lax.optimization_barrier((kv_all, home))
        if k == 0:
            inj, current = call(settle_kernel, (narrow, narrow), *home)
        if k == ITERS - 1:
            settled = home
        if k > 1:
            current = call(mix_kernel, wide, share, *images)
        own, send = call(
            attend_kernel,
            (pltpu.VMEM((64, D), F32), pltpu.VMEM((64, D), BF16)),
            q,
            scale,
            kv_all,
            w_out,
            specs=[VMEM, HBM, VMEM, HBM],
            vmem=16,
            scratch=[
                pltpu.VMEM((640, D), BF16),
                pltpu.VMEM((128, 128), F32),
                pltpu.VMEM((128, 640), BF16),
                pltpu.SemaphoreType.DMA((2,)),
            ],
            flops=2 * 128 * 640 * (2 * TOKENS + D),
            touched=9_000_000,
        )
        pair = own + lax.ppermute(send, "c", shift(2, 1)).astype(F32)
        arrived = [
            lax.ppermute(pair[16 * by : 16 * by + 16].astype(BF16), "y", shift(4, -by))
            for by in (1, 2, 3)
        ]
        shapes = [tokens, tokens] + ([home_wide] * 4 if k == ITERS - 1 else [])
        if k < ITERS - 1:
            shapes.append(narrow)
        if k > 0:
            shapes.append(pltpu.HBM((128, 1, 128), F32))
        outs = call(
            functools.partial(finish_kernel, k),
            tuple(shapes),
            pair[:16],
            *arrived,
            inj,
            current,
            gain_out,
            gain_in,
            *residuals,
            scratch=[
                pltpu.VMEM((16, D), F32),
                pltpu.VMEM((16, D), F32),
                pltpu.VMEM((128, 1, 128), F32),
                pltpu.SemaphoreType.DMA((11,)),
            ],
        )
        images.append(outs[0])
        residuals.append(outs[1])
        home = outs[2:6]
        payload = outs[2]
        if k == 0:
            current = outs[0]
        else:
            dots = outs[-1]
    settled = settled + move_home(home)
    tables.append(lax.all_to_all(dots, EVERY, split_axis=0, concat_axis=0, tiled=True))
    return call(
        functools.partial(last_kernel, ITERS - 1),
        pltpu.HBM((128, 640), F32),
        *tables,
        *settled,
        scratch=[pltpu.VMEM((128, 640), F32), pltpu.SemaphoreType.DMA],
    )


def solution(mesh):
    split = Mesh(mesh.devices.reshape(4, 4, 4, 2), EVERY)
    placed = (
        P(SEQ, FEAT),
        P(SEQ, FEAT),
        P(),
        P(),
        P(None, FEAT),
        P(None, FEAT),
        P(None, FEAT),
        P(FEAT, None),
    )
    return jax.shard_map(
        on_device, mesh=split, in_specs=placed, out_specs=P(SEQ, FEAT), check_vma=False
    )
```

```python
import functools
import math

import jax
import jax.numpy as jnp
from jax import lax
from jax.experimental import pallas as pl
from jax.experimental.pallas import tpu as pltpu
from jax.sharding import Mesh
from jax.sharding import PartitionSpec as P


D = 5120
HEADS = 40
KV_HEADS = 8
HEAD_DIM = 128
GROUP = HEADS // KV_HEADS
ITERS = 4
TOKENS = 2048
SEQ = ("x", "z")
FEAT = ("y", "c")
EVERY = ("x", "z", "y", "c")
EPS = 1e-06
LAMBDA = 0.03
SCORE_SCALE = 1.0 / math.sqrt(HEAD_DIM)
F32 = jnp.float32
BF16 = jnp.bfloat16

VMEM = pl.BlockSpec(memory_space=pltpu.VMEM)
HBM = pl.BlockSpec(memory_space=pltpu.HBM)


def shift(n, by):
    return [(at, (at + by) % n) for at in range(n)]


def call(kernel, outs, *args, specs=None, scratch=(), vmem=8, flops=0, touched=0, aliases=None):
    specs = [VMEM] * len(args) if specs is None else specs
    args = [
        pltpu.with_memory_space_constraint(arg, pltpu.HBM) if spec is HBM else arg
        for arg, spec in zip(args, specs)
    ]
    return pl.pallas_call(
        kernel,
        out_shape=outs,
        in_specs=specs,
        input_output_aliases=aliases or {},
        out_specs=jax.tree.map(lambda out: HBM if out.memory_space == pltpu.HBM else VMEM, outs),
        scratch_shapes=list(scratch),
        compiler_params=pltpu.CompilerParams(vmem_limit_bytes=vmem * 1024 * 1024),
        cost_estimate=pl.CostEstimate(flops=flops, bytes_accessed=touched, transcendentals=0),
    )(*args)


def total(x):
    return jnp.sum(jnp.sum(x, axis=1, keepdims=True), axis=0, keepdims=True)


def row_offset(row):
    y, c = lax.axis_index("y"), lax.axis_index("c")
    half, block, inner = row // 64, (row // 16) % 4, row % 16
    return (((y - block + 4) % 4) * 2 + (c + half) % 2) * 16 + inner


def load_keys(wk_ref, wv_ref, held, sem):
    copies = [
        pltpu.make_async_copy(wk_ref, held.at[:, :HEAD_DIM], sem.at[0]),
        pltpu.make_async_copy(wv_ref, held.at[:, HEAD_DIM:], sem.at[1]),
    ]
    for copy in copies:
        copy.start()
    return copies


def first_kernel(wk_ref, wv_ref, gain_ref, *refs):
    pieces, (rows_out, scale_ref, kv_ref, rows_ref, held, kv_held, sem) = refs[:2], refs[2:]
    loads = load_keys(wk_ref, wv_ref, held, sem)
    y, c = lax.axis_index("y"), lax.axis_index("c")
    for half in range(2):
        for block in range(4):
            column = (((y - block + 4) % 4) * 2 + (c + half) % 2) * 640
            columns = pl.ds(pl.multiple_of(column, 640), 640)
            for at in range(8):
                source = pl.multiple_of(row_offset(16 * at), 16)
                rows_ref[16 * at : 16 * at + 16, columns] = pieces[half][block, pl.ds(source, 16), :]
    keep = pltpu.make_async_copy(rows_ref, rows_out, sem.at[2])
    keep.start()

    def one_part(n, squares):
        at = pl.ds(pl.multiple_of(n * 640, 640), 640)
        part = rows_ref[:, at].astype(F32) * (1.0 / gain_ref[:, at])
        return squares + jnp.sum(part * part, axis=1, keepdims=True)

    squares = lax.fori_loop(0, 8, one_part, jnp.zeros((128, 1), F32))
    for load in loads:
        load.wait()
    raw = jnp.dot(rows_ref[...], held[...], preferred_element_type=F32)
    hand_out(raw, squares, scale_ref, kv_ref, kv_held, sem)
    keep.wait()


def hand_out(raw, squares, scale_ref, kv_ref, kv_held, sem):
    scale = lax.rsqrt(squares / D + EPS)
    kv_held[...] = (raw * scale).astype(BF16)
    stores = [pltpu.make_async_copy(kv_held, kv_ref.at[at], sem.at[3 + at]) for at in range(16)]
    for store in stores:
        store.start()
    scale_ref[...] = jnp.broadcast_to(scale, (128, 128))
    for store in stores:
        store.wait()


def project_kernel(k, *refs):
    (wk_ref, wv_ref, gain_ref), refs = refs[:3], refs[3:]
    older_hbm, pieces = refs[:k], refs[k : k + 2]
    rows_out, raw_ref, *hand, rows_ref, held, sem, older_ref, older_sem = refs[k + 2 :]
    for n in range(8):
        for at in range(k):
            columns = slice(640 * n, 640 * n + 640)
            pltpu.make_async_copy(
                older_hbm[at].at[:, columns], older_ref.at[at, :, columns], older_sem.at[at, n]
            ).start()
    loads = load_keys(wk_ref, wv_ref, held, sem)

    def one_part(n, sums):
        at = pl.ds(pl.multiple_of(n * 640, 640), 640)
        newest = jnp.concatenate([piece[:, at] for piece in pieces], axis=0)
        rows_ref[:, at] = newest
        newest = newest.astype(F32)
        inverse = 1.0 / gain_ref[:, at]
        weighed = newest * (inverse * inverse)
        sums = list(sums)
        for old in range(k):
            pltpu.make_async_copy(
                older_hbm[old].at[:, at], older_ref.at[old, :, at], older_sem.at[old, n]
            ).wait()
            other = older_ref[old, :, at].astype(F32)
            sums[old] = sums[old] + jnp.sum(weighed * other, axis=1, keepdims=True)
        sums[k] = sums[k] + jnp.sum(weighed * newest, axis=1, keepdims=True)
        return tuple(sums)

    sums = lax.fori_loop(0, 8, one_part, tuple(jnp.zeros((128, 1), F32) for _ in range(k + 1)))
    keep = pltpu.make_async_copy(rows_ref, rows_out, sem.at[2])
    keep.start()
    lane = lax.broadcasted_iota(jnp.int32, (1, 128), 1)
    raw_ref[:, 256:] = functools.reduce(
        lambda a, b: a + b, [jnp.where(lane == at, value, 0.0) for at, value in enumerate(sums)]
    )
    for load in loads:
        load.wait()
    raw = jnp.dot(rows_ref[...], held[...], preferred_element_type=F32)
    raw_ref[:, :256] = raw
    if k == 0:
        scale_ref, kv_ref, kv_held = hand
        hand_out(raw, sums[0], scale_ref, kv_ref, kv_held, sem)
    keep.wait()


def share_kernel(k, *refs):
    raws, (share_ref, scale_ref, kv_ref, kv_held, sem) = refs[k : 2 * k + 1], refs[2 * k + 1 :]
    shares = mix_shares(k, refs[:k])
    lane = lax.broadcasted_iota(jnp.int32, (1, 128), 1)
    share_ref[...] = functools.reduce(
        lambda a, b: a + b, [jnp.where(lane == at, share, 0.0) for at, share in enumerate(shares)]
    )
    squares = jnp.zeros((128, 1), F32)
    for at in range(k + 1):
        for other in range(at + 1):
            twice = 1.0 if other == at else 2.0
            pair = raws[at][:, 256 + other : 257 + other]
            squares = squares + (twice * shares[at] * shares[other]) * pair
    raw = functools.reduce(
        lambda a, b: a + b, [share * raws[at][:, :256] for at, share in enumerate(shares)]
    )
    hand_out(raw, jnp.maximum(squares, 0.0), scale_ref, kv_ref, kv_held, sem)


def take_share(share_ref, at):
    lane = lax.broadcasted_iota(jnp.int32, (1, 128), 1)
    return jnp.sum(jnp.where(lane == at, share_ref[...], 0.0), axis=1, keepdims=True)


def query_kernel(k, *refs):
    if k > 0:
        share_ref, refs = refs[0], refs[1:]
    parts, (w_ref, q_ref, acc) = refs[: k + 1], refs[k + 1 :]

    @pl.when(pl.program_id(0) == 0)
    def _():
        acc[...] = jnp.zeros_like(acc)

    if k == 0:
        rows = parts[0][...]
    else:
        rows = functools.reduce(
            lambda a, b: a + b,
            [take_share(share_ref, at) * part[...].astype(F32) for at, part in enumerate(parts)],
        ).astype(BF16)
    acc[...] += jnp.dot(rows, w_ref[...], preferred_element_type=F32)

    @pl.when(pl.program_id(0) == 4)
    def _():
        q_ref[...] = acc[...].astype(BF16)


def query_dot(share, parts, w_query):
    return pl.pallas_call(
        functools.partial(query_kernel, len(parts) - 1),
        grid=(5,),
        out_shape=pltpu.VMEM((128, 640), BF16),
        in_specs=[pl.BlockSpec((1, 128), lambda n: (0, 0))] * (len(parts) > 1)
        + [pl.BlockSpec((128, 1024), lambda n: (0, n))] * len(parts)
        + [pl.BlockSpec((1024, 640), lambda n: (n, 0))],
        out_specs=pl.BlockSpec((128, 640), lambda n: (0, 0)),
        scratch_shapes=[pltpu.VMEM((128, 640), F32)],
        compiler_params=pltpu.CompilerParams(vmem_limit_bytes=10 * 1024 * 1024),
        cost_estimate=pl.CostEstimate(
            flops=2 * 128 * D * 640, bytes_accessed=8_000_000, transcendentals=0
        ),
    )(*([share] if len(parts) > 1 else []), *[pltpu.with_memory_space_constraint(part, pltpu.HBM) for part in (*parts, w_query)])


def attend_kernel(
    q_ref, scale_ref, kv_ref, w_ref, own_ref, send_ref, w_held, attended, sem
):
    load = pltpu.make_async_copy(w_ref, w_held, sem)
    load.start()
    s = lax.axis_index("x") * 4 + lax.axis_index("z")
    row_at = s * 128 + row_offset(lax.broadcasted_iota(jnp.int32, (128, 1), 0))
    column = lax.broadcasted_iota(jnp.int32, (1, TOKENS), 1)
    allowed = row_at >= (column // 128) * 128 + row_offset(column % 128)
    factor = scale_ref[:, :1] * (SCORE_SCALE / math.log(2.0))

    def one_head(g, carry):
        at = pl.ds(pl.multiple_of(g * HEAD_DIM, HEAD_DIM), HEAD_DIM)
        keys = kv_ref[:, :, :HEAD_DIM].reshape(TOKENS, HEAD_DIM)
        values = kv_ref[:, :, HEAD_DIM:].reshape(TOKENS, HEAD_DIM)
        raw = lax.dot_general(
            q_ref[:, at], keys, (((1,), (1,)), ((), ())), preferred_element_type=F32
        )
        raw = jnp.where(allowed, raw, -1e30)
        weight = jnp.exp2((raw - jnp.max(raw, axis=1, keepdims=True)) * factor)
        row_sum = jnp.sum(weight, axis=1, keepdims=True)
        summed = jnp.dot(weight.astype(BF16), values, preferred_element_type=F32)
        attended[:, at] = (summed / row_sum).astype(BF16)
        return carry

    lax.fori_loop(0, GROUP, one_head, 0)
    load.wait()

    def one_part(n, carry):
        at = pl.ds(pl.multiple_of(n * 1280, 1280), 1280)
        part = jnp.dot(attended[...], w_held[:, at], preferred_element_type=F32)
        own_ref[:, at] = part[:64]
        send_ref[:, at] = part[64:].astype(BF16)
        return carry

    lax.fori_loop(0, 4, one_part, 0)


def home_copies(held, outs, at, sem, start):
    y, c = lax.axis_index("y"), lax.axis_index("c")
    copies = []
    for by in range(4):
        for half in range(2):
            column = (((y + by) % 4) * 2 + (c + half) % 2) * 640
            columns = pl.ds(pl.multiple_of(column, 640), 640)
            target = outs[half].at[at] if by == 0 else outs[1 + by].at[half, at]
            copies.append(
                pltpu.make_async_copy(held.at[:, columns], target, sem.at[start + 2 * by + half])
            )
    return copies


def finish_kernel(k, own_ref, a_ref, b_ref, d_ref, inj_ref, x_ref, gain_ref, gain_in_ref, *rest):
    older, rest = rest[:k], rest[k:]
    if k in (1, 2):
        rest = rest[5:]
    image_held, residual_held, dots_held, sem = rest[-4:]
    image_out, residual_out, *home_out = rest[:7]
    inj, x = inj_ref[...].astype(F32), x_ref[...].astype(F32)
    summed = (x + inj) + (
        own_ref[...] + a_ref[...].astype(F32) + b_ref[...].astype(F32) + d_ref[...].astype(F32)
    )
    scale = lax.rsqrt(jnp.sum(summed * summed, axis=1, keepdims=True) / D + EPS)
    image = summed * scale * gain_ref[...]
    residual = image - x
    image_held[...] = image
    residual_held[...] = residual
    copies = [
        pltpu.make_async_copy(image_held, image_out, sem.at[0]),
        pltpu.make_async_copy(residual_held, residual_out, sem.at[1]),
    ]
    copies += home_copies(image_held, home_out, k % (ITERS - 1), sem, 2)
    for copy in copies:
        copy.start()
    if k < ITERS - 1:
        rest[7][...] = ((image + inj) * gain_in_ref[...]).astype(BF16)
    if k > 0:
        lane = lax.broadcasted_iota(jnp.int32, (1, 128), 1)
        dots = jnp.where(lane == k, total(residual * residual), 0.0)
        for at, other in enumerate(older):
            dots = dots + jnp.where(lane == at, total(residual * other[...]), 0.0)
        if k == 1:
            dots = dots + jnp.where(lane == 7, total(older[0][...] * older[0][...]), 0.0)
        dots_held[...] = jnp.broadcast_to(dots.reshape(1, 1, 128), (128, 1, 128))
        table_out = rest[8] if k < ITERS - 1 else rest[7]
        copies.append(pltpu.make_async_copy(dots_held, table_out, sem.at[10]))
        copies[-1].start()
    for copy in copies:
        copy.wait()


def solve_small(matrix, size_now):
    rows = [list(row) for row in matrix]
    values = [jnp.ones((1, 1), F32) for _ in range(size_now)]
    for pivot in range(size_now):
        for below in range(pivot + 1, size_now):
            ratio = rows[below][pivot] / rows[pivot][pivot]
            rows[below] = [b - ratio * p for b, p in zip(rows[below], rows[pivot])]
            values[below] = values[below] - ratio * values[pivot]
    result = [None] * size_now
    for pivot in reversed(range(size_now)):
        running = values[pivot]
        for later in range(pivot + 1, size_now):
            running = running - rows[pivot][later] * result[later]
        result[pivot] = running / rows[pivot][pivot]
    return result


def mix_shares(k, tables):
    if k == 0:
        return [1.0]
    lane = lax.broadcasted_iota(jnp.int32, (1, 128), 1)
    gram = {}
    for at, table in enumerate(tables):
        sums = jnp.sum(table[:, 0, :], axis=0, keepdims=True)
        for other in range(at + 2):
            gram[at + 1, other] = jnp.sum(jnp.where(lane == other, sums, 0.0), axis=1, keepdims=True)
        if at == 0:
            gram[0, 0] = jnp.sum(jnp.where(lane == 7, sums, 0.0), axis=1, keepdims=True)
    system = [
        [
            gram[max(i, j), min(i, j)] / float(TOKENS * D) + (LAMBDA if i == j else 0.0)
            for j in range(k + 1)
        ]
        for i in range(k + 1)
    ]
    unscaled = solve_small(system, k + 1)
    whole = functools.reduce(lambda a, b: a + b, unscaled)
    return [u / whole for u in unscaled]


def mix_kernel(share_ref, *refs):
    refs[-1][...] = functools.reduce(
        lambda a, b: a + b,
        [take_share(share_ref, at) * image[...] for at, image in enumerate(refs[:-1])],
    )


def last_kernel(k, *refs):
    shares = mix_shares(k, refs[:k])
    older, newest, (out_hbm, out_ref, sem) = refs[k : k + 5], refs[k + 5 : k + 10], refs[-3:]
    y, c = lax.axis_index("y"), lax.axis_index("c")

    def piece(home, by, half, at):
        if half == 1:
            return home[4][by, at]
        return home[0][at] if by == 0 else home[by][0, at]

    for by in range(4):
        for half in range(2):
            row = (((y - by + 4) % 4) * 2 + (c + half) % 2) * 16
            rows = pl.ds(pl.multiple_of(row, 16), 16)
            mixed = shares[k] * piece(newest, by, half, 0)
            for at in range(k):
                mixed = mixed + shares[at] * piece(older, by, half, at)
            out_ref[rows, :] = mixed
    store = pltpu.make_async_copy(out_ref, out_hbm, sem)
    store.start()
    store.wait()


def start_kernel(inj_hbm, warm_hbm, gain_hbm, payload_ref, *refs):
    home_refs, (inj_ref, warm_ref, gain_ref, sem) = refs[:5], refs[5:]
    loads = [
        pltpu.make_async_copy(gain_hbm, gain_ref, sem.at[2]),
        pltpu.make_async_copy(inj_hbm, inj_ref, sem.at[0]),
        pltpu.make_async_copy(warm_hbm, warm_ref, sem.at[1]),
    ]
    for load in loads:
        load.start()
    y, c = lax.axis_index("y"), lax.axis_index("c")
    for load in loads:
        load.wait()
    gain = gain_ref[:, pl.ds(pl.multiple_of((y * 2 + c) * 640, 640), 640)]
    inj, warm = inj_ref[...].astype(F32), warm_ref[...].astype(F32)
    payload_ref[...] = ((inj + warm) * gain).astype(BF16)
    for by in range(4):
        for half in range(2):
            row = (((y + by) % 4) * 2 + (c + half) % 2) * 16
            rows = pl.ds(pl.multiple_of(row, 16), 16)
            for at, source in enumerate((inj_ref, warm_ref)):
                if by == 0:
                    home_refs[half][at] = source[rows, :]
                else:
                    home_refs[1 + by][half, at] = source[rows, :]


def settle_kernel(*refs):
    inj_ref, warm_ref = refs[5:]
    y, c = lax.axis_index("y"), lax.axis_index("c")
    for by in range(4):
        for half in range(2):
            column = (((y - by + 4) % 4) * 2 + (c + half) % 2) * 640
            columns = pl.ds(pl.multiple_of(column, 640), 640)
            for at, target in enumerate((inj_ref, warm_ref)):
                if half == 1:
                    target[:, columns] = refs[4][by, at]
                else:
                    target[:, columns] = refs[0][at] if by == 0 else refs[by][0, at]


def move_home(pieces):
    own, pair, *far = pieces
    near = [lax.ppermute(piece, "y", shift(4, by + 1)) for by, piece in enumerate(far)]
    joined = jnp.stack([pair] + [piece[1] for piece in near])
    return [own, *near, lax.ppermute(joined, "c", shift(2, 1))]


def on_device(injection, warm_start, gain_in, gain_out, w_query, w_key, w_value, w_out):
    gain_in, gain_out = gain_in.reshape(1, D), gain_out.reshape(1, D)
    tokens = pltpu.HBM((16, D), F32)
    wide = pltpu.VMEM((16, D), F32)
    narrow = pltpu.VMEM((16, D), BF16)
    home_narrow = [pltpu.VMEM((2, 16, 640), BF16)] * 2 + [pltpu.VMEM((2, 2, 16, 640), BF16)] * 3
    home_packed = [pltpu.HBM((3, 16, 640), F32)] * 2 + [pltpu.HBM((2, 3, 16, 640), F32)] * 3
    home_last = [pltpu.VMEM((1, 16, 640), F32)] * 2 + [pltpu.HBM((2, 1, 16, 640), F32)] * 3
    payload, *home = call(
        start_kernel,
        (pltpu.VMEM((128, 640), BF16), *home_narrow),
        injection,
        warm_start,
        gain_in,
        specs=[HBM, HBM, HBM],
        scratch=[
            pltpu.VMEM((128, 640), BF16),
            pltpu.VMEM((128, 640), BF16),
            pltpu.VMEM((1, D), F32),
            pltpu.SemaphoreType.DMA((3,)),
        ],
    )
    settled = []
    images, residuals, parts, tables, dots = [], [], [], [], None
    raws, share = [], None
    rows_out = pltpu.HBM((128, D), BF16)
    raw_out = pltpu.VMEM((128, 384), F32)
    hand_outs = [pltpu.VMEM((128, 128), F32), pltpu.HBM((16, 128, 2 * HEAD_DIM), BF16)]
    kv_scratch = pltpu.VMEM((128, 2 * HEAD_DIM), BF16)
    project_scratch = [pltpu.VMEM((128, D), BF16), pltpu.VMEM((D, 2 * HEAD_DIM), BF16)]
    many = pltpu.SemaphoreType.DMA((19,))
    for k in range(ITERS):
        pieces = [payload]
        for by in (1, 2, 3):
            pieces.append(lax.ppermute(payload, "y", shift(4, by)))
        if dots is not None:
            tables.append(lax.all_to_all(dots, EVERY, split_axis=0, concat_axis=0, tiled=True))
        mine = jnp.stack(pieces) if k == 0 else jnp.concatenate(pieces, axis=0)
        pieces = [mine, lax.ppermute(mine, "c", shift(2, 1))]
        if k == 1:
            parts, raws = [], []
        if k == 0:
            rows, scale, kv = call(
                first_kernel,
                [rows_out, *hand_outs],
                w_key,
                w_value,
                gain_in,
                *pieces,
                specs=[HBM] * 2 + [VMEM] * 3,
                vmem=8,
                scratch=[*project_scratch, kv_scratch, many],
                flops=2 * 128 * D * 256,
                touched=4_000_000,
            )
        else:
            rows, raw, *hand = call(
                functools.partial(project_kernel, k - 1),
                [rows_out, raw_out] + (hand_outs if k == 1 else []),
                w_key,
                w_value,
                gain_in,
                *parts,
                *pieces,
                specs=[HBM] * 2 + [VMEM] + [HBM] * len(parts) + [VMEM] * 2,
                vmem=10,
                scratch=([kv_scratch] if k == 1 else [])
                + project_scratch
                + [
                    many,
                    pltpu.VMEM((k - 1, 128, D) if k > 1 else (1, 8, 128), BF16),
                    pltpu.SemaphoreType.DMA((max(k - 1, 1), 8)),
                ],
                flops=2 * 128 * D * 256,
                touched=4_000_000,
            )
            raws.append(raw)
        parts.append(rows)
        if k == 1:
            scale, kv = hand
        if k > 1:
            share, scale, kv = call(
                functools.partial(share_kernel, len(parts) - 1),
                [pltpu.VMEM((1, 128), F32), *hand_outs],
                *tables,
                *raws,
                vmem=4,
                scratch=[kv_scratch, many],
            )
        kv_all = lax.all_to_all(kv, SEQ, split_axis=0, concat_axis=0, tiled=True)
        q = query_dot(share, parts, w_query)
        if k in (0, ITERS - 1):
            home = move_home(home)
            kv_all, home = lax.optimization_barrier((kv_all, home))
        if k == 0:
            inj, current = call(settle_kernel, (narrow, narrow), *home)
        if k == ITERS - 1:
            settled = home
        if k > 1:
            current = call(mix_kernel, wide, share, *images)
        own, send = call(
            attend_kernel,
            (pltpu.VMEM((64, D), F32), pltpu.VMEM((64, D), BF16)),
            q,
            scale,
            kv_all,
            w_out,
            specs=[VMEM, VMEM, VMEM, HBM],
            vmem=16,
            scratch=[
                pltpu.VMEM((640, D), BF16),
                pltpu.VMEM((128, 640), BF16),
                pltpu.SemaphoreType.DMA,
            ],
            flops=2 * 128 * 640 * (2 * TOKENS + D),
            touched=9_000_000,
        )
        pair = own + lax.ppermute(send, "c", shift(2, 1)).astype(F32)
        arrived = []
        for by in (1, 2, 3):
            piece = pair[16 * by : 16 * by + 16].astype(BF16)
            arrived.append(lax.ppermute(piece, "y", shift(4, -by)))
        shapes = [tokens, tokens, *(home_packed if k < ITERS - 1 else home_last)]
        if k < ITERS - 1:
            shapes.append(narrow)
        if k > 0:
            shapes.append(pltpu.HBM((128, 1, 128), F32))
        packed = list(home) if k in (1, 2) else []
        outs = call(
            functools.partial(finish_kernel, k),
            tuple(shapes),
            pair[:16],
            *arrived,
            inj,
            current,
            gain_out,
            gain_in,
            *residuals,
            *packed,
            specs=[VMEM] * (8 + len(residuals)) + [HBM] * len(packed),
            aliases={8 + k + at: 2 + at for at in range(len(packed))},
            scratch=[
                pltpu.VMEM((16, D), F32),
                pltpu.VMEM((16, D), F32),
                pltpu.VMEM((128, 1, 128), F32),
                pltpu.SemaphoreType.DMA((11,)),
            ],
        )
        images.append(outs[0])
        residuals.append(outs[1])
        home = outs[2:7]
        payload = outs[7]
        if k == 0:
            current = outs[0]
        else:
            dots = outs[-1]
    settled = settled + move_home(home)
    tables.append(lax.all_to_all(dots, EVERY, split_axis=0, concat_axis=0, tiled=True))
    return call(
        functools.partial(last_kernel, ITERS - 1),
        pltpu.HBM((128, 640), F32),
        *tables,
        *settled,
        scratch=[pltpu.VMEM((128, 640), F32), pltpu.SemaphoreType.DMA],
    )


def solution(mesh):
    split = Mesh(mesh.devices.reshape(4, 4, 4, 2), EVERY)
    placed = (
        P(SEQ, FEAT),
        P(SEQ, FEAT),
        P(),
        P(),
        P(None, FEAT),
        P(None, FEAT),
        P(None, FEAT),
        P(FEAT, None),
    )
    return jax.shard_map(
        on_device, mesh=split, in_specs=placed, out_specs=P(SEQ, FEAT), check_vma=False
    )
```

```python
import functools
import math

import jax
import jax.numpy as jnp
from jax import lax
from jax.experimental import pallas as pl
from jax.experimental.pallas import tpu as pltpu
from jax.sharding import Mesh
from jax.sharding import PartitionSpec as P


D = 5120
HEADS = 40
KV_HEADS = 8
HEAD_DIM = 128
GROUP = HEADS // KV_HEADS
ITERS = 4
TOKENS = 2048
SEQ = ("x", "z")
FEAT = ("y", "c")
EVERY = ("x", "z", "y", "c")
EPS = 1e-06
LAMBDA = 0.03
SCORE_SCALE = 1.0 / math.sqrt(HEAD_DIM)
F32 = jnp.float32
BF16 = jnp.bfloat16

VMEM = pl.BlockSpec(memory_space=pltpu.VMEM)
HBM = pl.BlockSpec(memory_space=pltpu.HBM)


def shift(n, by):
    return [(at, (at + by) % n) for at in range(n)]


def call(kernel, outs, *args, specs=None, scratch=(), vmem=8, flops=0, touched=0, aliases=None):
    specs = [VMEM] * len(args) if specs is None else specs
    args = [
        pltpu.with_memory_space_constraint(arg, pltpu.HBM) if spec is HBM else arg
        for arg, spec in zip(args, specs)
    ]
    return pl.pallas_call(
        kernel,
        out_shape=outs,
        in_specs=specs,
        input_output_aliases=aliases or {},
        out_specs=jax.tree.map(lambda out: HBM if out.memory_space == pltpu.HBM else VMEM, outs),
        scratch_shapes=list(scratch),
        compiler_params=pltpu.CompilerParams(vmem_limit_bytes=vmem * 1024 * 1024),
        cost_estimate=pl.CostEstimate(flops=flops, bytes_accessed=touched, transcendentals=0),
    )(*args)


def total(x):
    return jnp.sum(jnp.sum(x, axis=1, keepdims=True), axis=0, keepdims=True)


def row_offset(row):
    y, c = lax.axis_index("y"), lax.axis_index("c")
    half, block, inner = row // 64, (row // 16) % 4, row % 16
    return (((y - block + 4) % 4) * 2 + (c + half) % 2) * 16 + inner


def load_keys(wk_ref, wv_ref, held, sem):
    copies = [
        pltpu.make_async_copy(wk_ref, held.at[:, :HEAD_DIM], sem.at[0]),
        pltpu.make_async_copy(wv_ref, held.at[:, HEAD_DIM:], sem.at[1]),
    ]
    for copy in copies:
        copy.start()
    return copies


def first_kernel(wk_ref, wv_ref, gain_ref, *refs):
    pieces, (rows_out, scale_ref, kv_ref, rows_ref, held, kv_held, sem) = refs[:2], refs[2:]
    loads = load_keys(wk_ref, wv_ref, held, sem)
    y, c = lax.axis_index("y"), lax.axis_index("c")
    for half in range(2):
        for block in range(4):
            column = (((y - block + 4) % 4) * 2 + (c + half) % 2) * 640
            columns = pl.ds(pl.multiple_of(column, 640), 640)
            for at in range(8):
                source = pl.multiple_of(row_offset(16 * at), 16)
                rows_ref[16 * at : 16 * at + 16, columns] = pieces[half][block, pl.ds(source, 16), :]
    keep = pltpu.make_async_copy(rows_ref, rows_out, sem.at[2])
    keep.start()

    def one_part(n, squares):
        at = pl.ds(pl.multiple_of(n * 640, 640), 640)
        part = rows_ref[:, at].astype(F32) * (1.0 / gain_ref[:, at])
        return squares + jnp.sum(part * part, axis=1, keepdims=True)

    squares = lax.fori_loop(0, 8, one_part, jnp.zeros((128, 1), F32))
    for load in loads:
        load.wait()
    raw = jnp.dot(rows_ref[...], held[...], preferred_element_type=F32)
    hand_out(raw, squares, scale_ref, kv_ref, kv_held, sem)
    keep.wait()


def hand_out(raw, squares, scale_ref, kv_ref, kv_held, sem):
    scale = lax.rsqrt(squares / D + EPS)
    kv_held[...] = (raw * scale).astype(BF16)
    stores = [pltpu.make_async_copy(kv_held, kv_ref.at[at], sem.at[3 + at]) for at in range(16)]
    for store in stores:
        store.start()
    scale_ref[...] = jnp.broadcast_to(scale, (128, 128))
    for store in stores:
        store.wait()


def project_kernel(k, *refs):
    (wk_ref, wv_ref, gain_ref), refs = refs[:3], refs[3:]
    older_hbm, pieces = refs[:k], refs[k : k + 2]
    rows_out, raw_ref, *hand, rows_ref, held, sem, older_ref, older_sem = refs[k + 2 :]
    for n in range(8):
        for at in range(k):
            columns = slice(640 * n, 640 * n + 640)
            pltpu.make_async_copy(
                older_hbm[at].at[:, columns], older_ref.at[at, :, columns], older_sem.at[at, n]
            ).start()
    loads = load_keys(wk_ref, wv_ref, held, sem)

    def one_part(n, sums):
        at = pl.ds(pl.multiple_of(n * 640, 640), 640)
        newest = jnp.concatenate([piece[:, at] for piece in pieces], axis=0)
        rows_ref[:, at] = newest
        newest = newest.astype(F32)
        inverse = 1.0 / gain_ref[:, at]
        weighed = newest * (inverse * inverse)
        sums = list(sums)
        for old in range(k):
            pltpu.make_async_copy(
                older_hbm[old].at[:, at], older_ref.at[old, :, at], older_sem.at[old, n]
            ).wait()
            other = older_ref[old, :, at].astype(F32)
            sums[old] = sums[old] + jnp.sum(weighed * other, axis=1, keepdims=True)
        sums[k] = sums[k] + jnp.sum(weighed * newest, axis=1, keepdims=True)
        return tuple(sums)

    sums = lax.fori_loop(0, 8, one_part, tuple(jnp.zeros((128, 1), F32) for _ in range(k + 1)))
    keep = pltpu.make_async_copy(rows_ref, rows_out, sem.at[2])
    keep.start()
    lane = lax.broadcasted_iota(jnp.int32, (1, 128), 1)
    raw_ref[:, 256:] = functools.reduce(
        lambda a, b: a + b, [jnp.where(lane == at, value, 0.0) for at, value in enumerate(sums)]
    )
    for load in loads:
        load.wait()
    raw = jnp.dot(rows_ref[...], held[...], preferred_element_type=F32)
    raw_ref[:, :256] = raw
    if k == 0:
        scale_ref, kv_ref, kv_held = hand
        hand_out(raw, sums[0], scale_ref, kv_ref, kv_held, sem)
    keep.wait()


def share_kernel(k, *refs):
    raws, (share_ref, scale_ref, kv_ref, kv_held, sem) = refs[k : 2 * k + 1], refs[2 * k + 1 :]
    shares = mix_shares(k, refs[:k])
    lane = lax.broadcasted_iota(jnp.int32, (1, 128), 1)
    share_ref[...] = functools.reduce(
        lambda a, b: a + b, [jnp.where(lane == at, share, 0.0) for at, share in enumerate(shares)]
    )
    squares = jnp.zeros((128, 1), F32)
    for at in range(k + 1):
        for other in range(at + 1):
            twice = 1.0 if other == at else 2.0
            pair = raws[at][:, 256 + other : 257 + other]
            squares = squares + (twice * shares[at] * shares[other]) * pair
    raw = functools.reduce(
        lambda a, b: a + b, [share * raws[at][:, :256] for at, share in enumerate(shares)]
    )
    hand_out(raw, jnp.maximum(squares, 0.0), scale_ref, kv_ref, kv_held, sem)


def take_share(share_ref, at):
    lane = lax.broadcasted_iota(jnp.int32, (1, 128), 1)
    return jnp.sum(jnp.where(lane == at, share_ref[...], 0.0), axis=1, keepdims=True)


def query_kernel(k, *refs):
    if k > 0:
        share_ref, refs = refs[0], refs[1:]
    parts, (w_ref, q_ref, acc) = refs[: k + 1], refs[k + 1 :]

    @pl.when(pl.program_id(0) == 0)
    def _():
        acc[...] = jnp.zeros_like(acc)

    if k == 0:
        rows = parts[0][...]
    else:
        rows = functools.reduce(
            lambda a, b: a + b,
            [take_share(share_ref, at) * part[...].astype(F32) for at, part in enumerate(parts)],
        ).astype(BF16)
    acc[...] += jnp.dot(rows, w_ref[...], preferred_element_type=F32)

    @pl.when(pl.program_id(0) == 4)
    def _():
        q_ref[...] = acc[...].astype(BF16)


def query_dot(share, parts, w_query):
    return pl.pallas_call(
        functools.partial(query_kernel, len(parts) - 1),
        grid=(5,),
        out_shape=pltpu.VMEM((128, 640), BF16),
        in_specs=[pl.BlockSpec((1, 128), lambda n: (0, 0))] * (len(parts) > 1)
        + [pl.BlockSpec((128, 1024), lambda n: (0, n))] * len(parts)
        + [pl.BlockSpec((1024, 640), lambda n: (n, 0))],
        out_specs=pl.BlockSpec((128, 640), lambda n: (0, 0)),
        scratch_shapes=[pltpu.VMEM((128, 640), F32)],
        compiler_params=pltpu.CompilerParams(vmem_limit_bytes=10 * 1024 * 1024),
        cost_estimate=pl.CostEstimate(
            flops=2 * 128 * D * 640, bytes_accessed=8_000_000, transcendentals=0
        ),
    )(*([share] if len(parts) > 1 else []), *[pltpu.with_memory_space_constraint(part, pltpu.HBM) for part in (*parts, w_query)])


def attend_kernel(
    q_ref, scale_ref, kv_ref, w_ref, own_ref, send_ref, w_held, attended, sem
):
    load = pltpu.make_async_copy(w_ref, w_held, sem)
    load.start()
    s = lax.axis_index("x") * 4 + lax.axis_index("z")
    row_at = s * 128 + row_offset(lax.broadcasted_iota(jnp.int32, (128, 1), 0))
    column = lax.broadcasted_iota(jnp.int32, (1, TOKENS), 1)
    allowed = row_at >= (column // 128) * 128 + row_offset(column % 128)
    factor = scale_ref[:, :1] * (SCORE_SCALE / math.log(2.0))

    def one_head(g, carry):
        at = pl.ds(pl.multiple_of(g * HEAD_DIM, HEAD_DIM), HEAD_DIM)
        keys = kv_ref[:, :, :HEAD_DIM].reshape(TOKENS, HEAD_DIM)
        values = kv_ref[:, :, HEAD_DIM:].reshape(TOKENS, HEAD_DIM)
        raw = lax.dot_general(
            q_ref[:, at], keys, (((1,), (1,)), ((), ())), preferred_element_type=F32
        )
        raw = jnp.where(allowed, raw, -1e30)
        weight = jnp.exp2((raw - jnp.max(raw, axis=1, keepdims=True)) * factor)
        row_sum = jnp.sum(weight, axis=1, keepdims=True)
        summed = jnp.dot(weight.astype(BF16), values, preferred_element_type=F32)
        attended[:, at] = (summed / row_sum).astype(BF16)
        return carry

    lax.fori_loop(0, GROUP, one_head, 0)
    load.wait()

    def one_part(n, carry):
        at = pl.ds(pl.multiple_of(n * 1280, 1280), 1280)
        part = jnp.dot(attended[...], w_held[:, at], preferred_element_type=F32)
        own_ref[:, at] = part[:64]
        send_ref[:, at] = part[64:].astype(BF16)
        return carry

    lax.fori_loop(0, 4, one_part, 0)


def home_copies(held, outs, at, sem, start):
    y, c = lax.axis_index("y"), lax.axis_index("c")
    copies = []
    for by in range(4):
        for half in range(2):
            column = (((y + by) % 4) * 2 + (c + half) % 2) * 640
            columns = pl.ds(pl.multiple_of(column, 640), 640)
            target = outs[half].at[at] if by == 0 else outs[1 + by].at[half, at]
            copies.append(
                pltpu.make_async_copy(held.at[:, columns], target, sem.at[start + 2 * by + half])
            )
    return copies


def finish_kernel(k, own_ref, a_ref, b_ref, d_ref, inj_ref, x_ref, gain_ref, gain_in_ref, *rest):
    older, rest = rest[:k], rest[k:]
    if k % 2 == 1:
        rest = rest[5:]
    image_held, residual_held, dots_held, sem = rest[-4:]
    image_out, residual_out, *home_out = rest[:7]
    inj, x = inj_ref[...].astype(F32), x_ref[...].astype(F32)
    summed = (x + inj) + (
        own_ref[...] + a_ref[...].astype(F32) + b_ref[...].astype(F32) + d_ref[...].astype(F32)
    )
    scale = lax.rsqrt(jnp.sum(summed * summed, axis=1, keepdims=True) / D + EPS)
    image = summed * scale * gain_ref[...]
    residual = image - x
    image_held[...] = image
    residual_held[...] = residual
    copies = [
        pltpu.make_async_copy(image_held, image_out, sem.at[0]),
        pltpu.make_async_copy(residual_held, residual_out, sem.at[1]),
    ]
    copies += home_copies(image_held, home_out, k % 2, sem, 2)
    for copy in copies:
        copy.start()
    if k < ITERS - 1:
        rest[7][...] = ((image + inj) * gain_in_ref[...]).astype(BF16)
    if k > 0:
        lane = lax.broadcasted_iota(jnp.int32, (1, 128), 1)
        dots = jnp.where(lane == k, total(residual * residual), 0.0)
        for at, other in enumerate(older):
            dots = dots + jnp.where(lane == at, total(residual * other[...]), 0.0)
        if k == 1:
            dots = dots + jnp.where(lane == 7, total(older[0][...] * older[0][...]), 0.0)
        dots_held[...] = jnp.broadcast_to(dots.reshape(1, 1, 128), (128, 1, 128))
        table_out = rest[8] if k < ITERS - 1 else rest[7]
        copies.append(pltpu.make_async_copy(dots_held, table_out, sem.at[10]))
        copies[-1].start()
    for copy in copies:
        copy.wait()


def solve_small(matrix, size_now):
    rows = [list(row) for row in matrix]
    values = [jnp.ones((1, 1), F32) for _ in range(size_now)]
    for pivot in range(size_now):
        for below in range(pivot + 1, size_now):
            ratio = rows[below][pivot] / rows[pivot][pivot]
            rows[below] = [b - ratio * p for b, p in zip(rows[below], rows[pivot])]
            values[below] = values[below] - ratio * values[pivot]
    result = [None] * size_now
    for pivot in reversed(range(size_now)):
        running = values[pivot]
        for later in range(pivot + 1, size_now):
            running = running - rows[pivot][later] * result[later]
        result[pivot] = running / rows[pivot][pivot]
    return result


def mix_shares(k, tables):
    if k == 0:
        return [1.0]
    lane = lax.broadcasted_iota(jnp.int32, (1, 128), 1)
    gram = {}
    for at, table in enumerate(tables):
        sums = jnp.sum(table[:, 0, :], axis=0, keepdims=True)
        for other in range(at + 2):
            gram[at + 1, other] = jnp.sum(jnp.where(lane == other, sums, 0.0), axis=1, keepdims=True)
        if at == 0:
            gram[0, 0] = jnp.sum(jnp.where(lane == 7, sums, 0.0), axis=1, keepdims=True)
    system = [
        [
            gram[max(i, j), min(i, j)] / float(TOKENS * D) + (LAMBDA if i == j else 0.0)
            for j in range(k + 1)
        ]
        for i in range(k + 1)
    ]
    unscaled = solve_small(system, k + 1)
    whole = functools.reduce(lambda a, b: a + b, unscaled)
    return [u / whole for u in unscaled]


def mix_kernel(share_ref, *refs):
    refs[-1][...] = functools.reduce(
        lambda a, b: a + b,
        [take_share(share_ref, at) * image[...] for at, image in enumerate(refs[:-1])],
    )


def last_kernel(k, *refs):
    shares = mix_shares(k, refs[:k])
    older, newest, (out_hbm, out_ref, sem) = refs[k : k + 5], refs[k + 5 : k + 10], refs[-3:]
    y, c = lax.axis_index("y"), lax.axis_index("c")

    def piece(home, by, half, at):
        if half == 1:
            return home[4][by, at]
        return home[0][at] if by == 0 else home[by][0, at]

    for by in range(4):
        for half in range(2):
            row = (((y - by + 4) % 4) * 2 + (c + half) % 2) * 16
            rows = pl.ds(pl.multiple_of(row, 16), 16)
            mixed = jnp.zeros((16, 640), F32)
            for at in range(k + 1):
                mixed = mixed + shares[at] * piece(older if at < 2 else newest, by, half, at % 2)
            out_ref[rows, :] = mixed
    store = pltpu.make_async_copy(out_ref, out_hbm, sem)
    store.start()
    store.wait()


def start_kernel(inj_hbm, warm_hbm, gain_hbm, payload_ref, *refs):
    home_refs, (inj_ref, warm_ref, gain_ref, sem) = refs[:5], refs[5:]
    loads = [
        pltpu.make_async_copy(gain_hbm, gain_ref, sem.at[2]),
        pltpu.make_async_copy(inj_hbm, inj_ref, sem.at[0]),
        pltpu.make_async_copy(warm_hbm, warm_ref, sem.at[1]),
    ]
    for load in loads:
        load.start()
    y, c = lax.axis_index("y"), lax.axis_index("c")
    for load in loads:
        load.wait()
    gain = gain_ref[:, pl.ds(pl.multiple_of((y * 2 + c) * 640, 640), 640)]
    inj, warm = inj_ref[...].astype(F32), warm_ref[...].astype(F32)
    payload_ref[...] = ((inj + warm) * gain).astype(BF16)
    for by in range(4):
        for half in range(2):
            row = (((y + by) % 4) * 2 + (c + half) % 2) * 16
            rows = pl.ds(pl.multiple_of(row, 16), 16)
            for at, source in enumerate((inj_ref, warm_ref)):
                if by == 0:
                    home_refs[half][at] = source[rows, :]
                else:
                    home_refs[1 + by][half, at] = source[rows, :]


def settle_kernel(*refs):
    inj_ref, warm_ref = refs[5:]
    y, c = lax.axis_index("y"), lax.axis_index("c")
    for by in range(4):
        for half in range(2):
            column = (((y - by + 4) % 4) * 2 + (c + half) % 2) * 640
            columns = pl.ds(pl.multiple_of(column, 640), 640)
            for at, target in enumerate((inj_ref, warm_ref)):
                if half == 1:
                    target[:, columns] = refs[4][by, at]
                else:
                    target[:, columns] = refs[0][at] if by == 0 else refs[by][0, at]


def move_home(pieces):
    own, pair, *far = pieces
    near = []
    for by, piece in enumerate(far):
        near.append(lax.ppermute(piece, "y", shift(4, by + 1)))
    joined = jnp.stack([pair] + [piece[1] for piece in near])
    return [own, *near, lax.ppermute(joined, "c", shift(2, 1))]


def on_device(injection, warm_start, gain_in, gain_out, w_query, w_key, w_value, w_out):
    gain_in, gain_out = gain_in.reshape(1, D), gain_out.reshape(1, D)
    tokens = pltpu.HBM((16, D), F32)
    wide = pltpu.VMEM((16, D), F32)
    narrow = pltpu.VMEM((16, D), BF16)
    home_narrow = [pltpu.VMEM((2, 16, 640), BF16)] * 2 + [pltpu.VMEM((2, 2, 16, 640), BF16)] * 3
    home_packed = [pltpu.HBM((2, 16, 640), F32)] * 2 + [pltpu.HBM((2, 2, 16, 640), F32)] * 3
    payload, *home = call(
        start_kernel,
        (pltpu.VMEM((128, 640), BF16), *home_narrow),
        injection,
        warm_start,
        gain_in,
        specs=[HBM, HBM, HBM],
        scratch=[
            pltpu.VMEM((128, 640), BF16),
            pltpu.VMEM((128, 640), BF16),
            pltpu.VMEM((1, D), F32),
            pltpu.SemaphoreType.DMA((3,)),
        ],
    )
    settled = []
    images, residuals, parts, tables, dots = [], [], [], [], None
    raws, share = [], None
    rows_out = pltpu.HBM((128, D), BF16)
    raw_out = pltpu.VMEM((128, 384), F32)
    hand_outs = [pltpu.VMEM((128, 128), F32), pltpu.HBM((16, 128, 2 * HEAD_DIM), BF16)]
    kv_scratch = pltpu.VMEM((128, 2 * HEAD_DIM), BF16)
    project_scratch = [pltpu.VMEM((128, D), BF16), pltpu.VMEM((D, 2 * HEAD_DIM), BF16)]
    many = pltpu.SemaphoreType.DMA((19,))
    for k in range(ITERS):
        pieces = [payload]
        for by in (1, 2, 3):
            pieces.append(lax.ppermute(payload, "y", shift(4, by)))
        if dots is not None:
            tables.append(lax.all_to_all(dots, EVERY, split_axis=0, concat_axis=0, tiled=True))
        mine = jnp.stack(pieces) if k == 0 else jnp.concatenate(pieces, axis=0)
        pieces = [mine, lax.ppermute(mine, "c", shift(2, 1))]
        if k == 1:
            parts, raws = [], []
        if k == 0:
            rows, scale, kv = call(
                first_kernel,
                [rows_out, *hand_outs],
                w_key,
                w_value,
                gain_in,
                *pieces,
                specs=[HBM] * 2 + [VMEM] * 3,
                vmem=8,
                scratch=[*project_scratch, kv_scratch, many],
                flops=2 * 128 * D * 256,
                touched=4_000_000,
            )
        else:
            rows, raw, *hand = call(
                functools.partial(project_kernel, k - 1),
                [rows_out, raw_out] + (hand_outs if k == 1 else []),
                w_key,
                w_value,
                gain_in,
                *parts,
                *pieces,
                specs=[HBM] * 2 + [VMEM] + [HBM] * len(parts) + [VMEM] * 2,
                vmem=10,
                scratch=([kv_scratch] if k == 1 else [])
                + project_scratch
                + [
                    many,
                    pltpu.VMEM((k - 1, 128, D) if k > 1 else (1, 8, 128), BF16),
                    pltpu.SemaphoreType.DMA((max(k - 1, 1), 8)),
                ],
                flops=2 * 128 * D * 256,
                touched=4_000_000,
            )
            raws.append(raw)
        parts.append(rows)
        if k == 1:
            scale, kv = hand
        if k > 1:
            share, scale, kv = call(
                functools.partial(share_kernel, len(parts) - 1),
                [pltpu.VMEM((1, 128), F32), *hand_outs],
                *tables,
                *raws,
                vmem=4,
                scratch=[kv_scratch, many],
            )
        kv_all = lax.all_to_all(kv, SEQ, split_axis=0, concat_axis=0, tiled=True)
        q = query_dot(share, parts, w_query)
        if k in (0, 2):
            home = move_home(home)
            kv_all, home = lax.optimization_barrier((kv_all, home))
        if k == 0:
            inj, current = call(settle_kernel, (narrow, narrow), *home)
        if k == 2:
            settled = home
        if k > 1:
            current = call(mix_kernel, wide, share, *images)
        own, send = call(
            attend_kernel,
            (pltpu.VMEM((64, D), F32), pltpu.VMEM((64, D), BF16)),
            q,
            scale,
            kv_all,
            w_out,
            specs=[VMEM, VMEM, VMEM, HBM],
            vmem=16,
            scratch=[
                pltpu.VMEM((640, D), BF16),
                pltpu.VMEM((128, 640), BF16),
                pltpu.SemaphoreType.DMA,
            ],
            flops=2 * 128 * 640 * (2 * TOKENS + D),
            touched=9_000_000,
        )
        pair = own + lax.ppermute(send, "c", shift(2, 1)).astype(F32)
        arrived = []
        for by in (1, 2, 3):
            piece = pair[16 * by : 16 * by + 16].astype(BF16)
            arrived.append(lax.ppermute(piece, "y", shift(4, -by)))
        shapes = [tokens, tokens, *home_packed]
        if k < ITERS - 1:
            shapes.append(narrow)
        if k > 0:
            shapes.append(pltpu.HBM((128, 1, 128), F32))
        packed = list(home) if k % 2 == 1 else []
        outs = call(
            functools.partial(finish_kernel, k),
            tuple(shapes),
            pair[:16],
            *arrived,
            inj,
            current,
            gain_out,
            gain_in,
            *residuals,
            *packed,
            specs=[VMEM] * (8 + len(residuals)) + [HBM] * len(packed),
            aliases={8 + k + at: 2 + at for at in range(len(packed))},
            scratch=[
                pltpu.VMEM((16, D), F32),
                pltpu.VMEM((16, D), F32),
                pltpu.VMEM((128, 1, 128), F32),
                pltpu.SemaphoreType.DMA((11,)),
            ],
        )
        images.append(outs[0])
        residuals.append(outs[1])
        home = outs[2:7]
        payload = outs[7]
        if k == 0:
            current = outs[0]
        else:
            dots = outs[-1]
    settled = settled + move_home(home)
    tables.append(lax.all_to_all(dots, EVERY, split_axis=0, concat_axis=0, tiled=True))
    return call(
        functools.partial(last_kernel, ITERS - 1),
        pltpu.HBM((128, 640), F32),
        *tables,
        *settled,
        scratch=[pltpu.VMEM((128, 640), F32), pltpu.SemaphoreType.DMA],
    )


def solution(mesh):
    split = Mesh(mesh.devices.reshape(4, 4, 4, 2), EVERY)
    placed = (
        P(SEQ, FEAT),
        P(SEQ, FEAT),
        P(),
        P(),
        P(None, FEAT),
        P(None, FEAT),
        P(None, FEAT),
        P(FEAT, None),
    )
    return jax.shard_map(
        on_device, mesh=split, in_specs=placed, out_specs=P(SEQ, FEAT), check_vma=False
    )
```

```python
import functools
import math

import jax
import jax.numpy as jnp
from jax import lax
from jax.experimental import pallas as pl
from jax.experimental.pallas import tpu as pltpu
from jax.sharding import Mesh
from jax.sharding import PartitionSpec as P


D = 5120
HEADS = 40
KV_HEADS = 8
HEAD_DIM = 128
GROUP = HEADS // KV_HEADS
ITERS = 4
TOKENS = 2048
SEQ = ("x", "z")
FEAT = ("y", "c")
EVERY = ("x", "z", "y", "c")
EPS = 1e-06
LAMBDA = 0.03
SCORE_SCALE = 1.0 / math.sqrt(HEAD_DIM)
F32 = jnp.float32
BF16 = jnp.bfloat16

VMEM = pl.BlockSpec(memory_space=pltpu.VMEM)
HBM = pl.BlockSpec(memory_space=pltpu.HBM)


def shift(n, by):
    return [(at, (at + by) % n) for at in range(n)]


def call(kernel, outs, *args, specs=None, scratch=(), vmem=8, flops=0, touched=0, aliases=None):
    specs = [VMEM] * len(args) if specs is None else specs
    args = [
        pltpu.with_memory_space_constraint(arg, pltpu.HBM) if spec is HBM else arg
        for arg, spec in zip(args, specs)
    ]
    return pl.pallas_call(
        kernel,
        out_shape=outs,
        in_specs=specs,
        input_output_aliases=aliases or {},
        out_specs=jax.tree.map(lambda out: HBM if out.memory_space == pltpu.HBM else VMEM, outs),
        scratch_shapes=list(scratch),
        compiler_params=pltpu.CompilerParams(vmem_limit_bytes=vmem * 1024 * 1024),
        cost_estimate=pl.CostEstimate(flops=flops, bytes_accessed=touched, transcendentals=0),
    )(*args)


def total(x):
    return jnp.sum(jnp.sum(x, axis=1, keepdims=True), axis=0, keepdims=True)


def row_offset(row):
    y, c = lax.axis_index("y"), lax.axis_index("c")
    half, block, inner = row // 64, (row // 16) % 4, row % 16
    return (((y - block + 4) % 4) * 2 + (c + half) % 2) * 16 + inner


def load_keys(wk_ref, wv_ref, held, sem):
    copies = [
        pltpu.make_async_copy(wk_ref, held.at[:, :HEAD_DIM], sem.at[0]),
        pltpu.make_async_copy(wv_ref, held.at[:, HEAD_DIM:], sem.at[1]),
    ]
    for copy in copies:
        copy.start()
    return copies


def first_kernel(wk_ref, wv_ref, gain_ref, *refs):
    pieces, (rows_out, scale_ref, kv_ref, rows_ref, held, kv_held, sem) = refs[:2], refs[2:]
    loads = load_keys(wk_ref, wv_ref, held, sem)
    y, c = lax.axis_index("y"), lax.axis_index("c")
    for half in range(2):
        for block in range(4):
            column = (((y - block + 4) % 4) * 2 + (c + half) % 2) * 640
            columns = pl.ds(pl.multiple_of(column, 640), 640)
            for at in range(8):
                source = pl.multiple_of(row_offset(16 * at), 16)
                rows_ref[16 * at : 16 * at + 16, columns] = pieces[half][block, pl.ds(source, 16), :]
    keep = pltpu.make_async_copy(rows_ref, rows_out, sem.at[2])
    keep.start()

    def one_part(n, squares):
        at = pl.ds(pl.multiple_of(n * 640, 640), 640)
        part = rows_ref[:, at].astype(F32) * (1.0 / gain_ref[:, at])
        return squares + jnp.sum(part * part, axis=1, keepdims=True)

    squares = lax.fori_loop(0, 8, one_part, jnp.zeros((128, 1), F32))
    for load in loads:
        load.wait()
    raw = jnp.dot(rows_ref[...], held[...], preferred_element_type=F32)
    hand_out(raw, squares, scale_ref, kv_ref, kv_held, sem)
    keep.wait()


def hand_out(raw, squares, scale_ref, kv_ref, kv_held, sem):
    scale = lax.rsqrt(squares / D + EPS)
    kv_held[...] = (raw * scale).astype(BF16)
    stores = [pltpu.make_async_copy(kv_held, kv_ref.at[at], sem.at[3 + at]) for at in range(16)]
    for store in stores:
        store.start()
    scale_ref[...] = jnp.broadcast_to(scale, (128, 128))
    for store in stores:
        store.wait()


def project_kernel(k, *refs):
    (wk_ref, wv_ref, gain_ref), refs = refs[:3], refs[3:]
    older_hbm, pieces = refs[:k], refs[k : k + 2]
    rows_out, raw_ref, *hand, rows_ref, held, sem, older_ref, older_sem = refs[k + 2 :]
    for n in range(8):
        for at in range(k):
            columns = slice(640 * n, 640 * n + 640)
            pltpu.make_async_copy(
                older_hbm[at].at[:, columns], older_ref.at[at, :, columns], older_sem.at[at, n]
            ).start()
    loads = load_keys(wk_ref, wv_ref, held, sem)

    def one_part(n, sums):
        at = pl.ds(pl.multiple_of(n * 640, 640), 640)
        newest = jnp.concatenate([piece[:, at] for piece in pieces], axis=0)
        rows_ref[:, at] = newest
        newest = newest.astype(F32)
        inverse = 1.0 / gain_ref[:, at]
        weighed = newest * (inverse * inverse)
        sums = list(sums)
        for old in range(k):
            pltpu.make_async_copy(
                older_hbm[old].at[:, at], older_ref.at[old, :, at], older_sem.at[old, n]
            ).wait()
            other = older_ref[old, :, at].astype(F32)
            sums[old] = sums[old] + jnp.sum(weighed * other, axis=1, keepdims=True)
        sums[k] = sums[k] + jnp.sum(weighed * newest, axis=1, keepdims=True)
        return tuple(sums)

    sums = lax.fori_loop(0, 8, one_part, tuple(jnp.zeros((128, 1), F32) for _ in range(k + 1)))
    keep = pltpu.make_async_copy(rows_ref, rows_out, sem.at[2])
    keep.start()
    lane = lax.broadcasted_iota(jnp.int32, (1, 128), 1)
    raw_ref[:, 256:] = functools.reduce(
        lambda a, b: a + b, [jnp.where(lane == at, value, 0.0) for at, value in enumerate(sums)]
    )
    for load in loads:
        load.wait()
    raw = jnp.dot(rows_ref[...], held[...], preferred_element_type=F32)
    raw_ref[:, :256] = raw
    if k == 0:
        scale_ref, kv_ref, kv_held = hand
        hand_out(raw, sums[0], scale_ref, kv_ref, kv_held, sem)
    keep.wait()


def share_kernel(k, *refs):
    raws, (share_ref, scale_ref, kv_ref, kv_held, sem) = refs[k : 2 * k + 1], refs[2 * k + 1 :]
    shares = mix_shares(k, refs[:k])
    lane = lax.broadcasted_iota(jnp.int32, (1, 128), 1)
    share_ref[...] = functools.reduce(
        lambda a, b: a + b, [jnp.where(lane == at, share, 0.0) for at, share in enumerate(shares)]
    )
    squares = jnp.zeros((128, 1), F32)
    for at in range(k + 1):
        for other in range(at + 1):
            twice = 1.0 if other == at else 2.0
            pair = raws[at][:, 256 + other : 257 + other]
            squares = squares + (twice * shares[at] * shares[other]) * pair
    raw = functools.reduce(
        lambda a, b: a + b, [share * raws[at][:, :256] for at, share in enumerate(shares)]
    )
    hand_out(raw, jnp.maximum(squares, 0.0), scale_ref, kv_ref, kv_held, sem)


def take_share(share_ref, at):
    lane = lax.broadcasted_iota(jnp.int32, (1, 128), 1)
    return jnp.sum(jnp.where(lane == at, share_ref[...], 0.0), axis=1, keepdims=True)


def query_kernel(k, *refs):
    if k > 0:
        share_ref, refs = refs[0], refs[1:]
    parts, (w_ref, q_ref, acc) = refs[: k + 1], refs[k + 1 :]

    @pl.when(pl.program_id(0) == 0)
    def _():
        acc[...] = jnp.zeros_like(acc)

    if k == 0:
        rows = parts[0][...]
    else:
        rows = functools.reduce(
            lambda a, b: a + b,
            [take_share(share_ref, at) * part[...].astype(F32) for at, part in enumerate(parts)],
        ).astype(BF16)
    acc[...] += jnp.dot(rows, w_ref[...], preferred_element_type=F32)

    @pl.when(pl.program_id(0) == 4)
    def _():
        q_ref[...] = acc[...].astype(BF16)


def query_dot(share, parts, w_query):
    return pl.pallas_call(
        functools.partial(query_kernel, len(parts) - 1),
        grid=(5,),
        out_shape=pltpu.VMEM((128, 640), BF16),
        in_specs=[pl.BlockSpec((1, 128), lambda n: (0, 0))] * (len(parts) > 1)
        + [pl.BlockSpec((128, 1024), lambda n: (0, n))] * len(parts)
        + [pl.BlockSpec((1024, 640), lambda n: (n, 0))],
        out_specs=pl.BlockSpec((128, 640), lambda n: (0, 0)),
        scratch_shapes=[pltpu.VMEM((128, 640), F32)],
        compiler_params=pltpu.CompilerParams(vmem_limit_bytes=10 * 1024 * 1024),
        cost_estimate=pl.CostEstimate(
            flops=2 * 128 * D * 640, bytes_accessed=8_000_000, transcendentals=0
        ),
    )(*([share] if len(parts) > 1 else []), *[pltpu.with_memory_space_constraint(part, pltpu.HBM) for part in (*parts, w_query)])


def attend_kernel(
    q_ref, scale_ref, kv_ref, w_ref, own_ref, send_ref, w_held, attended, sem
):
    load = pltpu.make_async_copy(w_ref, w_held, sem)
    load.start()
    s = lax.axis_index("x") * 4 + lax.axis_index("z")
    row_at = s * 128 + row_offset(lax.broadcasted_iota(jnp.int32, (128, 1), 0))
    column_at = row_offset(lax.broadcasted_iota(jnp.int32, (1, 128), 1))
    allowed = row_at >= jnp.concatenate([128 * n + column_at for n in range(16)], axis=1)
    factor = scale_ref[:, :1] * (SCORE_SCALE / math.log(2.0))

    def one_head(g, carry):
        at = pl.ds(pl.multiple_of(g * HEAD_DIM, HEAD_DIM), HEAD_DIM)
        keys = kv_ref[:, :, :HEAD_DIM].reshape(TOKENS, HEAD_DIM)
        values = kv_ref[:, :, HEAD_DIM:].reshape(TOKENS, HEAD_DIM)
        raw = lax.dot_general(
            q_ref[:, at], keys, (((1,), (1,)), ((), ())), preferred_element_type=F32
        )
        raw = jnp.where(allowed, raw, -1e30)
        weight = jnp.exp2((raw - jnp.max(raw, axis=1, keepdims=True)) * factor)
        row_sum = jnp.sum(weight, axis=1, keepdims=True)
        summed = jnp.dot(weight.astype(BF16), values, preferred_element_type=F32)
        attended[:, at] = (summed / row_sum).astype(BF16)
        return carry

    lax.fori_loop(0, GROUP, one_head, 0)
    load.wait()

    def one_part(n, carry):
        at = pl.ds(pl.multiple_of(n * 1280, 1280), 1280)
        part = jnp.dot(attended[...], w_held[:, at], preferred_element_type=F32)
        own_ref[:, at] = part[:64]
        send_ref[:, at] = part[64:].astype(BF16)
        return carry

    lax.fori_loop(0, 4, one_part, 0)


def home_copies(held, outs, at, sem, start):
    y, c = lax.axis_index("y"), lax.axis_index("c")
    copies = []
    for by in range(4):
        for half in range(2):
            column = (((y + by) % 4) * 2 + (c + half) % 2) * 640
            columns = pl.ds(pl.multiple_of(column, 640), 640)
            target = outs[half].at[at] if by == 0 else outs[1 + by].at[half, at]
            copies.append(
                pltpu.make_async_copy(held.at[:, columns], target, sem.at[start + 2 * by + half])
            )
    return copies


def finish_kernel(k, own_ref, a_ref, b_ref, d_ref, inj_ref, x_ref, gain_ref, gain_in_ref, *rest):
    older, rest = rest[:k], rest[k:]
    inj, x = inj_ref[...].astype(F32), x_ref[...].astype(F32)
    summed = (x + inj) + (
        own_ref[...] + a_ref[...].astype(F32) + b_ref[...].astype(F32) + d_ref[...].astype(F32)
    )
    scale = lax.rsqrt(jnp.sum(summed * summed, axis=1, keepdims=True) / D + EPS)
    image = summed * scale * gain_ref[...]
    residual = image - x
    copies = []
    if k >= 2:
        rest, (image_ref, residual_ref, sem) = rest[:-3], rest[-3:]
        rest = rest[5:] if k == ITERS - 1 else rest
        image_ref[...] = image
        copies = home_copies(image_ref, rest[:5], k % 2, sem, 3)
        rest = rest[5:]
        if k == 2:
            residual_ref[...] = residual
            copies.append(pltpu.make_async_copy(image_ref, rest[0], sem.at[1]))
            copies.append(pltpu.make_async_copy(residual_ref, rest[1], sem.at[2]))
            rest[2][...] = ((image + inj) * gain_in_ref[...]).astype(BF16)
            rest = rest[3:]
        for copy in copies:
            copy.start()
    else:
        rest[0][...] = image
        rest[1][...] = ((image + inj) * gain_in_ref[...]).astype(BF16)
        rest = rest[2:]
    if k > 0:
        table_out, dots_held = rest[0], rest[1]
        table_sem = sem.at[0] if k >= 2 else rest[2]
        lane = lax.broadcasted_iota(jnp.int32, (1, 128), 1)
        dots = jnp.where(lane == k, total(residual * residual), 0.0)
        for at, other in enumerate(older):
            dots = dots + jnp.where(lane == at, total(residual * other[...]), 0.0)
        if k == 1:
            dots = dots + jnp.where(lane == 7, total(older[0][...] * older[0][...]), 0.0)
        dots_held[...] = jnp.broadcast_to(dots.reshape(1, 1, 128), (128, 1, 128))
        copies.append(pltpu.make_async_copy(dots_held, table_out, table_sem))
        copies[-1].start()
    for copy in copies:
        copy.wait()


def store_kernel(k, image_ref, x_ref, *rest):
    rest = rest[5:] if k % 2 == 1 else rest
    (image_out, residual_out), home_out, (residual_ref, sem) = rest[:2], rest[2:7], rest[7:]
    copies = [pltpu.make_async_copy(image_ref, image_out, sem.at[0])]
    copies += home_copies(image_ref, home_out, k % 2, sem, 2)
    for copy in copies:
        copy.start()
    residual_ref[...] = image_ref[...] - x_ref[...].astype(F32)
    copies.append(pltpu.make_async_copy(residual_ref, residual_out, sem.at[1]))
    copies[-1].start()
    for copy in copies:
        copy.wait()


def solve_small(matrix, size_now):
    rows = [list(row) for row in matrix]
    values = [jnp.ones((1, 1), F32) for _ in range(size_now)]
    for pivot in range(size_now):
        for below in range(pivot + 1, size_now):
            ratio = rows[below][pivot] / rows[pivot][pivot]
            rows[below] = [b - ratio * p for b, p in zip(rows[below], rows[pivot])]
            values[below] = values[below] - ratio * values[pivot]
    result = [None] * size_now
    for pivot in reversed(range(size_now)):
        running = values[pivot]
        for later in range(pivot + 1, size_now):
            running = running - rows[pivot][later] * result[later]
        result[pivot] = running / rows[pivot][pivot]
    return result


def mix_shares(k, tables):
    if k == 0:
        return [1.0]
    lane = lax.broadcasted_iota(jnp.int32, (1, 128), 1)
    gram = {}
    for at, table in enumerate(tables):
        sums = jnp.sum(table[:, 0, :], axis=0, keepdims=True)
        for other in range(at + 2):
            gram[at + 1, other] = jnp.sum(jnp.where(lane == other, sums, 0.0), axis=1, keepdims=True)
        if at == 0:
            gram[0, 0] = jnp.sum(jnp.where(lane == 7, sums, 0.0), axis=1, keepdims=True)
    system = [
        [
            gram[max(i, j), min(i, j)] / float(TOKENS * D) + (LAMBDA if i == j else 0.0)
            for j in range(k + 1)
        ]
        for i in range(k + 1)
    ]
    unscaled = solve_small(system, k + 1)
    whole = functools.reduce(lambda a, b: a + b, unscaled)
    return [u / whole for u in unscaled]


def mix_kernel(share_ref, *refs):
    refs[-1][...] = functools.reduce(
        lambda a, b: a + b,
        [take_share(share_ref, at) * image[...] for at, image in enumerate(refs[:-1])],
    )


def last_kernel(k, *refs):
    shares = mix_shares(k, refs[:k])
    older, newest, (out_hbm, out_ref, sem) = refs[k : k + 5], refs[k + 5 : k + 10], refs[-3:]
    y, c = lax.axis_index("y"), lax.axis_index("c")

    def piece(home, by, half, at):
        if half == 1:
            return home[4][by, at]
        return home[0][at] if by == 0 else home[by][0, at]

    for by in range(4):
        for half in range(2):
            row = (((y - by + 4) % 4) * 2 + (c + half) % 2) * 16
            rows = pl.ds(pl.multiple_of(row, 16), 16)
            mixed = jnp.zeros((16, 640), F32)
            for at in range(k + 1):
                mixed = mixed + shares[at] * piece(older if at < 2 else newest, by, half, at % 2)
            out_ref[rows, :] = mixed
    store = pltpu.make_async_copy(out_ref, out_hbm, sem)
    store.start()
    store.wait()


def start_kernel(inj_hbm, warm_hbm, gain_hbm, payload_ref, *refs):
    home_refs, (inj_ref, warm_ref, gain_ref, sem) = refs[:5], refs[5:]
    loads = [
        pltpu.make_async_copy(gain_hbm, gain_ref, sem.at[2]),
        pltpu.make_async_copy(inj_hbm, inj_ref, sem.at[0]),
        pltpu.make_async_copy(warm_hbm, warm_ref, sem.at[1]),
    ]
    for load in loads:
        load.start()
    y, c = lax.axis_index("y"), lax.axis_index("c")
    for load in loads:
        load.wait()
    gain = gain_ref[:, pl.ds(pl.multiple_of((y * 2 + c) * 640, 640), 640)]
    inj, warm = inj_ref[...].astype(F32), warm_ref[...].astype(F32)
    payload_ref[...] = ((inj + warm) * gain).astype(BF16)
    for by in range(4):
        for half in range(2):
            row = (((y + by) % 4) * 2 + (c + half) % 2) * 16
            rows = pl.ds(pl.multiple_of(row, 16), 16)
            for at, source in enumerate((inj_ref, warm_ref)):
                if by == 0:
                    home_refs[half][at] = source[rows, :]
                else:
                    home_refs[1 + by][half, at] = source[rows, :]


def settle_kernel(*refs):
    inj_ref, warm_ref = refs[5:]
    y, c = lax.axis_index("y"), lax.axis_index("c")
    for by in range(4):
        for half in range(2):
            column = (((y - by + 4) % 4) * 2 + (c + half) % 2) * 640
            columns = pl.ds(pl.multiple_of(column, 640), 640)
            for at, target in enumerate((inj_ref, warm_ref)):
                if half == 1:
                    target[:, columns] = refs[4][by, at]
                else:
                    target[:, columns] = refs[0][at] if by == 0 else refs[by][0, at]


def move_home(pieces):
    own, pair, *far = pieces
    near = []
    for by, piece in enumerate(far):
        near.append(lax.ppermute(piece, "y", shift(4, by + 1)))
    joined = jnp.stack([pair] + [piece[1] for piece in near])
    return [own, *near, lax.ppermute(joined, "c", shift(2, 1))]


def on_device(injection, warm_start, gain_in, gain_out, w_query, w_key, w_value, w_out):
    gain_in, gain_out = gain_in.reshape(1, D), gain_out.reshape(1, D)
    tokens = pltpu.HBM((16, D), F32)
    wide = pltpu.VMEM((16, D), F32)
    narrow = pltpu.VMEM((16, D), BF16)
    home_narrow = [pltpu.VMEM((2, 16, 640), BF16)] * 2 + [pltpu.VMEM((2, 2, 16, 640), BF16)] * 3
    home_packed = [pltpu.HBM((2, 16, 640), F32)] * 2 + [pltpu.HBM((2, 2, 16, 640), F32)] * 3
    payload, *home = call(
        start_kernel,
        (pltpu.VMEM((128, 640), BF16), *home_narrow),
        injection,
        warm_start,
        gain_in,
        specs=[HBM, HBM, HBM],
        scratch=[
            pltpu.VMEM((128, 640), BF16),
            pltpu.VMEM((128, 640), BF16),
            pltpu.VMEM((1, D), F32),
            pltpu.SemaphoreType.DMA((3,)),
        ],
    )
    settled = []
    images, residuals, parts, tables, dots = [], [], [], [], None
    raws, share = [], None
    rows_out = pltpu.HBM((128, D), BF16)
    raw_out = pltpu.VMEM((128, 384), F32)
    hand_outs = [pltpu.VMEM((128, 128), F32), pltpu.HBM((16, 128, 2 * HEAD_DIM), BF16)]
    kv_scratch = pltpu.VMEM((128, 2 * HEAD_DIM), BF16)
    project_scratch = [pltpu.VMEM((128, D), BF16), pltpu.VMEM((D, 2 * HEAD_DIM), BF16)]
    many = pltpu.SemaphoreType.DMA((19,))
    for k in range(ITERS):
        pieces = [payload]
        for by in (1, 2, 3):
            pieces.append(lax.ppermute(payload, "y", shift(4, by)))
        if dots is not None:
            tables.append(lax.all_to_all(dots, EVERY, split_axis=0, concat_axis=0, tiled=True))
        mine = jnp.stack(pieces) if k == 0 else jnp.concatenate(pieces, axis=0)
        pieces = [mine, lax.ppermute(mine, "c", shift(2, 1))]
        if k == 1:
            parts, raws = [], []
        if k == 0:
            rows, scale, kv = call(
                first_kernel,
                [rows_out, *hand_outs],
                w_key,
                w_value,
                gain_in,
                *pieces,
                specs=[HBM] * 2 + [VMEM] * 3,
                vmem=8,
                scratch=[*project_scratch, kv_scratch, many],
                flops=2 * 128 * D * 256,
                touched=4_000_000,
            )
        else:
            rows, raw, *hand = call(
                functools.partial(project_kernel, k - 1),
                [rows_out, raw_out] + (hand_outs if k == 1 else []),
                w_key,
                w_value,
                gain_in,
                *parts,
                *pieces,
                specs=[HBM] * 2 + [VMEM] + [HBM] * len(parts) + [VMEM] * 2,
                vmem=10,
                scratch=([kv_scratch] if k == 1 else [])
                + project_scratch
                + [
                    many,
                    pltpu.VMEM((k - 1, 128, D) if k > 1 else (1, 8, 128), BF16),
                    pltpu.SemaphoreType.DMA((max(k - 1, 1), 8)),
                ],
                flops=2 * 128 * D * 256,
                touched=4_000_000,
            )
            raws.append(raw)
        parts.append(rows)
        if k == 1:
            scale, kv = hand
        if k > 1:
            share, scale, kv = call(
                functools.partial(share_kernel, len(parts) - 1),
                [pltpu.VMEM((1, 128), F32), *hand_outs],
                *tables,
                *raws,
                vmem=4,
                scratch=[kv_scratch, many],
            )
        kv_all = lax.all_to_all(kv, SEQ, split_axis=0, concat_axis=0, tiled=True)
        q = query_dot(share, parts, w_query)
        if k in (0, 2):
            home = move_home(home)
            kv_all, home = lax.optimization_barrier((kv_all, home))
        if k == 0:
            inj, current = call(settle_kernel, (narrow, narrow), *home)
        if k == 2:
            settled = home
        if k > 1:
            current = call(mix_kernel, wide, share, *images)
        own, send = call(
            attend_kernel,
            (pltpu.VMEM((64, D), F32), pltpu.VMEM((64, D), BF16)),
            q,
            scale,
            kv_all,
            w_out,
            specs=[VMEM, VMEM, VMEM, HBM],
            vmem=16,
            scratch=[
                pltpu.VMEM((640, D), BF16),
                pltpu.VMEM((128, 640), BF16),
                pltpu.SemaphoreType.DMA,
            ],
            flops=2 * 128 * 640 * (2 * TOKENS + D),
            touched=9_000_000,
        )
        pair = own + lax.ppermute(send, "c", shift(2, 1)).astype(F32)
        arrived = []
        for by in (1, 2, 3):
            piece = pair[16 * by : 16 * by + 16].astype(BF16)
            arrived.append(lax.ppermute(piece, "y", shift(4, -by)))
        last = k == ITERS - 1
        shapes = [*home_packed, *([] if last else [tokens, tokens, narrow])] if k >= 2 else [wide, narrow]
        scratch = []
        if k > 0:
            shapes.append(pltpu.HBM((128, 1, 128), F32))
            scratch.append(pltpu.VMEM((128, 1, 128), F32))
        if k == 1:
            scratch.append(pltpu.SemaphoreType.DMA)
        if k >= 2:
            scratch += [pltpu.VMEM((16, D), F32)] * 2 + [pltpu.SemaphoreType.DMA((11,))]
        packed = list(home) if last else []
        outs = call(
            functools.partial(finish_kernel, k),
            tuple(shapes),
            pair[:16],
            *arrived,
            inj,
            current,
            gain_out,
            gain_in,
            *residuals,
            *packed,
            specs=[VMEM] * (8 + len(residuals)) + [HBM] * len(packed),
            aliases={8 + k + at: at for at in range(len(packed))},
            scratch=scratch,
        )
        dots = outs[-1] if k > 0 else None
        if k >= 2:
            home = outs[:5]
        if k == 2:
            image, residual, payload = outs[5:8]
            images.append(image)
            residuals.append(residual)
        if k < 2:
            image, payload = outs[:2]
        if k < 2:
            packed = list(home) if k % 2 == 1 else []
            outs = call(
                functools.partial(store_kernel, k),
                (tokens, tokens, *home_packed),
                image,
                current,
                *packed,
                specs=[VMEM] * 2 + [HBM] * len(packed),
                aliases={2 + at: 2 + at for at in range(len(packed))},
                scratch=[pltpu.VMEM((16, D), F32), pltpu.SemaphoreType.DMA((10,))],
            )
            images.append(outs[0])
            residuals.append(outs[1])
            home = outs[2:7]
            if k == 0:
                current = outs[0]
    settled = settled + move_home(home)
    tables.append(lax.all_to_all(dots, EVERY, split_axis=0, concat_axis=0, tiled=True))
    return call(
        functools.partial(last_kernel, ITERS - 1),
        pltpu.HBM((128, 640), F32),
        *tables,
        *settled,
        scratch=[pltpu.VMEM((128, 640), F32), pltpu.SemaphoreType.DMA],
    )


def solution(mesh):
    split = Mesh(mesh.devices.reshape(4, 4, 4, 2), EVERY)
    placed = (
        P(SEQ, FEAT),
        P(SEQ, FEAT),
        P(),
        P(),
        P(None, FEAT),
        P(None, FEAT),
        P(None, FEAT),
        P(FEAT, None),
    )
    return jax.shard_map(
        on_device, mesh=split, in_specs=placed, out_specs=P(SEQ, FEAT), check_vma=False
    )
```

```python
import functools
import math

import jax
import jax.numpy as jnp
from jax import lax
from jax.experimental import pallas as pl
from jax.experimental.pallas import tpu as pltpu
from jax.sharding import Mesh
from jax.sharding import PartitionSpec as P


D = 5120
HEADS = 40
KV_HEADS = 8
HEAD_DIM = 128
GROUP = HEADS // KV_HEADS
ITERS = 4
TOKENS = 2048
SEQ = ("x", "z")
FEAT = ("y", "c")
EVERY = ("x", "z", "y", "c")
EPS = 1e-06
LAMBDA = 0.03
SCORE_SCALE = 1.0 / math.sqrt(HEAD_DIM)
F32 = jnp.float32
BF16 = jnp.bfloat16

VMEM = pl.BlockSpec(memory_space=pltpu.VMEM)
HBM = pl.BlockSpec(memory_space=pltpu.HBM)


def shift(n, by):
    return [(at, (at + by) % n) for at in range(n)]


def call(kernel, outs, *args, specs=None, scratch=(), vmem=8, flops=0, touched=0, aliases=None):
    specs = [VMEM] * len(args) if specs is None else specs
    args = [
        pltpu.with_memory_space_constraint(arg, pltpu.HBM) if spec is HBM else arg
        for arg, spec in zip(args, specs)
    ]
    return pl.pallas_call(
        kernel,
        out_shape=outs,
        in_specs=specs,
        input_output_aliases=aliases or {},
        out_specs=jax.tree.map(lambda out: HBM if out.memory_space == pltpu.HBM else VMEM, outs),
        scratch_shapes=list(scratch),
        compiler_params=pltpu.CompilerParams(vmem_limit_bytes=vmem * 1024 * 1024),
        cost_estimate=pl.CostEstimate(flops=flops, bytes_accessed=touched, transcendentals=0),
    )(*args)


def total(x):
    return jnp.sum(jnp.sum(x, axis=1, keepdims=True), axis=0, keepdims=True)


def row_offset(row):
    y, c = lax.axis_index("y"), lax.axis_index("c")
    half, block, inner = row // 64, (row // 16) % 4, row % 16
    return (((y - block + 4) % 4) * 2 + (c + half) % 2) * 16 + inner


def load_keys(wk_ref, wv_ref, held, sem):
    copies = [
        pltpu.make_async_copy(wk_ref, held.at[:, :HEAD_DIM], sem.at[0]),
        pltpu.make_async_copy(wv_ref, held.at[:, HEAD_DIM:], sem.at[1]),
    ]
    for copy in copies:
        copy.start()
    return copies


def fetch_kernel(wk_ref, wv_ref, payload_ref, held, sem):
    for load in load_keys(wk_ref, wv_ref, held, sem):
        load.wait()


def first_kernel(w_ref, gain_ref, *refs):
    pieces, (rows_out, scale_ref, kv_ref, rows_ref, kv_held, sem) = refs[:2], refs[2:]
    y, c = lax.axis_index("y"), lax.axis_index("c")
    for half in range(2):
        for block in range(4):
            column = (((y - block + 4) % 4) * 2 + (c + half) % 2) * 640
            columns = pl.ds(pl.multiple_of(column, 640), 640)
            for at in range(8):
                source = pl.multiple_of(row_offset(16 * at), 16)
                rows_ref[16 * at : 16 * at + 16, columns] = pieces[half][block, pl.ds(source, 16), :]
    keep = pltpu.make_async_copy(rows_ref, rows_out, sem.at[2])
    keep.start()

    def one_part(n, squares):
        at = pl.ds(pl.multiple_of(n * 640, 640), 640)
        part = rows_ref[:, at].astype(F32) * (1.0 / gain_ref[:, at])
        return squares + jnp.sum(part * part, axis=1, keepdims=True)

    squares = lax.fori_loop(0, 8, one_part, jnp.zeros((128, 1), F32))
    raw = jnp.dot(rows_ref[...], w_ref[...], preferred_element_type=F32)
    hand_out(raw, squares, scale_ref, kv_ref, kv_held, sem)
    keep.wait()


def hand_out(raw, squares, scale_ref, kv_ref, kv_held, sem):
    scale = lax.rsqrt(squares / D + EPS)
    kv_held[...] = (raw * scale).astype(BF16)
    stores = [pltpu.make_async_copy(kv_held, kv_ref.at[at], sem.at[3 + at]) for at in range(16)]
    for store in stores:
        store.start()
    scale_ref[...] = jnp.broadcast_to(scale, (128, 128))
    for store in stores:
        store.wait()


def project_kernel(k, *refs):
    weights, refs = (refs[:2], refs[2:]) if k > 0 else (refs[:1], refs[1:])
    gain_ref, refs = refs[0], refs[1:]
    older_hbm, pieces = refs[:k], refs[k : k + 2]
    rows_out, raw_ref, *hand, rows_ref, sem, older_ref, older_sem = refs[k + 2 :]
    held = hand[-1] if k > 0 else weights[0]
    for n in range(8):
        for at in range(k):
            columns = slice(640 * n, 640 * n + 640)
            pltpu.make_async_copy(
                older_hbm[at].at[:, columns], older_ref.at[at, :, columns], older_sem.at[at, n]
            ).start()
    loads = load_keys(*weights, held, sem) if k > 0 else []

    def one_part(n, sums):
        at = pl.ds(pl.multiple_of(n * 640, 640), 640)
        newest = jnp.concatenate([piece[:, at] for piece in pieces], axis=0)
        rows_ref[:, at] = newest
        newest = newest.astype(F32)
        inverse = 1.0 / gain_ref[:, at]
        weighed = newest * (inverse * inverse)
        sums = list(sums)
        for old in range(k):
            pltpu.make_async_copy(
                older_hbm[old].at[:, at], older_ref.at[old, :, at], older_sem.at[old, n]
            ).wait()
            other = older_ref[old, :, at].astype(F32)
            sums[old] = sums[old] + jnp.sum(weighed * other, axis=1, keepdims=True)
        sums[k] = sums[k] + jnp.sum(weighed * newest, axis=1, keepdims=True)
        return tuple(sums)

    sums = lax.fori_loop(0, 8, one_part, tuple(jnp.zeros((128, 1), F32) for _ in range(k + 1)))
    keep = pltpu.make_async_copy(rows_ref, rows_out, sem.at[2])
    keep.start()
    lane = lax.broadcasted_iota(jnp.int32, (1, 128), 1)
    raw_ref[:, 256:] = functools.reduce(
        lambda a, b: a + b, [jnp.where(lane == at, value, 0.0) for at, value in enumerate(sums)]
    )
    for load in loads:
        load.wait()
    raw = jnp.dot(rows_ref[...], held[...], preferred_element_type=F32)
    raw_ref[:, :256] = raw
    if k == 0:
        scale_ref, kv_ref, kv_held = hand
        hand_out(raw, sums[0], scale_ref, kv_ref, kv_held, sem)
    keep.wait()


def share_kernel(k, *refs):
    raws, (share_ref, scale_ref, kv_ref, kv_held, sem) = refs[k : 2 * k + 1], refs[2 * k + 1 :]
    shares = mix_shares(k, refs[:k])
    lane = lax.broadcasted_iota(jnp.int32, (1, 128), 1)
    share_ref[...] = functools.reduce(
        lambda a, b: a + b, [jnp.where(lane == at, share, 0.0) for at, share in enumerate(shares)]
    )
    squares = jnp.zeros((128, 1), F32)
    for at in range(k + 1):
        for other in range(at + 1):
            twice = 1.0 if other == at else 2.0
            pair = raws[at][:, 256 + other : 257 + other]
            squares = squares + (twice * shares[at] * shares[other]) * pair
    raw = functools.reduce(
        lambda a, b: a + b, [share * raws[at][:, :256] for at, share in enumerate(shares)]
    )
    hand_out(raw, jnp.maximum(squares, 0.0), scale_ref, kv_ref, kv_held, sem)


def take_share(share_ref, at):
    lane = lax.broadcasted_iota(jnp.int32, (1, 128), 1)
    return jnp.sum(jnp.where(lane == at, share_ref[...], 0.0), axis=1, keepdims=True)


def query_kernel(k, *refs):
    if k > 0:
        share_ref, refs = refs[0], refs[1:]
    parts, (w_ref, q_ref, acc) = refs[: k + 1], refs[k + 1 :]

    @pl.when(pl.program_id(0) == 0)
    def _():
        acc[...] = jnp.zeros_like(acc)

    if k == 0:
        rows = parts[0][...]
    else:
        rows = functools.reduce(
            lambda a, b: a + b,
            [take_share(share_ref, at) * part[...].astype(F32) for at, part in enumerate(parts)],
        ).astype(BF16)
    acc[...] += jnp.dot(rows, w_ref[...], preferred_element_type=F32)

    @pl.when(pl.program_id(0) == 4)
    def _():
        q_ref[...] = acc[...].astype(BF16)


def query_dot(share, parts, w_query):
    return pl.pallas_call(
        functools.partial(query_kernel, len(parts) - 1),
        grid=(5,),
        out_shape=pltpu.VMEM((128, 640), BF16),
        in_specs=[pl.BlockSpec((1, 128), lambda n: (0, 0))] * (len(parts) > 1)
        + [pl.BlockSpec((128, 1024), lambda n: (0, n))] * len(parts)
        + [pl.BlockSpec((1024, 640), lambda n: (n, 0))],
        out_specs=pl.BlockSpec((128, 640), lambda n: (0, 0)),
        scratch_shapes=[pltpu.VMEM((128, 640), F32)],
        compiler_params=pltpu.CompilerParams(vmem_limit_bytes=10 * 1024 * 1024),
        cost_estimate=pl.CostEstimate(
            flops=2 * 128 * D * 640, bytes_accessed=8_000_000, transcendentals=0
        ),
    )(*([share] if len(parts) > 1 else []), *[pltpu.with_memory_space_constraint(part, pltpu.HBM) for part in (*parts, w_query)])


def attend_kernel(
    q_ref, scale_ref, kv_ref, w_ref, own_ref, send_ref, w_held, attended, sem
):
    load = pltpu.make_async_copy(w_ref, w_held, sem)
    load.start()
    s = lax.axis_index("x") * 4 + lax.axis_index("z")
    row_at = s * 128 + row_offset(lax.broadcasted_iota(jnp.int32, (128, 1), 0))
    column_at = row_offset(lax.broadcasted_iota(jnp.int32, (1, 128), 1))
    allowed = row_at >= jnp.concatenate([128 * n + column_at for n in range(16)], axis=1)
    factor = scale_ref[:, :1] * (SCORE_SCALE / math.log(2.0))

    def one_head(g, carry):
        at = pl.ds(pl.multiple_of(g * HEAD_DIM, HEAD_DIM), HEAD_DIM)
        keys = kv_ref[:, :, :HEAD_DIM].reshape(TOKENS, HEAD_DIM)
        values = kv_ref[:, :, HEAD_DIM:].reshape(TOKENS, HEAD_DIM)
        raw = lax.dot_general(
            q_ref[:, at], keys, (((1,), (1,)), ((), ())), preferred_element_type=F32
        )
        raw = jnp.where(allowed, raw, -1e30)
        weight = jnp.exp2((raw - jnp.max(raw, axis=1, keepdims=True)) * factor)
        row_sum = jnp.sum(weight, axis=1, keepdims=True)
        summed = jnp.dot(weight.astype(BF16), values, preferred_element_type=F32)
        attended[:, at] = (summed / row_sum).astype(BF16)
        return carry

    lax.fori_loop(0, GROUP, one_head, 0)
    load.wait()

    def one_part(n, carry):
        at = pl.ds(pl.multiple_of(n * 1280, 1280), 1280)
        part = jnp.dot(attended[...], w_held[:, at], preferred_element_type=F32)
        own_ref[:, at] = part[:64]
        send_ref[:, at] = part[64:].astype(BF16)
        return carry

    lax.fori_loop(0, 4, one_part, 0, unroll=2)


def home_copies(held, outs, at, sem, start):
    y, c = lax.axis_index("y"), lax.axis_index("c")
    copies = []
    for by in range(4):
        for half in range(2):
            column = (((y + by) % 4) * 2 + (c + half) % 2) * 640
            columns = pl.ds(pl.multiple_of(column, 640), 640)
            target = outs[half].at[at] if by == 0 else outs[1 + by].at[half, at]
            copies.append(
                pltpu.make_async_copy(held.at[:, columns], target, sem.at[start + 2 * by + half])
            )
    return copies


def finish_kernel(k, own_ref, a_ref, b_ref, d_ref, inj_ref, x_ref, gain_ref, gain_in_ref, *rest):
    older, rest = rest[:k], rest[k:]
    inj, x = inj_ref[...].astype(F32), x_ref[...].astype(F32)
    summed = (x + inj) + (
        own_ref[...] + a_ref[...].astype(F32) + b_ref[...].astype(F32) + d_ref[...].astype(F32)
    )
    scale = lax.rsqrt(jnp.sum(summed * summed, axis=1, keepdims=True) / D + EPS)
    image = summed * scale * gain_ref[...]
    residual = image - x
    copies = []
    if k >= 2:
        rest, (image_ref, residual_ref, sem) = rest[:-3], rest[-3:]
        rest = rest[5:] if k == ITERS - 1 else rest
        image_ref[...] = image
        copies = home_copies(image_ref, rest[:5], k % 2, sem, 3)
        rest = rest[5:]
        if k == 2:
            residual_ref[...] = residual
            copies.append(pltpu.make_async_copy(image_ref, rest[0], sem.at[1]))
            copies.append(pltpu.make_async_copy(residual_ref, rest[1], sem.at[2]))
            rest[2][...] = ((image + inj) * gain_in_ref[...]).astype(BF16)
            rest = rest[3:]
        for copy in copies:
            copy.start()
    else:
        rest[0][...] = image
        rest[1][...] = ((image + inj) * gain_in_ref[...]).astype(BF16)
        rest = rest[2:]
    if k > 0:
        table_out, dots_held = rest[0], rest[1]
        table_sem = sem.at[0] if k >= 2 else rest[2]
        lane = lax.broadcasted_iota(jnp.int32, (1, 128), 1)
        dots = jnp.where(lane == k, total(residual * residual), 0.0)
        for at, other in enumerate(older):
            dots = dots + jnp.where(lane == at, total(residual * other[...]), 0.0)
        if k == 1:
            dots = dots + jnp.where(lane == 7, total(older[0][...] * older[0][...]), 0.0)
        dots_held[...] = jnp.broadcast_to(dots.reshape(1, 1, 128), (128, 1, 128))
        copies.append(pltpu.make_async_copy(dots_held, table_out, table_sem))
        copies[-1].start()
    for copy in copies:
        copy.wait()


def store_kernel(k, image_ref, x_ref, *rest):
    rest = rest[5:] if k % 2 == 1 else rest
    (image_out, residual_out), home_out, (residual_ref, sem) = rest[:2], rest[2:7], rest[7:]
    copies = [pltpu.make_async_copy(image_ref, image_out, sem.at[0])]
    copies += home_copies(image_ref, home_out, k % 2, sem, 2)
    for copy in copies:
        copy.start()
    residual_ref[...] = image_ref[...] - x_ref[...].astype(F32)
    copies.append(pltpu.make_async_copy(residual_ref, residual_out, sem.at[1]))
    copies[-1].start()
    for copy in copies:
        copy.wait()


def solve_small(matrix, size_now):
    rows = [list(row) for row in matrix]
    values = [jnp.ones((1, 1), F32) for _ in range(size_now)]
    for pivot in range(size_now):
        for below in range(pivot + 1, size_now):
            ratio = rows[below][pivot] / rows[pivot][pivot]
            rows[below] = [b - ratio * p for b, p in zip(rows[below], rows[pivot])]
            values[below] = values[below] - ratio * values[pivot]
    result = [None] * size_now
    for pivot in reversed(range(size_now)):
        running = values[pivot]
        for later in range(pivot + 1, size_now):
            running = running - rows[pivot][later] * result[later]
        result[pivot] = running / rows[pivot][pivot]
    return result


def mix_shares(k, tables):
    if k == 0:
        return [1.0]
    lane = lax.broadcasted_iota(jnp.int32, (1, 128), 1)
    gram = {}
    for at, table in enumerate(tables):
        sums = jnp.sum(table[:, 0, :], axis=0, keepdims=True)
        for other in range(at + 2):
            gram[at + 1, other] = jnp.sum(jnp.where(lane == other, sums, 0.0), axis=1, keepdims=True)
        if at == 0:
            gram[0, 0] = jnp.sum(jnp.where(lane == 7, sums, 0.0), axis=1, keepdims=True)
    system = [
        [
            gram[max(i, j), min(i, j)] / float(TOKENS * D) + (LAMBDA if i == j else 0.0)
            for j in range(k + 1)
        ]
        for i in range(k + 1)
    ]
    unscaled = solve_small(system, k + 1)
    whole = functools.reduce(lambda a, b: a + b, unscaled)
    return [u / whole for u in unscaled]


def mix_kernel(share_ref, *refs):
    refs[-1][...] = functools.reduce(
        lambda a, b: a + b,
        [take_share(share_ref, at) * image[...] for at, image in enumerate(refs[:-1])],
    )


def last_kernel(k, *refs):
    shares = mix_shares(k, refs[:k])
    older, newest, (out_hbm, out_ref, sem) = refs[k : k + 5], refs[k + 5 : k + 10], refs[-3:]
    y, c = lax.axis_index("y"), lax.axis_index("c")

    def piece(home, by, half, at):
        if half == 1:
            return home[4][by, at]
        return home[0][at] if by == 0 else home[by][0, at]

    for by in range(4):
        for half in range(2):
            row = (((y - by + 4) % 4) * 2 + (c + half) % 2) * 16
            rows = pl.ds(pl.multiple_of(row, 16), 16)
            mixed = jnp.zeros((16, 640), F32)
            for at in range(k + 1):
                mixed = mixed + shares[at] * piece(older if at < 2 else newest, by, half, at % 2)
            out_ref[rows, :] = mixed
    store = pltpu.make_async_copy(out_ref, out_hbm, sem)
    store.start()
    store.wait()


def start_kernel(inj_hbm, warm_hbm, gain_hbm, payload_ref, *refs):
    home_refs, (inj_ref, warm_ref, gain_ref, sem) = refs[:5], refs[5:]
    loads = [
        pltpu.make_async_copy(gain_hbm, gain_ref, sem.at[2]),
        pltpu.make_async_copy(inj_hbm, inj_ref, sem.at[0]),
        pltpu.make_async_copy(warm_hbm, warm_ref, sem.at[1]),
    ]
    for load in loads:
        load.start()
    y, c = lax.axis_index("y"), lax.axis_index("c")
    for load in loads:
        load.wait()
    gain = gain_ref[:, pl.ds(pl.multiple_of((y * 2 + c) * 640, 640), 640)]
    inj, warm = inj_ref[...].astype(F32), warm_ref[...].astype(F32)
    payload_ref[...] = ((inj + warm) * gain).astype(BF16)
    for by in range(4):
        for half in range(2):
            row = (((y + by) % 4) * 2 + (c + half) % 2) * 16
            rows = pl.ds(pl.multiple_of(row, 16), 16)
            for at, source in enumerate((inj_ref, warm_ref)):
                if by == 0:
                    home_refs[half][at] = source[rows, :]
                else:
                    home_refs[1 + by][half, at] = source[rows, :]


def settle_kernel(*refs):
    inj_ref, warm_ref = refs[5:]
    y, c = lax.axis_index("y"), lax.axis_index("c")
    for by in range(4):
        for half in range(2):
            column = (((y - by + 4) % 4) * 2 + (c + half) % 2) * 640
            columns = pl.ds(pl.multiple_of(column, 640), 640)
            for at, target in enumerate((inj_ref, warm_ref)):
                if half == 1:
                    target[:, columns] = refs[4][by, at]
                else:
                    target[:, columns] = refs[0][at] if by == 0 else refs[by][0, at]


def move_home(pieces):
    own, pair, *far = pieces
    near = []
    for by, piece in enumerate(far):
        near.append(lax.ppermute(piece, "y", shift(4, by + 1)))
    joined = jnp.stack([pair] + [piece[1] for piece in near])
    return [own, *near, lax.ppermute(joined, "c", shift(2, 1))]


def on_device(injection, warm_start, gain_in, gain_out, w_query, w_key, w_value, w_out):
    gain_in, gain_out = gain_in.reshape(1, D), gain_out.reshape(1, D)
    tokens = pltpu.HBM((16, D), F32)
    wide = pltpu.VMEM((16, D), F32)
    narrow = pltpu.VMEM((16, D), BF16)
    home_narrow = [pltpu.VMEM((2, 16, 640), BF16)] * 2 + [pltpu.VMEM((2, 2, 16, 640), BF16)] * 3
    home_packed = [pltpu.HBM((2, 16, 640), F32)] * 2 + [pltpu.HBM((2, 2, 16, 640), F32)] * 3
    payload, *home = call(
        start_kernel,
        (pltpu.VMEM((128, 640), BF16), *home_narrow),
        injection,
        warm_start,
        gain_in,
        specs=[HBM, HBM, HBM],
        scratch=[
            pltpu.VMEM((128, 640), BF16),
            pltpu.VMEM((128, 640), BF16),
            pltpu.VMEM((1, D), F32),
            pltpu.SemaphoreType.DMA((3,)),
        ],
    )
    settled = []
    images, residuals, parts, tables, dots = [], [], [], [], None
    raws, share = [], None
    rows_out = pltpu.HBM((128, D), BF16)
    raw_out = pltpu.VMEM((128, 384), F32)
    hand_outs = [pltpu.VMEM((128, 128), F32), pltpu.HBM((16, 128, 2 * HEAD_DIM), BF16)]
    kv_scratch = pltpu.VMEM((128, 2 * HEAD_DIM), BF16)
    rows_scratch = pltpu.VMEM((128, D), BF16)
    key_scratch = pltpu.VMEM((D, 2 * HEAD_DIM), BF16)
    many = pltpu.SemaphoreType.DMA((19,))
    for k in range(ITERS):
        pieces = [payload]
        for by in (1, 2, 3):
            pieces.append(lax.ppermute(payload, "y", shift(4, by)))
        if dots is not None:
            tables.append(lax.all_to_all(dots, EVERY, split_axis=0, concat_axis=0, tiled=True))
        if k < 2:
            fetched = call(
                fetch_kernel,
                pltpu.VMEM((D, 2 * HEAD_DIM), BF16),
                w_key,
                w_value,
                payload,
                specs=[HBM, HBM, VMEM],
                vmem=2,
                scratch=[pltpu.SemaphoreType.DMA((2,))],
            )
        mine = jnp.stack(pieces) if k == 0 else jnp.concatenate(pieces, axis=0)
        pieces = [mine, lax.ppermute(mine, "c", shift(2, 1))]
        if k == 1:
            parts, raws = [], []
        if k == 0:
            rows, scale, kv = call(
                first_kernel,
                [rows_out, *hand_outs],
                fetched,
                gain_in,
                *pieces,
                vmem=8,
                scratch=[rows_scratch, kv_scratch, many],
                flops=2 * 128 * D * 256,
                touched=4_000_000,
            )
        else:
            rows, raw, *hand = call(
                functools.partial(project_kernel, k - 1),
                [rows_out, raw_out] + (hand_outs if k == 1 else []),
                *([fetched] if k == 1 else [w_key, w_value]),
                gain_in,
                *parts,
                *pieces,
                specs=([VMEM] if k == 1 else [HBM] * 2)
                + [VMEM]
                + [HBM] * len(parts)
                + [VMEM] * 2,
                vmem=10,
                scratch=[kv_scratch if k == 1 else key_scratch]
                + [
                    rows_scratch,
                    many,
                    pltpu.VMEM((k - 1, 128, D) if k > 1 else (1, 8, 128), BF16),
                    pltpu.SemaphoreType.DMA((max(k - 1, 1), 8)),
                ],
                flops=2 * 128 * D * 256,
                touched=4_000_000,
            )
            raws.append(raw)
        parts.append(rows)
        if k == 1:
            scale, kv = hand
        if k > 1:
            share, scale, kv = call(
                functools.partial(share_kernel, len(parts) - 1),
                [pltpu.VMEM((1, 128), F32), *hand_outs],
                *tables,
                *raws,
                vmem=4,
                scratch=[kv_scratch, many],
            )
        kv_all = lax.all_to_all(kv, SEQ, split_axis=0, concat_axis=0, tiled=True)
        q = query_dot(share, parts, w_query)
        if k in (0, 2):
            home = move_home(home)
            kv_all, home = lax.optimization_barrier((kv_all, home))
        if k == 0:
            inj, current = call(settle_kernel, (narrow, narrow), *home)
        if k == 2:
            settled = home
        if k > 1:
            current = call(mix_kernel, wide, share, *images)
        own, send = call(
            attend_kernel,
            (pltpu.VMEM((64, D), F32), pltpu.VMEM((64, D), BF16)),
            q,
            scale,
            kv_all,
            w_out,
            specs=[VMEM, VMEM, VMEM, HBM],
            vmem=16,
            scratch=[
                pltpu.VMEM((640, D), BF16),
                pltpu.VMEM((128, 640), BF16),
                pltpu.SemaphoreType.DMA,
            ],
            flops=2 * 128 * 640 * (2 * TOKENS + D),
            touched=9_000_000,
        )
        pair = own + lax.ppermute(send, "c", shift(2, 1)).astype(F32)
        arrived = []
        for by in (1, 2, 3):
            piece = pair[16 * by : 16 * by + 16].astype(BF16)
            arrived.append(lax.ppermute(piece, "y", shift(4, -by)))
        last = k == ITERS - 1
        shapes = [*home_packed, *([] if last else [tokens, tokens, narrow])] if k >= 2 else [wide, narrow]
        scratch = []
        if k > 0:
            shapes.append(pltpu.HBM((128, 1, 128), F32))
            scratch.append(pltpu.VMEM((128, 1, 128), F32))
        if k == 1:
            scratch.append(pltpu.SemaphoreType.DMA)
        if k >= 2:
            scratch += [pltpu.VMEM((16, D), F32)] * 2 + [pltpu.SemaphoreType.DMA((11,))]
        packed = list(home) if last else []
        outs = call(
            functools.partial(finish_kernel, k),
            tuple(shapes),
            pair[:16],
            *arrived,
            inj,
            current,
            gain_out,
            gain_in,
            *residuals,
            *packed,
            specs=[VMEM] * (8 + len(residuals)) + [HBM] * len(packed),
            aliases={8 + k + at: at for at in range(len(packed))},
            scratch=scratch,
        )
        dots = outs[-1] if k > 0 else None
        if k >= 2:
            home = outs[:5]
        if k == 2:
            image, residual, payload = outs[5:8]
            images.append(image)
            residuals.append(residual)
        if k < 2:
            image, payload = outs[:2]
        if k < 2:
            packed = list(home) if k % 2 == 1 else []
            outs = call(
                functools.partial(store_kernel, k),
                (tokens, tokens, *home_packed),
                image,
                current,
                *packed,
                specs=[VMEM] * 2 + [HBM] * len(packed),
                aliases={2 + at: 2 + at for at in range(len(packed))},
                scratch=[pltpu.VMEM((16, D), F32), pltpu.SemaphoreType.DMA((10,))],
            )
            images.append(outs[0])
            residuals.append(outs[1])
            home = outs[2:7]
            if k == 0:
                current = outs[0]
    settled = settled + move_home(home)
    tables.append(lax.all_to_all(dots, EVERY, split_axis=0, concat_axis=0, tiled=True))
    return call(
        functools.partial(last_kernel, ITERS - 1),
        pltpu.HBM((128, 640), F32),
        *tables,
        *settled,
        scratch=[pltpu.VMEM((128, 640), F32), pltpu.SemaphoreType.DMA],
    )


def solution(mesh):
    split = Mesh(mesh.devices.reshape(4, 4, 4, 2), EVERY)
    placed = (
        P(SEQ, FEAT),
        P(SEQ, FEAT),
        P(),
        P(),
        P(None, FEAT),
        P(None, FEAT),
        P(None, FEAT),
        P(FEAT, None),
    )
    return jax.shard_map(
        on_device, mesh=split, in_specs=placed, out_specs=P(SEQ, FEAT), check_vma=False
    )
```
